32 devices in a mesh: tp: 4 (over z), fsdp: 8 (over y, x, core).
Axes of the slice: x: 2, y: 2, z: 4, core: 2. Of those that a mesh axis runs over, the one named last changes fastest.
Arguments:
- g_qkv: float32 [8, 1, 1408, 4224], P('fsdp', None, None, 'tp')
- g_out: float32 [8, 1, 1408, 1408], P('fsdp', None, None, 'tp')
- g_up: float32 [8, 1, 1408, 6144], P('fsdp', None, None, 'tp')
- g_down: float32 [8, 1, 6144, 1408], P('fsdp', None, None, 'tp')
- g_vec: float32 [8, 1, 18816], P('fsdp', None, 'tp')
- w_qkv: float32 [1, 1408, 4224], P(None, 'fsdp', 'tp')
- w_out: float32 [1, 1408, 1408], P(None, 'fsdp', 'tp')
- w_up: float32 [1, 1408, 6144], P(None, 'fsdp', 'tp')
- w_down: float32 [1, 6144, 1408], P(None, 'fsdp', 'tp')
- w_vec: float32 [1, 18816], P(None, 'tp')
- m_qkv: bfloat16 [1, 1408, 4224], P(None, 'fsdp', 'tp')
- m_out: bfloat16 [1, 1408, 1408], P(None, 'fsdp', 'tp')
- m_up: bfloat16 [1, 1408, 6144], P(None, 'fsdp', 'tp')
- m_down: bfloat16 [1, 6144, 1408], P(None, 'fsdp', 'tp')
- m_vec: bfloat16 [1, 18816], P(None, 'tp')
- vr_qkv: float32 [1, 1408], P(None, 'fsdp')
- vc_qkv: float32 [1, 4224], P(None, 'tp')
- vr_out: float32 [1, 1408], P(None, 'fsdp')
- vc_out: float32 [1, 1408], P(None, 'tp')
- vr_up: float32 [1, 1408], P(None, 'fsdp')
- vc_up: float32 [1, 6144], P(None, 'tp')
- vr_down: float32 [1, 6144], P(None, 'fsdp')
- vc_down: float32 [1, 1408], P(None, 'tp')
- v_vec: float32 [1, 18816], P(None, 'tp')
Outputs:
- output 1: float32 [1, 1408, 4224], P(None, 'fsdp', 'tp')
- output 2: float32 [1, 1408, 1408], P(None, 'fsdp', 'tp')
- output 3: float32 [1, 1408, 6144], P(None, 'fsdp', 'tp')
- output 4: float32 [1, 6144, 1408], P(None, 'fsdp', 'tp')
- output 5: float32 [1, 18816], P(None, 'tp')
- output 6: bfloat16 [1, 1408, 4224], P(None, 'fsdp', 'tp')
- output 7: bfloat16 [1, 1408, 1408], P(None, 'fsdp', 'tp')
- output 8: bfloat16 [1, 1408, 6144], P(None, 'fsdp', 'tp')
- output 9: bfloat16 [1, 6144, 1408], P(None, 'fsdp', 'tp')
- output 10: bfloat16 [1, 18816], P(None, 'tp')
- output 11: float32 [1, 1408], P(None, 'fsdp')
- output 12: float32 [1, 4224], P(None, 'tp')
- output 13: float32 [1, 1408], P(None, 'fsdp')
- output 14: float32 [1, 1408], P(None, 'tp')
- output 15: float32 [1, 1408], P(None, 'fsdp')
- output 16: float32 [1, 6144], P(None, 'tp')
- output 17: float32 [1, 6144], P(None, 'fsdp')
- output 18: float32 [1, 1408], P(None, 'tp')
- output 19: float32 [1, 18816], P(None, 'tp')
All inputs are finite; a program needn't handle non-finite values.
Results may differ from the reference program's by a relative error of at most 0.001.
Values sent between devices are 32-bit elements.
A program may use at most 1 GiB of HBM per device.

```python
import jax
import jax.numpy as jnp

MODEL_DIM = 1408
MLP_DIM = 6144
NUM_LAYERS = 1
GRAD_SHARDS = 8
TRAIN_STEP = 3
VEC_LEN = 9 * MODEL_DIM + MLP_DIM
MAT_PARAMS = 4 * MODEL_DIM * MODEL_DIM + 2 * MODEL_DIM * MLP_DIM
VEC_SCALE = (0.25 * MAT_PARAMS / VEC_LEN) ** 0.5
LEARN_RATE = 0.0008
WEIGHT_DECAY = 0.03
MOMENTUM = 0.9
EPSILON = 1e-30
BETA_TWO = 1.0 - TRAIN_STEP ** -0.8
LEVELS = ((0.2, 0.6), (2.0, 4.0), (0.2, 0.6), (2.0, 4.0))


def mat_shapes():
    return [(MODEL_DIM, 3 * MODEL_DIM), (MODEL_DIM, MODEL_DIM), (MODEL_DIM, MLP_DIM), (MLP_DIM, MODEL_DIM)]


def profile(key, count):
    key_sign, key_noise = jax.random.split(key)
    sign_val = 2.0 * jax.random.randint(key_sign, (NUM_LAYERS, 1), 0, 2).astype(jnp.float32) - 1.0
    ramp_val = jnp.linspace(-1.0, 1.0, count, dtype=jnp.float32)
    noise_val = jax.random.normal(key_noise, (NUM_LAYERS, count), jnp.float32)
    return jnp.exp(0.8 * sign_val * ramp_val[None, :] + 0.4 * noise_val)


def draw_partials(key, row_count, col_count):
    key_row, key_col, key_dev, key_val = jax.random.split(key, 4)
    row_scale = profile(key_row, row_count)
    col_scale = profile(key_col, col_count)
    dev_scale = jax.random.uniform(key_dev, (GRAD_SHARDS, NUM_LAYERS, 1, 1), jnp.float32, 0.5, 1.5)
    noise_val = jax.random.normal(key_val, (GRAD_SHARDS, NUM_LAYERS, row_count, col_count), jnp.float32)
    return noise_val * dev_scale * row_scale[None, :, :, None] * col_scale[None, :, None, :]


def draw_vector_partials(key):
    key_col, key_dev, key_val = jax.random.split(key, 3)
    col_scale = VEC_SCALE * profile(key_col, VEC_LEN)
    dev_scale = jax.random.uniform(key_dev, (GRAD_SHARDS, NUM_LAYERS, 1), jnp.float32, 0.5, 1.5)
    noise_val = jax.random.normal(key_val, (GRAD_SHARDS, NUM_LAYERS, VEC_LEN), jnp.float32)
    return noise_val * dev_scale * col_scale[None]


def setup_inputs(seed: int = 0) -> dict:
    key_list = jax.random.split(jax.random.key(seed), 8)
    shapes = mat_shapes()
    mat_names = ['qkv', 'out', 'up', 'down']
    partials = [draw_partials(jax.random.fold_in(key_list[0], mat_index), shapes[mat_index][0], shapes[mat_index][1]) for mat_index in range(4)]
    vec_partials = draw_vector_partials(key_list[1])
    grad_sums = [jnp.sum(part_val, axis=0) for part_val in partials + [vec_partials]]
    total_sq = sum([jnp.sum(jnp.square(grad_sum)) for grad_sum in grad_sums])
    clip_scale = jnp.minimum(1.0, 1.0 / jnp.sqrt(total_sq))
    result = {}
    for mat_index in range(4):
        result['g_' + mat_names[mat_index]] = partials[mat_index]
    result['g_vec'] = vec_partials
    for mat_index in range(4):
        full_shape = (NUM_LAYERS,) + shapes[mat_index]
        result['w_' + mat_names[mat_index]] = jax.random.normal(jax.random.fold_in(key_list[2], mat_index), full_shape, jnp.float32) * shapes[mat_index][0] ** -0.5
    result['w_vec'] = 0.5 * jax.random.normal(key_list[3], (NUM_LAYERS, VEC_LEN), jnp.float32)
    for mat_index in range(4):
        full_shape = (NUM_LAYERS,) + shapes[mat_index]
        result['m_' + mat_names[mat_index]] = (0.1 * jax.random.normal(jax.random.fold_in(key_list[4], mat_index), full_shape, jnp.float32)).astype(jnp.bfloat16)
    result['m_vec'] = (0.1 * jax.random.normal(key_list[5], (NUM_LAYERS, VEC_LEN), jnp.float32)).astype(jnp.bfloat16)
    for mat_index in range(4):
        key_level, key_row, key_col = jax.random.split(jax.random.fold_in(key_list[6], mat_index), 3)
        grad_sq = jnp.square(grad_sums[mat_index] * clip_scale)
        level_val = jax.random.uniform(key_level, (NUM_LAYERS, 1), jnp.float32, LEVELS[mat_index][0], LEVELS[mat_index][1])
        row_factor = jax.random.uniform(key_row, (NUM_LAYERS, shapes[mat_index][0]), jnp.float32, 0.3, 1.2)
        col_factor = jax.random.uniform(key_col, (NUM_LAYERS, shapes[mat_index][1]), jnp.float32, 0.3, 1.2)
        result['vr_' + mat_names[mat_index]] = level_val * row_factor * jnp.mean(grad_sq, axis=2)
        result['vc_' + mat_names[mat_index]] = level_val * col_factor * jnp.mean(grad_sq, axis=1)
    key_level, key_val = jax.random.split(key_list[7])
    vec_sq = jnp.square(grad_sums[4] * clip_scale)
    level_val = jax.random.uniform(key_level, (NUM_LAYERS, 1), jnp.float32, 0.1, 0.3)
    result['v_vec'] = level_val * jnp.exp(0.5 * jax.random.normal(key_val, (NUM_LAYERS, VEC_LEN), jnp.float32)) * jnp.mean(vec_sq, axis=1, keepdims=True)
    return result


def finish_step(update_val, weight, moment):
    moment_new = (MOMENTUM * moment.astype(jnp.float32) + (1.0 - MOMENTUM) * update_val).astype(jnp.bfloat16)
    weight_new = weight - LEARN_RATE * (moment_new.astype(jnp.float32) + WEIGHT_DECAY * weight)
    return weight_new, moment_new


def matrix_step(grad_sum, clip_scale, weight, moment, row_var, col_var):
    grad_val = grad_sum * clip_scale
    grad_sq = jnp.square(grad_val) + EPSILON
    row_new = BETA_TWO * row_var + (1.0 - BETA_TWO) * jnp.mean(grad_sq, axis=2)
    col_new = BETA_TWO * col_var + (1.0 - BETA_TWO) * jnp.mean(grad_sq, axis=1)
    row_norm = row_new / jnp.mean(row_new, axis=1, keepdims=True)
    update_val = grad_val / jnp.sqrt(row_norm[:, :, None] * col_new[:, None, :])
    update_rms = jnp.sqrt(jnp.mean(jnp.square(update_val), axis=(1, 2), keepdims=True))
    update_val = update_val / jnp.maximum(1.0, update_rms)
    weight_new, moment_new = finish_step(update_val, weight, moment)
    return weight_new, moment_new, row_new, col_new


def vector_step(grad_sum, clip_scale, weight, moment, var_old):
    grad_val = grad_sum * clip_scale
    var_new = BETA_TWO * var_old + (1.0 - BETA_TWO) * (jnp.square(grad_val) + EPSILON)
    update_val = grad_val / jnp.sqrt(var_new)
    update_rms = jnp.sqrt(jnp.mean(jnp.square(update_val), axis=1, keepdims=True))
    update_val = update_val / jnp.maximum(1.0, update_rms)
    weight_new, moment_new = finish_step(update_val, weight, moment)
    return weight_new, moment_new, var_new


def reference(g_qkv, g_out, g_up, g_down, g_vec, w_qkv, w_out, w_up, w_down, w_vec, m_qkv, m_out, m_up, m_down, m_vec, vr_qkv, vc_qkv, vr_out, vc_out, vr_up, vc_up, vr_down, vc_down, v_vec):
    grad_sums = [jnp.sum(g_part, axis=0) for g_part in (g_qkv, g_out, g_up, g_down, g_vec)]
    total_sq = sum([jnp.sum(jnp.square(grad_sum)) for grad_sum in grad_sums])
    clip_scale = jnp.minimum(1.0, 1.0 / jnp.sqrt(total_sq))
    weights = (w_qkv, w_out, w_up, w_down)
    moments = (m_qkv, m_out, m_up, m_down)
    row_vars = (vr_qkv, vr_out, vr_up, vr_down)
    col_vars = (vc_qkv, vc_out, vc_up, vc_down)
    results = [matrix_step(grad_sums[mat_index], clip_scale, weights[mat_index], moments[mat_index], row_vars[mat_index], col_vars[mat_index]) for mat_index in range(4)]
    vec_res = vector_step(grad_sums[4], clip_scale, w_vec, m_vec, v_vec)
    return (results[0][0], results[1][0], results[2][0], results[3][0], vec_res[0], results[0][1], results[1][1], results[2][1], results[3][1], vec_res[1], results[0][2], results[0][3], results[1][2], results[1][3], results[2][2], results[2][3], results[3][2], results[3][3], vec_res[2])
```

```python
import jax
import jax.numpy as jnp
from jax import lax
from jax.experimental import pallas as pl
from jax.experimental.pallas import tpu as pltpu
from jax.sharding import PartitionSpec as P

TRAIN_STEP = 3
LEARN_RATE = 0.0008
WEIGHT_DECAY = 0.03
MOMENTUM = 0.9
EPSILON = 1e-30
BETA_TWO = 1.0 - TRAIN_STEP ** -0.8
KEEP, MIX = BETA_TWO, 1.0 - BETA_TWO

F32 = jnp.float32
BF16 = jnp.bfloat16
MESH = pl.DeviceIdType.MESH
HIGHEST = lax.Precision.HIGHEST
TP, FSDP, DEVICES = 4, 8, 32
SUB, LANE = 8, 128

ROWS = (176, 176, 176, 768)
COLS = (1056, 352, 1536, 352)
VEC = 4704
R, QO, UP, DR, DC = ROWS[0], COLS[0] + COLS[1], COLS[2], ROWS[3], COLS[3]
HALF_R, HALF_DC = R // 2, DC // 2
STEPS = QO // LANE
D_STEP = HALF_DC // STEPS
Q_FULL = COLS[0] // LANE
Q_LEFT = COLS[0] - Q_FULL * LANE
ROW_TILES = R // SUB
D_TILES = DC // SUB
WIDE = -(-(QO + UP) // (SUB * LANE)) * SUB * LANE
LOOK, SLOTS = 3, 4
U_, QO_, D_ = 0, 1, 2
VR_AT, VEC_AT = 4, 8


def lanes(shape):
    return lax.broadcasted_iota(jnp.int32, shape, len(shape) - 1)


def sublanes(shape):
    return lax.broadcasted_iota(jnp.int32, shape, len(shape) - 2)


def total(x):
    return jnp.sum(jnp.sum(x, axis=1, keepdims=True), axis=0, keepdims=True)


def pick(x, lane):
    return jnp.sum(jnp.where(lanes(x.shape) == lane, x, 0.0), axis=1, keepdims=True)


def dot(a, b):
    return lax.dot_general(a, b, (((1,), (0,)), ((), ())), precision=HIGHEST, preferred_element_type=F32)


def own_sublane(n):
    return lanes((SUB, n)) % SUB == sublanes((SUB, n))


def to_tiles(row, at):
    n = row.shape[1]
    chosen = (sublanes((n, LANE)) // SUB + at == lanes((n, LANE))).astype(F32)
    return dot(jnp.where(own_sublane(n), row, 0.0), chosen)


def from_tiles(tiles, at, n):
    chosen = (lanes((LANE, n)) // SUB + at == sublanes((LANE, n))).astype(F32)
    return jnp.sum(jnp.where(own_sublane(n), dot(tiles, chosen), 0.0), axis=0, keepdims=True)


def across(tiles, t):
    return jnp.broadcast_to(tiles[:, t:t + 1], (SUB, LANE))


def reduce_kernel(*refs):
    (gq, go, gu, gd, gv, vrq, vro, vru, vrd, vcq, vco, vcu, vcd, vv,
     hqo, hu, hd, hv, inv_out,
     n_rq, n_ro, n_ru, n_rd, n_cq, n_co, n_cu, n_cd, vv_new,
     own_qo, own_u, own_d, peer_qo, peer_u, peer_d, s_qo,
     a_qo, a_u, a_d, b_qo, b_u, b_d,
     vec_own, vec_in, vec_mid, vv_in,
     r_q, r_o, r_u, r_d, c_q, c_o, c_u, c_d,
     p_q, p_o, cs_qo, cs_u, rs_d, rp_acc, rpd_acc, rp_old, rpd_old, col_buf, rowd_buf,
     cs_all, rp_all, rsd_all, rpd_all, s_all, u_all,
     own_sem, peer_sem, push_sem, first_sem, second_sem, a_sem, b_sem,
     vec_sem, vec_send, vec_recv, small_sem, stat_send, stat_recv) = refs

    me = lax.axis_index("fsdp")
    z = lax.axis_index("tp")
    core = lax.rem(me, 2)
    x = lax.rem(me // 2, 2)
    y = me // 4
    linear = z * FSDP + me
    mate = {"fsdp": me + 1 - 2 * core}
    across_x = {"fsdp": me + 2 - 4 * x}
    across_y = {"fsdp": me + 4 - 8 * y}
    every = slice(None)

    owns, peers = (own_u, own_qo, own_d), (peer_u, peer_qo, peer_d)
    sums, firsts, seconds = (own_u, s_qo, own_d), (a_u, a_qo, a_d), (b_u, b_qo, b_d)

    def send(src, dst, ssem, rsem, to):
        return pltpu.make_async_remote_copy(
            src_ref=src, dst_ref=dst, send_sem=ssem, recv_sem=rsem,
            device_id=to, device_id_type=MESH)

    def index(kind, lead, side, k):
        if kind == QO_:
            return (k,) + lead + (pl.ds(HALF_R * side, HALF_R),)
        if kind == U_:
            return lead + (pl.ds(pl.multiple_of(HALF_R * side + SUB * k, SUB), SUB),)
        return lead + (pl.ds(pl.multiple_of(HALF_DC * side + D_STEP * k, SUB), D_STEP),)

    def whole(kind, lead, side):
        if kind == QO_:
            return (every,) + lead + (pl.ds(HALF_R * side, HALF_R),)
        n = HALF_R if kind == U_ else HALF_DC
        return lead + (pl.ds(n * side, n),)

    def first(kind, side, at, sem):
        lead, to = (((every, 1 - x), across_x), ((1 - y, every), across_y))[side]
        return send(sums[kind].at[at(kind, lead, side)], firsts[kind].at[at(kind, (every,), side)],
                    first_sem.at[kind, side], sem, to)

    def second(kind, side, at, sem):
        lead, to = (((1 - y, x), across_y), ((y, 1 - x), across_x))[side]
        return send(sums[kind].at[at(kind, lead, side)], seconds[kind].at[at(kind, (), side)],
                    second_sem.at[kind, side], sem, to)

    def chunk(k):
        return lambda kind, lead, side: index(kind, lead, side, k)

    def load(kind, k, side, away):
        if away:
            dst, sem, c = peers[kind], peer_sem.at[kind, side, k], 1 - core
            copy = lambda a, b: send(a, b, push_sem.at[kind], sem, mate)
        else:
            dst, sem, c = owns[kind], own_sem.at[kind, side, k], core
            copy = lambda a, b: pltpu.make_async_copy(a, b, sem)
        if kind == U_:
            at = index(kind, (), side, k)
            return [(None, copy(gu.at[(every, every, c) + at], dst.at[(every, every) + at]))]
        if kind == D_:
            at = index(kind, (), side, k)
            return [(None, copy(gd.at[at + (pl.ds(pl.multiple_of(DR * (2 * b + c), LANE), DR),)],
                                dst.at[(b // 2, b % 2) + at])) for b in range(4)]
        slot = dst.at[k if away else lax.rem(k, SLOTS)]
        rest = LANE - Q_LEFT
        at_q = pl.multiple_of(LANE * jnp.minimum(k, Q_FULL - 1), LANE)
        at_o = pl.multiple_of(rest + LANE * jnp.maximum(k - Q_FULL - 1, 0), SUB)
        return [(k < Q_FULL, copy(gq.at[pl.ds(at_q, LANE)], slot)),
                (k == Q_FULL, copy(gq.at[pl.ds(Q_FULL * LANE, Q_LEFT)], slot.at[pl.ds(0, Q_LEFT)])),
                (k == Q_FULL, copy(go.at[pl.ds(0, rest)], slot.at[pl.ds(Q_LEFT, rest)])),
                (k > Q_FULL, copy(go.at[pl.ds(at_o, LANE)], slot))]

    def start_kind(kind, k, away):
        for side in range(1 if kind == QO_ else 2):
            for cond, copy in load(kind, k, side, away):
                if cond is None:
                    copy.start()
                else:
                    pl.when(cond)(copy.start)

    def start_loads(step, away):
        for kind in range(3):
            k = step - kind * STEPS
            pl.when(jnp.logical_and(k >= 0, k < STEPS))(lambda kind=kind, k=k: start_kind(kind, k, away))

    def loaded(kind, side, k):
        if kind == QO_:
            here, there = own_qo.at[lax.rem(k, SLOTS)], peer_qo.at[k]
        else:
            at = index(kind, (every, every), side, k)
            here, there = owns[kind].at[at], peers[kind].at[at]
        pltpu.make_async_copy(here, here, own_sem.at[kind, side, k]).wait()
        send(there, there, push_sem.at[kind], peer_sem.at[kind, side, k], mate).wait_recv()

    smalls = [(vrq, r_q), (vro, r_o), (vru, r_u), (vrd, r_d),
              (vcq, c_q), (vco, c_o), (vcu, c_u), (vcd, c_d), (vv, vv_in)]
    small_copies = [pltpu.make_async_copy(a, b, small_sem.at[i]) for i, (a, b) in enumerate(smalls)]
    vec_copy = pltpu.make_async_copy(gv, vec_own, vec_sem.at[0])

    for step in range(LOOK):
        start_kind(U_, step, False)
    vec_copy.start()
    for copy in small_copies:
        copy.start()
    barrier = pltpu.get_barrier_semaphore()

    def other(d):
        to = lax.rem(linear + d, DEVICES)
        return {"tp": to // FSDP, "fsdp": lax.rem(to, FSDP)}

    for d in range(1, DEVICES):
        pl.semaphore_signal(barrier, inc=1, device_id=other(d), device_id_type=MESH)
    pl.semaphore_wait(barrier, DEVICES - 1)

    for step in range(LOOK):
        start_kind(U_, step, True)
    vec_copy.wait()
    vec_core = send(vec_own, vec_in.at[0], vec_send.at[0], vec_recv.at[0], mate)
    vec_x = send(vec_mid.at[0], vec_in.at[1], vec_send.at[1], vec_recv.at[1], across_x)
    vec_y = send(vec_mid.at[1], vec_in.at[2], vec_send.at[2], vec_recv.at[2], across_y)
    vec_core.start()

    def turn(k, which):
        slot = lax.rem(k, SLOTS)
        for tile in range(STEPS):
            lo = LANE * tile
            cuts = [(b, max(lo, R * (2 * b + which)), min(lo + LANE, R * (2 * b + which) + R)) for b in range(4)]
            cuts = [cut for cut in cuts if cut[1] < cut[2]]
            if cuts:
                at = (every, pl.ds(lo, LANE))
                turned = (own_qo[(slot,) + at] + peer_qo[(k,) + at]).T
                for b, start, stop in cuts:
                    first_row = start - R * (2 * b + which)
                    s_qo[k, b // 2, b % 2, pl.ds(first_row, stop - start), :] = turned[start - lo:stop - lo]

    def stage1(kind):
        def body(k, _):
            start_loads(k + kind * STEPS + LOOK, False)
            start_loads(k + kind * STEPS + LOOK, True)
            if kind == QO_:
                loaded(kind, 0, k)
                for which in range(2):
                    pl.when(core == which)(lambda which=which: turn(k, which))
            for side in range(2):
                if kind != QO_:
                    loaded(kind, side, k)
                    for b in range(4):
                        at = index(kind, (b // 2, b % 2), side, k)
                        owns[kind][at] = owns[kind][at] + peers[kind][at]
                first(kind, side, chunk(k), a_sem.at[kind, side, k]).start()
            return _
        return body

    vec_core.wait_recv()
    vec_mid[0] = vec_own[...] + vec_in[0]
    lax.fori_loop(0, 1, stage1(U_), 0)
    vec_x.start()
    lax.fori_loop(1, STEPS, stage1(U_), 0)
    for kind in (QO_, D_):
        lax.fori_loop(0, STEPS, stage1(kind), 0)

    for copy in small_copies:
        copy.wait()
    for ref in (cs_qo, cs_u, rs_d, rp_acc, rpd_acc, p_q, p_o):
        ref[...] = jnp.zeros_like(ref)
    old = to_tiles(r_q[...], 0) + to_tiles(r_o[...], ROW_TILES) + to_tiles(r_u[...], 2 * ROW_TILES)
    rp_old[...] = old
    rpd_old[...] = to_tiles(c_d[...], 0)
    lane = lanes((SUB, LANE))
    lane1 = lanes((1, LANE))
    masks = [jnp.logical_and(lane >= ROW_TILES * m, lane < ROW_TILES * (m + 1)) for m in range(3)]
    old_sums = [total(jnp.where(masks[m], old, 0.0)) for m in range(3)] + [total(r_d[...])]

    def stage2(kind):
        def body(k, _):
            for side in range(2):
                first(kind, side, chunk(k), a_sem.at[kind, side, k]).wait_recv()
                lead, mine = (((1 - y, x), 1 - y), ((y, 1 - x), 1 - x))[side]
                at = index(kind, lead, side, k)
                sums[kind][at] = sums[kind][at] + firsts[kind][index(kind, (mine,), side, k)]
                second(kind, side, chunk(k), b_sem.at[kind, side, k]).start()
            return _
        return body

    for kind in (U_, QO_):
        lax.fori_loop(0, STEPS, stage2(kind), 0)
    vec_x.wait_recv()
    vec_mid[1] = vec_mid[0] + vec_in[1]
    vec_y.start()
    lax.fori_loop(0, STEPS, stage2(D_), 0)

    def finished(kind, side, k):
        second(kind, side, chunk(k), b_sem.at[kind, side, k]).wait_recv()
        return (sums[kind][index(kind, (y, x), side, k)]
                + firsts[kind][index(kind, ((y, x)[side],), side, k)]
                + seconds[kind][index(kind, (), side, k)])

    def stage3_u(k, _):
        for side in range(2):
            full = finished(U_, side, k)
            hu[index(U_, (), side, k)] = full
            sq = full * full
            cs_u[...] += sq
            row = jnp.sum(sq, axis=1, keepdims=True)
            rp_acc[...] = jnp.where(lane == 2 * ROW_TILES + STEPS * side + k, row, rp_acc[...])
        return _

    def stage3_qo(k, _):
        for side in range(2):
            rows = pl.ds(HALF_R * side, HALF_R)
            full = finished(QO_, side, k)
            hqo[rows, pl.ds(pl.multiple_of(LANE * k, LANE), LANE)] = full
            sq = full * full
            in_q = lanes(sq.shape) + LANE * k < COLS[0]
            p_q[rows, :] += jnp.where(in_q, sq, 0.0)
            p_o[rows, :] += jnp.where(in_q, 0.0, sq)
            part = sq[:SUB]
            for t in range(1, STEPS):
                part = part + sq[SUB * t:SUB * t + SUB]
            cs_qo[k] += part
        return _

    def stage3_d(k, _):
        for side in range(2):
            full = finished(D_, side, k)
            hd[index(D_, (), side, k)] = full
            sq = full * full
            both = rpd_acc[...]
            for t in range(D_STEP // SUB):
                part = sq[SUB * t:SUB * t + SUB]
                rs_d[...] += part
                col = jnp.sum(part, axis=1, keepdims=True)
                at = (HALF_DC * side + D_STEP * k) // SUB + t
                both = jnp.where(lane == at, col, both)
            rpd_acc[...] = both
        return _

    def to_group(buf, at, i, n, axis, here):
        for d in range(1, n):
            send(buf.at[at], buf.at[at], stat_send.at[i], stat_recv.at[i],
                 {axis: lax.rem(here + d, n)}).start()

    def to_all(buf, i):
        for d in range(1, DEVICES):
            send(buf.at[linear], buf.at[linear], stat_send.at[i], stat_recv.at[i], other(d)).start()

    def spread(buf, i, n):
        part = buf.at[pl.ds(0, n - 1)]
        return send(part, part, stat_send.at[i], stat_recv.at[i], mate)

    def gathered(buf, i, n):
        spread(buf, i, n).wait_recv()
        out = buf[0]
        for d in range(1, n):
            out = out + buf[d]
        return out

    lax.fori_loop(0, STEPS, stage3_u, 0)
    lax.fori_loop(0, STEPS, stage3_qo, 0)
    vec_y.wait_recv()
    vec = vec_mid[1] + vec_in[2]
    hv[...] = vec
    rp = rp_acc[...]
    for t in range(ROW_TILES):
        for m, ref in enumerate((p_q, p_o)):
            row = jnp.sum(ref[pl.ds(SUB * t, SUB), :], axis=1, keepdims=True)
            rp = jnp.where(lane == ROW_TILES * m + t, row, rp)
    rp_all[z] = rp
    cs = [jnp.sum(cs_qo[k], axis=0, keepdims=True) for k in range(STEPS)]
    cs.append(jnp.sum(cs_u[...], axis=0, keepdims=True))
    cs_all[me] = jnp.concatenate(cs + [jnp.zeros((1, WIDE - QO - UP), F32)], axis=1)
    to_group(rp_all, z, 0, TP, "tp", z)
    to_group(cs_all, me, 1, FSDP, "fsdp", me)
    pack = jnp.where(lane1 == VEC_AT, jnp.sum(vec * vec, axis=1, keepdims=True), 0.0)
    for m in range(4):
        pack = jnp.where(lane1 == VR_AT + m, old_sums[m], pack)
    for m in range(3):
        pack = jnp.where(lane1 == m, total(jnp.where(masks[m], rp, 0.0)), pack)

    lax.fori_loop(0, STEPS, stage3_d, 0)
    rs = rs_d[...]
    s_all[linear] = jnp.where(lane1 == 3, total(rs), pack)
    to_all(s_all, 4)
    rsd_all[z] = jnp.sum(rs, axis=0, keepdims=True)
    to_group(rsd_all, z, 2, TP, "tp", z)
    rpd_all[me] = rpd_acc[...]
    to_group(rpd_all, me, 3, FSDP, "fsdp", me)

    vc_old = jnp.concatenate([c_q[...], c_o[...], c_u[...], jnp.ones((1, WIDE - QO - UP), F32)], axis=1)
    rp = gathered(rp_all, 0, TP)
    cs = gathered(cs_all, 1, FSDP)
    rsd = gathered(rsd_all, 2, TP)
    rpd = gathered(rpd_all, 3, FSDP)
    pack = gathered(s_all, 4, DEVICES)
    squares = [pick(pack, m) for m in range(4)]
    norm = jnp.sqrt((squares[0] + squares[1]) + (squares[2] + squares[3]) + pick(pack, VEC_AT) / FSDP)
    clip = jnp.minimum(1.0, 1.0 / norm)

    def clipped(v):
        return jnp.where(clip > 0.0, (v * clip) * clip, 0.0)

    means = []
    for m in range(4):
        r_all, c_all = float(ROWS[m] * FSDP), float(COLS[m] * TP)
        means.append(KEEP * (pick(pack, VR_AT + m) / (TP * r_all))
                     + MIX * (clipped(squares[m]) / (r_all * c_all) + EPSILON))
    mean_rp = jnp.where(masks[0], means[0], jnp.where(masks[1], means[1], means[2]))
    wide = jnp.where(masks[0], float(COLS[0] * TP), jnp.where(masks[1], float(COLS[1] * TP), float(COLS[2] * TP)))
    row_new = KEEP * rp_old[...] + MIX * (clipped(rp) / wide + EPSILON)
    row_sq = mean_rp / row_new
    rowd_new = KEEP * r_d[...] + MIX * (clipped(rsd) / float(DC * TP) + EPSILON)
    rowd_buf[...] = clip * jnp.sqrt(means[3] / rowd_new)
    col_new = KEEP * vc_old + MIX * (clipped(cs) / float(R * FSDP) + EPSILON)
    col_buf[...] = clip / jnp.sqrt(col_new)
    cold_new = KEEP * rpd_old[...] + MIX * (clipped(rpd) / float(DR * FSDP) + EPSILON)
    cold_sq = 1.0 / cold_new

    def tile(ref, j):
        return jnp.broadcast_to(ref[:, pl.ds(LANE * j, LANE)], (SUB, LANE))

    zero = jnp.zeros((SUB, LANE), F32)
    acc = [zero] * 4
    in_q = lane < Q_LEFT
    col_t = [tile(col_buf, j) for j in range(STEPS + UP // LANE)]
    for t in range(ROW_TILES):
        rows = pl.ds(SUB * t, SUB)
        part = [zero] * 3
        for j in range(STEPS):
            u = hqo[rows, pl.ds(LANE * j, LANE)] * col_t[j]
            u = u * u
            if j == Q_FULL:
                part[0] = part[0] + jnp.where(in_q, u, 0.0)
                part[1] = part[1] + jnp.where(in_q, 0.0, u)
            else:
                part[j // Q_FULL] = part[j // Q_FULL] + u
        for j in range(UP // LANE):
            u = hu[rows, pl.ds(LANE * j, LANE)] * col_t[STEPS + j]
            part[2] = part[2] + u * u
        for m in range(3):
            acc[m] = acc[m] + part[m] * across(row_sq, ROW_TILES * m + t)
    rowd_t = [tile(rowd_buf, j) for j in range(DR // LANE)]
    for t in range(D_TILES):
        part = zero
        for j in range(DR // LANE):
            u = hd[pl.ds(SUB * t, SUB), pl.ds(LANE * j, LANE)] * rowd_t[j]
            part = part + u * u
        acc[3] = acc[3] + part * across(cold_sq, t)
    vec = hv[...] * clip
    v_new = KEEP * vv_in[...] + MIX * (vec * vec + EPSILON)
    vec = vec / jnp.sqrt(v_new)
    pack = jnp.where(lane1 == VEC_AT, jnp.sum(vec * vec, axis=1, keepdims=True), 0.0)
    for m in range(4):
        pack = jnp.where(lane1 == m, total(acc[m]), pack)
    u_all[linear] = pack
    to_all(u_all, 5)

    vv_new[...] = v_new
    hv[...] = vec
    row = jnp.sqrt(row_sq)
    cold = jnp.sqrt(cold_sq)
    for t in range(ROW_TILES):
        rows = pl.ds(SUB * t, SUB)
        scale = [across(row, ROW_TILES * m + t) for m in range(3)]
        mixed = jnp.where(in_q, scale[0], scale[1])
        for j in range(STEPS):
            at = pl.ds(LANE * j, LANE)
            hqo[rows, at] = hqo[rows, at] * col_t[j] * (mixed if j == Q_FULL else scale[j // Q_FULL])
        for j in range(UP // LANE):
            at = pl.ds(LANE * j, LANE)
            hu[rows, at] = hu[rows, at] * col_t[STEPS + j] * scale[2]
    for t in range(D_TILES):
        rows = pl.ds(SUB * t, SUB)
        scale = across(cold, t)
        for j in range(DR // LANE):
            at = pl.ds(LANE * j, LANE)
            hd[rows, at] = hd[rows, at] * rowd_t[j] * scale
    for m, ref in enumerate((n_rq, n_ro, n_ru)):
        ref[...] = from_tiles(row_new, ROW_TILES * m, R)
    n_rd[...] = rowd_new
    n_cq[...] = col_new[:, :COLS[0]]
    n_co[...] = col_new[:, COLS[0]:QO]
    n_cu[...] = col_new[:, QO:QO + UP]
    n_cd[...] = from_tiles(cold_new, 0, DC)

    for kind in range(3):
        send(peers[kind], peers[kind], push_sem.at[kind], peer_sem.at[kind, 0, 0], mate).wait_send()
        for side in range(2):
            first(kind, side, whole, a_sem.at[kind, side, 0]).wait_send()
            second(kind, side, whole, b_sem.at[kind, side, 0]).wait_send()
    for copy in (vec_core, vec_x, vec_y):
        copy.wait_send()
    groups = ((rp_all, TP), (cs_all, FSDP), (rsd_all, TP), (rpd_all, FSDP), (s_all, DEVICES), (u_all, DEVICES))
    for i, (buf, n) in enumerate(groups):
        if i < len(groups) - 1:
            spread(buf, i, n).wait_send()

    pack = gathered(u_all, len(groups) - 1, DEVICES)
    count = jnp.full((1, LANE), float(VEC * TP * FSDP), F32)
    for m in range(4):
        count = jnp.where(lane1 == m, float(ROWS[m] * FSDP * COLS[m] * TP), count)
    inv_out[...] = 1.0 / jnp.maximum(1.0, jnp.sqrt(pack / count))
    spread(u_all, len(groups) - 1, DEVICES).wait_send()


PIECES = ((3, 0, HALF_DC), (3, HALF_DC, HALF_DC), (2, 0, R), (0, 0, R), (1, 0, R))
HELD = (ROWS[:3] + (DC,), COLS[:3] + (DR,))
GROUP = 16


def update_kernel(*refs):
    (hqo, hu, hd, hv, inv, vrq, vro, vru, vrd, vcq, vco, vcu, vcd, vv,
     wq, wo, wu, wd, wv, mq, mo, mu, md, mv,
     wq_out, wo_out, wu_out, wd_out, wv_out, mq_out, mo_out, mu_out, md_out, mv_out,
     vrq_out, vcq_out, vro_out, vco_out, vru_out, vcu_out, vrd_out, vcd_out, vv_out,
     bwq, bwo, bwu, bwd, bmq, bmo, bmu, bmd, out_sem) = refs
    held = ((hqo, 0), (hqo, COLS[0]), (hu, 0), (hd, 0))
    w_in, m_in = (wq, wo, wu, wd), (mq, mo, mu, md)
    w_buf, m_buf = (bwq, bwo, bwu, bwd), (bmq, bmo, bmu, bmd)
    w_out, m_out = (wq_out, wo_out, wu_out, wd_out), (mq_out, mo_out, mu_out, md_out)

    def finish(u, w, m):
        m_new = (MOMENTUM * m.astype(F32) + (1.0 - MOMENTUM) * u).astype(BF16)
        return w - LEARN_RATE * (m_new.astype(F32) + WEIGHT_DECAY * w), m_new

    stores = []
    for i, (m, r0, n) in enumerate(PIECES):
        scale = inv[:, m:m + 1]
        buf, c0 = held[m]

        for k in range(n // GROUP):
            rows = pl.ds(r0 + GROUP * k, GROUP)
            u = buf[rows, pl.ds(c0 // LANE * LANE, c0 % LANE + HELD[1][m])][:, c0 % LANE:]
            w_new, m_new = finish(u * scale, w_in[m][rows, :], m_in[m][rows, :])
            w_buf[m][rows, :] = w_new
            m_buf[m][rows, :] = m_new
        rows = pl.ds(r0, n)
        for j, (src, dst) in enumerate(((w_buf, w_out), (m_buf, m_out))):
            stores.append(pltpu.make_async_copy(src[m].at[rows, :], dst[m].at[rows, :], out_sem.at[i, j]))
            stores[-1].start()
    w_new, m_new = finish(hv[...] * inv[:, VEC_AT:VEC_AT + 1], wv[...], mv[...])
    wv_out[...] = w_new
    mv_out[...] = m_new
    for src, dst in ((vrq, vrq_out), (vro, vro_out), (vru, vru_out), (vrd, vrd_out),
                     (vcq, vcq_out), (vco, vco_out), (vcu, vcu_out), (vcd, vcd_out), (vv, vv_out)):
        dst[...] = src[...]
    for copy in stores:
        copy.wait()


IN_HBM = pl.BlockSpec(memory_space=pltpu.HBM)
IN_VMEM = pl.BlockSpec(memory_space=pltpu.VMEM)
MIB = 1024 * 1024


def f32(*shape):
    return jax.ShapeDtypeStruct(shape, F32)


def vmem(*shape):
    return pltpu.VMEM(shape, F32)


def local_step(g_qkv, g_out, g_up, g_down, g_vec, w_qkv, w_out, w_up, w_down, w_vec,
               m_qkv, m_out, m_up, m_down, m_vec, vr_qkv, vc_qkv, vr_out, vc_out,
               vr_up, vc_up, vr_down, vc_down, v_vec):
    dma = pltpu.SemaphoreType.DMA
    rows_shapes = [(1, n) for n in ROWS]
    cols_shapes = [(1, n) for n in COLS]
    h_shapes = [(R, QO), (R, UP), (DC, DR)]
    wide_u, wide_d, vec = (R, UP), (DC, DR), (1, VEC)
    shapes = [
        (SLOTS, LANE, QO), (2, 2) + wide_u, (2, 2) + wide_d,
        (STEPS, LANE, QO), (2, 2) + wide_u, (2, 2) + wide_d, (STEPS, 2, 2, R, LANE),
        (STEPS, 2, R, LANE), (2,) + wide_u, (2,) + wide_d, (STEPS, R, LANE), wide_u, wide_d,
        vec, (3,) + vec, (2,) + vec, vec] + rows_shapes + cols_shapes + [
        (R, LANE), (R, LANE), (STEPS, SUB, LANE), (SUB, UP), (SUB, DR)] + [(SUB, LANE)] * 4 + [
        (1, WIDE), (1, DR),
        (FSDP, 1, WIDE), (TP, SUB, LANE), (TP, 1, DR), (FSDP, SUB, LANE),
        (DEVICES, 1, LANE), (DEVICES, 1, LANE)]
    sems = [(3, 2, STEPS)] * 2 + [(3,), (3, 2), (3, 2)] + [(3, 2, STEPS)] * 2 + [(1,), (3,), (3,), (9,), (6,), (6,)]
    inputs = [pltpu.with_memory_space_constraint(a, pltpu.HBM)
              for a in (g_qkv[0, 0].T, g_out[0, 0].T, g_up.reshape(2, 2, 2, R, UP), g_down[0, 0].T, g_vec[0],
                        vr_qkv, vr_out, vr_up, vr_down, vc_qkv, vc_out, vc_up, vc_down, v_vec)]
    reduced = pl.pallas_call(
        reduce_kernel,
        name="reduce_and_scale",
        out_shape=[f32(*s) for s in h_shapes + [vec, (1, LANE)] + rows_shapes + cols_shapes + [vec]],
        in_specs=[IN_HBM] * 14,
        out_specs=[IN_VMEM] * 14,
        scratch_shapes=[vmem(*s) for s in shapes] + [dma(s) for s in sems],
        compiler_params=pltpu.CompilerParams(
            collective_id=0, has_side_effects=True, vmem_limit_bytes=A_MIB * MIB),
    )(*inputs)

    ws = [w_qkv[0], w_out[0], w_up[0], w_down[0].T, w_vec]
    ms = [m_qkv[0], m_out[0], m_up[0], m_down[0].T, m_vec]
    mats = list(zip(*HELD))
    outs = pl.pallas_call(
        update_kernel,
        name="update",
        out_shape=([f32(*s) for s in mats + [vec]] + [jax.ShapeDtypeStruct(s, BF16) for s in mats + [vec]]
                   + [f32(*s) for m in range(4) for s in (rows_shapes[m], cols_shapes[m])] + [f32(*vec)]),
        in_specs=[IN_VMEM] * 24,
        out_specs=([IN_HBM] * 4 + [IN_VMEM]) * 2 + [IN_VMEM] * 9,
        scratch_shapes=([vmem(*s) for s in mats] + [pltpu.VMEM(s, BF16) for s in mats] + [dma((len(PIECES), 2))]),
        compiler_params=pltpu.CompilerParams(vmem_limit_bytes=B_MIB * MIB),
    )(*reduced, *ws, *ms)
    outs = list(outs)
    for i in range(10):
        if i % 5 == 3:
            outs[i] = outs[i].T
        if i % 5 != 4:
            outs[i] = outs[i][None]
    return tuple(outs)


A_MIB, B_MIB = 46, 12


def solution(mesh):
    grad_spec = P("fsdp", None, None, "tp")
    vec_grad_spec = P("fsdp", None, "tp")
    mat_spec = P(None, "fsdp", "tp")
    vec_spec = P(None, "tp")
    row_spec = P(None, "fsdp")
    col_spec = P(None, "tp")
    state_specs = ((mat_spec,) * 4 + (vec_spec,) + (mat_spec,) * 4 + (vec_spec,)
                   + (row_spec, col_spec) * 4 + (vec_spec,))
    arg_specs = (grad_spec,) * 4 + (vec_grad_spec,) + state_specs
    return jax.shard_map(local_step, mesh=mesh, in_specs=arg_specs, out_specs=state_specs, check_vma=False)
```

```python
import jax
import jax.numpy as jnp
from jax import lax
from jax.experimental import pallas as pl
from jax.experimental.pallas import tpu as pltpu
from jax.sharding import PartitionSpec as P

TRAIN_STEP = 3
LEARN_RATE = 0.0008
WEIGHT_DECAY = 0.03
MOMENTUM = 0.9
EPSILON = 1e-30
BETA_TWO = 1.0 - TRAIN_STEP ** -0.8
KEEP, MIX = BETA_TWO, 1.0 - BETA_TWO

F32 = jnp.float32
BF16 = jnp.bfloat16
MESH = pl.DeviceIdType.MESH
HIGHEST = lax.Precision.HIGHEST
TP, FSDP, DEVICES = 4, 8, 32
SUB, LANE = 8, 128

ROWS = (176, 176, 176, 768)
COLS = (1056, 352, 1536, 352)
VEC = 4704
R, QO, UP, DR, DC = ROWS[0], COLS[0] + COLS[1], COLS[2], ROWS[3], COLS[3]
HALF_R, HALF_DC = R // 2, DC // 2
STEPS = QO // LANE
D_STEP = HALF_DC // STEPS
Q_FULL = COLS[0] // LANE
Q_LEFT = COLS[0] - Q_FULL * LANE
ROW_TILES = R // SUB
D_TILES = DC // SUB
WIDE = -(-(QO + UP) // (SUB * LANE)) * SUB * LANE
LOOK, SLOTS = 3, 4
U_, QO_, D_ = 0, 1, 2
VR_AT, VEC_AT = 4, 8


def lanes(shape):
    return lax.broadcasted_iota(jnp.int32, shape, len(shape) - 1)


def sublanes(shape):
    return lax.broadcasted_iota(jnp.int32, shape, len(shape) - 2)


def total(x):
    return jnp.sum(jnp.sum(x, axis=1, keepdims=True), axis=0, keepdims=True)


def pick(x, lane):
    return jnp.sum(jnp.where(lanes(x.shape) == lane, x, 0.0), axis=1, keepdims=True)


def dot(a, b):
    return lax.dot_general(a, b, (((1,), (0,)), ((), ())), precision=HIGHEST, preferred_element_type=F32)


def own_sublane(n):
    return lanes((SUB, n)) % SUB == sublanes((SUB, n))


def to_tiles(row, at):
    n = row.shape[1]
    chosen = (sublanes((n, LANE)) // SUB + at == lanes((n, LANE))).astype(F32)
    return dot(jnp.where(own_sublane(n), row, 0.0), chosen)


def from_tiles(tiles, at, n):
    chosen = (lanes((LANE, n)) // SUB + at == sublanes((LANE, n))).astype(F32)
    return jnp.sum(jnp.where(own_sublane(n), dot(tiles, chosen), 0.0), axis=0, keepdims=True)


def across(tiles, t):
    return jnp.broadcast_to(tiles[:, t:t + 1], (SUB, LANE))


def reduce_kernel(*refs):
    (gq, go, gu, gd, gv, vrq, vro, vru, vrd, vcq, vco, vcu, vcd, vv,
     hqo, hu, hd, hv, inv_out,
     n_rq, n_ro, n_ru, n_rd, n_cq, n_co, n_cu, n_cd, vv_new,
     own_qo, own_u, own_d, peer_qo, peer_u, peer_d, s_qo,
     a_qo, a_u, a_d, b_qo, b_u, b_d,
     vec_own, vec_in, vec_mid, vv_in,
     r_q, r_o, r_u, r_d, c_q, c_o, c_u, c_d,
     p_q, p_o, cs_qo, cs_u, rs_d, rp_acc, rpd_acc, rp_old, rpd_old, col_buf, rowd_buf,
     cs_all, rp_all, rsd_all, rpd_all, s_all, u_all,
     own_sem, peer_sem, push_sem, first_sem, second_sem, a_sem, b_sem,
     vec_sem, vec_send, vec_recv, small_sem, stat_send, stat_recv, round_sem) = refs

    me = lax.axis_index("fsdp")
    z = lax.axis_index("tp")
    core = lax.rem(me, 2)
    x = lax.rem(me // 2, 2)
    y = me // 4
    linear = z * FSDP + me
    mate = {"fsdp": me + 1 - 2 * core}
    across_x = {"fsdp": me + 2 - 4 * x}
    across_y = {"fsdp": me + 4 - 8 * y}
    every = slice(None)

    def flip(v, bits):
        for bit in range(3):
            step = 2 ** bit
            if bits & step:
                v = v + step - 2 * step * lax.rem(v // step, 2)
        return v

    others = [{"tp": flip(z, a), "fsdp": flip(me, b)} for a in range(TP - 1, -1, -1)
              for b in range(FSDP - 1, -1, -1) if a + b > 0]

    owns, peers = (own_u, own_qo, own_d), (peer_u, peer_qo, peer_d)
    sums, firsts, seconds = (own_u, s_qo, own_d), (a_u, a_qo, a_d), (b_u, b_qo, b_d)

    def send(src, dst, ssem, rsem, to):
        return pltpu.make_async_remote_copy(
            src_ref=src, dst_ref=dst, send_sem=ssem, recv_sem=rsem,
            device_id=to, device_id_type=MESH)

    def index(kind, lead, side, k):
        if kind == QO_:
            return (k,) + lead + (pl.ds(HALF_R * side, HALF_R),)
        if kind == U_:
            return lead + (pl.ds(pl.multiple_of(HALF_R * side + SUB * k, SUB), SUB),)
        return lead + (pl.ds(pl.multiple_of(HALF_DC * side + D_STEP * k, SUB), D_STEP),)

    def whole(kind, lead, side):
        if kind == QO_:
            return (every,) + lead + (pl.ds(HALF_R * side, HALF_R),)
        n = HALF_R if kind == U_ else HALF_DC
        return lead + (pl.ds(n * side, n),)

    def first(kind, side, at, sem):
        lead, to = (((every, 1 - x), across_x), ((1 - y, every), across_y))[side]
        return send(sums[kind].at[at(kind, lead, side)], firsts[kind].at[at(kind, (every,), side)],
                    first_sem.at[kind, side], sem, to)

    def second(kind, side, at, sem):
        lead, to = (((1 - y, x), across_y), ((y, 1 - x), across_x))[side]
        return send(sums[kind].at[at(kind, lead, side)], seconds[kind].at[at(kind, (), side)],
                    second_sem.at[kind, side], sem, to)

    def chunk(k):
        return lambda kind, lead, side: index(kind, lead, side, k)

    def load(kind, k, side, away):
        if away:
            dst, sem, c = peers[kind], peer_sem.at[kind, side, k], 1 - core
            copy = lambda a, b: send(a, b, push_sem.at[kind], sem, mate)
        else:
            dst, sem, c = owns[kind], own_sem.at[kind, side, k], core
            copy = lambda a, b: pltpu.make_async_copy(a, b, sem)
        if kind == U_:
            at = index(kind, (), side, k)
            return [(None, copy(gu.at[(every, every, c) + at], dst.at[(every, every) + at]))]
        if kind == D_:
            at = index(kind, (), side, k)
            return [(None, copy(gd.at[at + (pl.ds(pl.multiple_of(DR * (2 * b + c), LANE), DR),)],
                                dst.at[(b // 2, b % 2) + at])) for b in range(4)]
        slot = dst.at[k if away else lax.rem(k, SLOTS)]
        rest = LANE - Q_LEFT
        at_q = pl.multiple_of(LANE * jnp.minimum(k, Q_FULL - 1), LANE)
        at_o = pl.multiple_of(rest + LANE * jnp.maximum(k - Q_FULL - 1, 0), SUB)
        return [(k < Q_FULL, copy(gq.at[pl.ds(at_q, LANE)], slot)),
                (k == Q_FULL, copy(gq.at[pl.ds(Q_FULL * LANE, Q_LEFT)], slot.at[pl.ds(0, Q_LEFT)])),
                (k == Q_FULL, copy(go.at[pl.ds(0, rest)], slot.at[pl.ds(Q_LEFT, rest)])),
                (k > Q_FULL, copy(go.at[pl.ds(at_o, LANE)], slot))]

    def start_kind(kind, k, away):
        for side in range(1 if kind == QO_ else 2):
            for cond, copy in load(kind, k, side, away):
                if cond is None:
                    copy.start()
                else:
                    pl.when(cond)(copy.start)

    def start_loads(step, away):
        for kind in range(3):
            k = step - kind * STEPS
            pl.when(jnp.logical_and(k >= 0, k < STEPS))(lambda kind=kind, k=k: start_kind(kind, k, away))

    def loaded(kind, side, k):
        if kind == QO_:
            here, there = own_qo.at[lax.rem(k, SLOTS)], peer_qo.at[k]
        else:
            at = index(kind, (every, every), side, k)
            here, there = owns[kind].at[at], peers[kind].at[at]
        pltpu.make_async_copy(here, here, own_sem.at[kind, side, k]).wait()
        send(there, there, push_sem.at[kind], peer_sem.at[kind, side, k], mate).wait_recv()

    smalls = [(vrq, r_q), (vro, r_o), (vru, r_u), (vrd, r_d),
              (vcq, c_q), (vco, c_o), (vcu, c_u), (vcd, c_d), (vv, vv_in)]
    small_copies = [pltpu.make_async_copy(a, b, small_sem.at[i]) for i, (a, b) in enumerate(smalls)]
    vec_copy = pltpu.make_async_copy(gv, vec_own, vec_sem.at[0])

    for step in range(LOOK):
        start_kind(U_, step, False)
    vec_copy.start()
    for copy in small_copies:
        copy.start()
    barrier = pltpu.get_barrier_semaphore()

    def signal(sem, to):
        pl.semaphore_signal(sem, inc=1, device_id=to, device_id_type=MESH)

    def signal_z(sem):
        pl.when(z > 0)(lambda: signal(sem, {"tp": z - 1}))
        pl.when(z < TP - 1)(lambda: signal(sem, {"tp": z + 1}))

    beside = jnp.where(z > 0, 1, 0) + jnp.where(z < TP - 1, 1, 0)
    near = (mate, across_x, across_y)
    for to in near:
        signal(barrier, to)
    signal_z(barrier)
    pl.semaphore_wait(barrier, len(near) + beside)

    for step in range(LOOK):
        start_kind(U_, step, True)
    vec_copy.wait()
    vec_core = send(vec_own, vec_in.at[0], vec_send.at[0], vec_recv.at[0], mate)
    vec_x = send(vec_mid.at[0], vec_in.at[1], vec_send.at[1], vec_recv.at[1], across_x)
    vec_y = send(vec_mid.at[1], vec_in.at[2], vec_send.at[2], vec_recv.at[2], across_y)
    vec_core.start()

    def turn(k, which):
        slot = lax.rem(k, SLOTS)
        for tile in range(STEPS):
            lo = LANE * tile
            cuts = [(b, max(lo, R * (2 * b + which)), min(lo + LANE, R * (2 * b + which) + R)) for b in range(4)]
            cuts = [cut for cut in cuts if cut[1] < cut[2]]
            if cuts:
                at = (every, pl.ds(lo, LANE))
                turned = (own_qo[(slot,) + at] + peer_qo[(k,) + at]).T
                for b, start, stop in cuts:
                    first_row = start - R * (2 * b + which)
                    s_qo[k, b // 2, b % 2, pl.ds(first_row, stop - start), :] = turned[start - lo:stop - lo]

    def stage1(kind):
        def body(k, _):
            start_loads(k + kind * STEPS + LOOK, False)
            start_loads(k + kind * STEPS + LOOK, True)
            if kind == QO_:
                loaded(kind, 0, k)
                for which in range(2):
                    pl.when(core == which)(lambda which=which: turn(k, which))
            for side in range(2):
                if kind != QO_:
                    loaded(kind, side, k)
                    for b in range(4):
                        at = index(kind, (b // 2, b % 2), side, k)
                        owns[kind][at] = owns[kind][at] + peers[kind][at]
                first(kind, side, chunk(k), a_sem.at[kind, side, k]).start()
            return _
        return body

    vec_core.wait_recv()
    vec_mid[0] = vec_own[...] + vec_in[0]
    lax.fori_loop(0, 1, stage1(U_), 0)
    vec_x.start()
    lax.fori_loop(1, STEPS, stage1(U_), 0)
    for kind in (QO_, D_):
        lax.fori_loop(0, STEPS, stage1(kind), 0)

    for copy in small_copies:
        copy.wait()
    for ref in (cs_qo, cs_u, rs_d, rp_acc, rpd_acc, p_q, p_o):
        ref[...] = jnp.zeros_like(ref)
    old = to_tiles(r_q[...], 0) + to_tiles(r_o[...], ROW_TILES) + to_tiles(r_u[...], 2 * ROW_TILES)
    rp_old[...] = old
    rpd_old[...] = to_tiles(c_d[...], 0)
    lane = lanes((SUB, LANE))
    lane1 = lanes((1, LANE))
    masks = [jnp.logical_and(lane >= ROW_TILES * m, lane < ROW_TILES * (m + 1)) for m in range(3)]
    old_sums = [total(jnp.where(masks[m], old, 0.0)) for m in range(3)] + [total(r_d[...])]

    for i, to in enumerate(near):
        signal(round_sem.at[i], to)
        pl.semaphore_wait(round_sem.at[i], 1)
    for i in range(len(near), len(near) + TP - 2):
        signal_z(round_sem.at[i])
        pl.semaphore_wait(round_sem.at[i], beside)

    def stage2(kind):
        def body(k, _):
            for side in range(2):
                first(kind, side, chunk(k), a_sem.at[kind, side, k]).wait_recv()
                lead, mine = (((1 - y, x), 1 - y), ((y, 1 - x), 1 - x))[side]
                at = index(kind, lead, side, k)
                sums[kind][at] = sums[kind][at] + firsts[kind][index(kind, (mine,), side, k)]
                second(kind, side, chunk(k), b_sem.at[kind, side, k]).start()
            return _
        return body

    for kind in (U_, QO_):
        lax.fori_loop(0, STEPS, stage2(kind), 0)
    vec_x.wait_recv()
    vec_mid[1] = vec_mid[0] + vec_in[1]
    vec_y.start()
    lax.fori_loop(0, STEPS, stage2(D_), 0)

    def finished(kind, side, k):
        second(kind, side, chunk(k), b_sem.at[kind, side, k]).wait_recv()
        return (sums[kind][index(kind, (y, x), side, k)]
                + firsts[kind][index(kind, ((y, x)[side],), side, k)]
                + seconds[kind][index(kind, (), side, k)])

    def stage3_u(k, _):
        for side in range(2):
            full = finished(U_, side, k)
            hu[index(U_, (), side, k)] = full
            sq = full * full
            cs_u[...] += sq
            row = jnp.sum(sq, axis=1, keepdims=True)
            rp_acc[...] = jnp.where(lane == 2 * ROW_TILES + STEPS * side + k, row, rp_acc[...])
        return _

    def stage3_qo(k, _):
        for side in range(2):
            rows = pl.ds(HALF_R * side, HALF_R)
            full = finished(QO_, side, k)
            hqo[rows, pl.ds(pl.multiple_of(LANE * k, LANE), LANE)] = full
            sq = full * full
            in_q = lanes(sq.shape) + LANE * k < COLS[0]
            p_q[rows, :] += jnp.where(in_q, sq, 0.0)
            p_o[rows, :] += jnp.where(in_q, 0.0, sq)
            part = sq[:SUB]
            for t in range(1, STEPS):
                part = part + sq[SUB * t:SUB * t + SUB]
            cs_qo[k] += part
        return _

    def stage3_d(k, _):
        for side in range(2):
            full = finished(D_, side, k)
            hd[index(D_, (), side, k)] = full
            sq = full * full
            both = rpd_acc[...]
            for t in range(D_STEP // SUB):
                part = sq[SUB * t:SUB * t + SUB]
                rs_d[...] += part
                col = jnp.sum(part, axis=1, keepdims=True)
                at = (HALF_DC * side + D_STEP * k) // SUB + t
                both = jnp.where(lane == at, col, both)
            rpd_acc[...] = both
        return _

    def to_group(buf, at, i, n, axis, here):
        for d in range(1, n):
            send(buf.at[at], buf.at[at], stat_send.at[i], stat_recv.at[i],
                 {axis: lax.rem(here + d, n)}).start()

    def to_all(buf, i):
        for to in others:
            send(buf.at[linear], buf.at[linear], stat_send.at[i], stat_recv.at[i], to).start()

    def spread(buf, i, n):
        part = buf.at[pl.ds(0, n - 1)]
        return send(part, part, stat_send.at[i], stat_recv.at[i], mate)

    def gathered(buf, i, n):
        spread(buf, i, n).wait_recv()
        out = buf[0]
        for d in range(1, n):
            out = out + buf[d]
        return out

    lax.fori_loop(0, STEPS, stage3_u, 0)
    lax.fori_loop(0, STEPS, stage3_qo, 0)
    vec_y.wait_recv()
    vec = vec_mid[1] + vec_in[2]
    hv[...] = vec
    rp = rp_acc[...]
    for t in range(ROW_TILES):
        for m, ref in enumerate((p_q, p_o)):
            row = jnp.sum(ref[pl.ds(SUB * t, SUB), :], axis=1, keepdims=True)
            rp = jnp.where(lane == ROW_TILES * m + t, row, rp)
    rp_all[z] = rp
    cs = [jnp.sum(cs_qo[k], axis=0, keepdims=True) for k in range(STEPS)]
    cs.append(jnp.sum(cs_u[...], axis=0, keepdims=True))
    cs_all[me] = jnp.concatenate(cs + [jnp.zeros((1, WIDE - QO - UP), F32)], axis=1)
    to_group(rp_all, z, 0, TP, "tp", z)
    to_group(cs_all, me, 1, FSDP, "fsdp", me)
    pack = jnp.where(lane1 == VEC_AT, jnp.sum(vec * vec, axis=1, keepdims=True), 0.0)
    for m in range(4):
        pack = jnp.where(lane1 == VR_AT + m, old_sums[m], pack)
    for m in range(3):
        pack = jnp.where(lane1 == m, total(jnp.where(masks[m], rp, 0.0)), pack)

    lax.fori_loop(0, STEPS, stage3_d, 0)
    rs = rs_d[...]
    s_all[linear] = jnp.where(lane1 == 3, total(rs), pack)
    to_all(s_all, 4)
    rsd_all[z] = jnp.sum(rs, axis=0, keepdims=True)
    to_group(rsd_all, z, 2, TP, "tp", z)
    rpd_all[me] = rpd_acc[...]
    to_group(rpd_all, me, 3, FSDP, "fsdp", me)

    vc_old = jnp.concatenate([c_q[...], c_o[...], c_u[...], jnp.ones((1, WIDE - QO - UP), F32)], axis=1)
    rp = gathered(rp_all, 0, TP)
    cs = gathered(cs_all, 1, FSDP)
    rsd = gathered(rsd_all, 2, TP)
    rpd = gathered(rpd_all, 3, FSDP)
    pack = gathered(s_all, 4, DEVICES)
    squares = [pick(pack, m) for m in range(4)]
    norm = jnp.sqrt((squares[0] + squares[1]) + (squares[2] + squares[3]) + pick(pack, VEC_AT) / FSDP)
    clip = jnp.minimum(1.0, 1.0 / norm)

    def clipped(v):
        return jnp.where(clip > 0.0, (v * clip) * clip, 0.0)

    means = []
    for m in range(4):
        r_all, c_all = float(ROWS[m] * FSDP), float(COLS[m] * TP)
        means.append(KEEP * (pick(pack, VR_AT + m) / (TP * r_all))
                     + MIX * (clipped(squares[m]) / (r_all * c_all) + EPSILON))
    mean_rp = jnp.where(masks[0], means[0], jnp.where(masks[1], means[1], means[2]))
    wide = jnp.where(masks[0], float(COLS[0] * TP), jnp.where(masks[1], float(COLS[1] * TP), float(COLS[2] * TP)))
    row_new = KEEP * rp_old[...] + MIX * (clipped(rp) / wide + EPSILON)
    row_sq = mean_rp / row_new
    rowd_new = KEEP * r_d[...] + MIX * (clipped(rsd) / float(DC * TP) + EPSILON)
    rowd_buf[...] = clip * jnp.sqrt(means[3] / rowd_new)
    col_new = KEEP * vc_old + MIX * (clipped(cs) / float(R * FSDP) + EPSILON)
    col_buf[...] = clip / jnp.sqrt(col_new)
    cold_new = KEEP * rpd_old[...] + MIX * (clipped(rpd) / float(DR * FSDP) + EPSILON)
    cold_sq = 1.0 / cold_new

    def tile(ref, j):
        return jnp.broadcast_to(ref[:, pl.ds(LANE * j, LANE)], (SUB, LANE))

    zero = jnp.zeros((SUB, LANE), F32)
    acc = [zero] * 4
    in_q = lane < Q_LEFT
    col_t = [tile(col_buf, j) for j in range(STEPS + UP // LANE)]
    for t in range(ROW_TILES):
        rows = pl.ds(SUB * t, SUB)
        part = [zero] * 3
        for j in range(STEPS):
            u = hqo[rows, pl.ds(LANE * j, LANE)] * col_t[j]
            u = u * u
            if j == Q_FULL:
                part[0] = part[0] + jnp.where(in_q, u, 0.0)
                part[1] = part[1] + jnp.where(in_q, 0.0, u)
            else:
                part[j // Q_FULL] = part[j // Q_FULL] + u
        for j in range(UP // LANE):
            u = hu[rows, pl.ds(LANE * j, LANE)] * col_t[STEPS + j]
            part[2] = part[2] + u * u
        for m in range(3):
            acc[m] = acc[m] + part[m] * across(row_sq, ROW_TILES * m + t)
    rowd_t = [tile(rowd_buf, j) for j in range(DR // LANE)]
    for t in range(D_TILES):
        part = zero
        for j in range(DR // LANE):
            u = hd[pl.ds(SUB * t, SUB), pl.ds(LANE * j, LANE)] * rowd_t[j]
            part = part + u * u
        acc[3] = acc[3] + part * across(cold_sq, t)
    vec = hv[...] * clip
    v_new = KEEP * vv_in[...] + MIX * (vec * vec + EPSILON)
    vec = vec / jnp.sqrt(v_new)
    pack = jnp.where(lane1 == VEC_AT, jnp.sum(vec * vec, axis=1, keepdims=True), 0.0)
    for m in range(4):
        pack = jnp.where(lane1 == m, total(acc[m]), pack)
    u_all[linear] = pack
    to_all(u_all, 5)

    vv_new[...] = v_new
    hv[...] = vec
    row = jnp.sqrt(row_sq)
    cold = jnp.sqrt(cold_sq)
    for t in range(ROW_TILES):
        rows = pl.ds(SUB * t, SUB)
        scale = [across(row, ROW_TILES * m + t) for m in range(3)]
        mixed = jnp.where(in_q, scale[0], scale[1])
        for j in range(STEPS):
            at = pl.ds(LANE * j, LANE)
            hqo[rows, at] = hqo[rows, at] * col_t[j] * (mixed if j == Q_FULL else scale[j // Q_FULL])
        for j in range(UP // LANE):
            at = pl.ds(LANE * j, LANE)
            hu[rows, at] = hu[rows, at] * col_t[STEPS + j] * scale[2]
    for t in range(D_TILES):
        rows = pl.ds(SUB * t, SUB)
        scale = across(cold, t)
        for j in range(DR // LANE):
            at = pl.ds(LANE * j, LANE)
            hd[rows, at] = hd[rows, at] * rowd_t[j] * scale
    for m, ref in enumerate((n_rq, n_ro, n_ru)):
        ref[...] = from_tiles(row_new, ROW_TILES * m, R)
    n_rd[...] = rowd_new
    n_cq[...] = col_new[:, :COLS[0]]
    n_co[...] = col_new[:, COLS[0]:QO]
    n_cu[...] = col_new[:, QO:QO + UP]
    n_cd[...] = from_tiles(cold_new, 0, DC)

    for kind in range(3):
        send(peers[kind], peers[kind], push_sem.at[kind], peer_sem.at[kind, 0, 0], mate).wait_send()
        for side in range(2):
            first(kind, side, whole, a_sem.at[kind, side, 0]).wait_send()
            second(kind, side, whole, b_sem.at[kind, side, 0]).wait_send()
    for copy in (vec_core, vec_x, vec_y):
        copy.wait_send()
    groups = ((rp_all, TP), (cs_all, FSDP), (rsd_all, TP), (rpd_all, FSDP), (s_all, DEVICES), (u_all, DEVICES))
    for i, (buf, n) in enumerate(groups):
        if i < len(groups) - 1:
            spread(buf, i, n).wait_send()

    pack = gathered(u_all, len(groups) - 1, DEVICES)
    count = jnp.full((1, LANE), float(VEC * TP * FSDP), F32)
    for m in range(4):
        count = jnp.where(lane1 == m, float(ROWS[m] * FSDP * COLS[m] * TP), count)
    inv_out[...] = 1.0 / jnp.maximum(1.0, jnp.sqrt(pack / count))
    spread(u_all, len(groups) - 1, DEVICES).wait_send()


PIECES = ((3, 0, HALF_DC), (3, HALF_DC, HALF_DC), (2, 0, R), (0, 0, R), (1, 0, R))
HELD = (ROWS[:3] + (DC,), COLS[:3] + (DR,))
GROUP = 16


def update_kernel(*refs):
    (hqo, hu, hd, hv, inv, vrq, vro, vru, vrd, vcq, vco, vcu, vcd, vv,
     wq, wo, wu, wd, wv, mq, mo, mu, md, mv,
     wq_out, wo_out, wu_out, wd_out, wv_out, mq_out, mo_out, mu_out, md_out, mv_out,
     vrq_out, vcq_out, vro_out, vco_out, vru_out, vcu_out, vrd_out, vcd_out, vv_out,
     bwq, bwo, bwu, bwd, bmq, bmo, bmu, bmd, bwv, bmv, out_sem, small_sem) = refs
    held = ((hqo, 0), (hqo, COLS[0]), (hu, 0), (hd, 0))
    w_in, m_in = (wq, wo, wu, wd), (mq, mo, mu, md)
    w_buf, m_buf = (bwq, bwo, bwu, bwd), (bmq, bmo, bmu, bmd)
    w_out, m_out = (wq_out, wo_out, wu_out, wd_out), (mq_out, mo_out, mu_out, md_out)

    def finish(u, w, m):
        m_new = (MOMENTUM * m.astype(F32) + (1.0 - MOMENTUM) * u).astype(BF16)
        return w - LEARN_RATE * (m_new.astype(F32) + WEIGHT_DECAY * w), m_new

    passed = ((vrq, vrq_out), (vro, vro_out), (vru, vru_out), (vrd, vrd_out),
              (vcq, vcq_out), (vco, vco_out), (vcu, vcu_out), (vcd, vcd_out), (vv, vv_out))
    stores = [pltpu.make_async_copy(src, dst, small_sem.at[i]) for i, (src, dst) in enumerate(passed)]
    w_new, m_new = finish(hv[...] * inv[:, VEC_AT:VEC_AT + 1], wv[...], mv[...])
    bwv[...] = w_new
    bmv[...] = m_new
    stores.append(pltpu.make_async_copy(bwv, wv_out, small_sem.at[len(passed)]))
    stores.append(pltpu.make_async_copy(bmv, mv_out, small_sem.at[len(passed) + 1]))
    for copy in stores:
        copy.start()
    for i, (m, r0, n) in enumerate(PIECES):
        scale = inv[:, m:m + 1]
        buf, c0 = held[m]

        for k in range(n // GROUP):
            rows = pl.ds(r0 + GROUP * k, GROUP)
            u = buf[rows, pl.ds(c0 // LANE * LANE, c0 % LANE + HELD[1][m])][:, c0 % LANE:]
            w_new, m_new = finish(u * scale, w_in[m][rows, :], m_in[m][rows, :])
            w_buf[m][rows, :] = w_new
            m_buf[m][rows, :] = m_new
        rows = pl.ds(r0, n)
        for j, (src, dst) in enumerate(((w_buf, w_out), (m_buf, m_out))):
            stores.append(pltpu.make_async_copy(src[m].at[rows, :], dst[m].at[rows, :], out_sem.at[i, j]))
            stores[-1].start()
    for copy in stores:
        copy.wait()


IN_HBM = pl.BlockSpec(memory_space=pltpu.HBM)
IN_VMEM = pl.BlockSpec(memory_space=pltpu.VMEM)
MIB = 1024 * 1024


def f32(*shape):
    return jax.ShapeDtypeStruct(shape, F32)


def vmem(*shape):
    return pltpu.VMEM(shape, F32)


def local_step(g_qkv, g_out, g_up, g_down, g_vec, w_qkv, w_out, w_up, w_down, w_vec,
               m_qkv, m_out, m_up, m_down, m_vec, vr_qkv, vc_qkv, vr_out, vc_out,
               vr_up, vc_up, vr_down, vc_down, v_vec):
    dma = pltpu.SemaphoreType.DMA
    rows_shapes = [(1, n) for n in ROWS]
    cols_shapes = [(1, n) for n in COLS]
    h_shapes = [(R, QO), (R, UP), (DC, DR)]
    wide_u, wide_d, vec = (R, UP), (DC, DR), (1, VEC)
    shapes = [
        (SLOTS, LANE, QO), (2, 2) + wide_u, (2, 2) + wide_d,
        (STEPS, LANE, QO), (2, 2) + wide_u, (2, 2) + wide_d, (STEPS, 2, 2, R, LANE),
        (STEPS, 2, R, LANE), (2,) + wide_u, (2,) + wide_d, (STEPS, R, LANE), wide_u, wide_d,
        vec, (3,) + vec, (2,) + vec, vec] + rows_shapes + cols_shapes + [
        (R, LANE), (R, LANE), (STEPS, SUB, LANE), (SUB, UP), (SUB, DR)] + [(SUB, LANE)] * 4 + [
        (1, WIDE), (1, DR),
        (FSDP, 1, WIDE), (TP, SUB, LANE), (TP, 1, DR), (FSDP, SUB, LANE),
        (DEVICES, 1, LANE), (DEVICES, 1, LANE)]
    sems = [(3, 2, STEPS)] * 2 + [(3,), (3, 2), (3, 2)] + [(3, 2, STEPS)] * 2 + [(1,), (3,), (3,), (9,), (6,), (6,)]
    inputs = [pltpu.with_memory_space_constraint(a, pltpu.HBM)
              for a in (g_qkv[0, 0].T, g_out[0, 0].T, g_up.reshape(2, 2, 2, R, UP), g_down[0, 0].T, g_vec[0],
                        vr_qkv, vr_out, vr_up, vr_down, vc_qkv, vc_out, vc_up, vc_down, v_vec)]
    reduced = pl.pallas_call(
        reduce_kernel,
        name="reduce_and_scale",
        out_shape=[f32(*s) for s in h_shapes + [vec, (1, LANE)] + rows_shapes + cols_shapes + [vec]],
        in_specs=[IN_HBM] * 14,
        out_specs=[IN_VMEM] * 14,
        scratch_shapes=[vmem(*s) for s in shapes] + [dma(s) for s in sems] + [pltpu.SemaphoreType.REGULAR((TP + 1,))],
        compiler_params=pltpu.CompilerParams(
            collective_id=0, has_side_effects=True, vmem_limit_bytes=A_MIB * MIB),
    )(*inputs)

    ws = [w_qkv[0], w_out[0], w_up[0], w_down[0].T, w_vec]
    ms = [m_qkv[0], m_out[0], m_up[0], m_down[0].T, m_vec]
    mats = list(zip(*HELD))
    outs = pl.pallas_call(
        update_kernel,
        name="update",
        out_shape=([f32(*s) for s in mats + [vec]] + [jax.ShapeDtypeStruct(s, BF16) for s in mats + [vec]]
                   + [f32(*s) for m in range(4) for s in (rows_shapes[m], cols_shapes[m])] + [f32(*vec)]),
        in_specs=[IN_VMEM] * 24,
        out_specs=[IN_HBM] * 19,
        scratch_shapes=([vmem(*s) for s in mats] + [pltpu.VMEM(s, BF16) for s in mats]
                        + [vmem(*vec), pltpu.VMEM(vec, BF16), dma((len(PIECES), 2)), dma((11,))]),
        compiler_params=pltpu.CompilerParams(vmem_limit_bytes=B_MIB * MIB),
    )(*reduced, *ws, *ms)
    outs = list(outs)
    for i in range(10):
        if i % 5 == 3:
            outs[i] = outs[i].T
        if i % 5 != 4:
            outs[i] = outs[i][None]
    return tuple(outs)


A_MIB, B_MIB = 46, 12


def solution(mesh):
    grad_spec = P("fsdp", None, None, "tp")
    vec_grad_spec = P("fsdp", None, "tp")
    mat_spec = P(None, "fsdp", "tp")
    vec_spec = P(None, "tp")
    row_spec = P(None, "fsdp")
    col_spec = P(None, "tp")
    state_specs = ((mat_spec,) * 4 + (vec_spec,) + (mat_spec,) * 4 + (vec_spec,)
                   + (row_spec, col_spec) * 4 + (vec_spec,))
    arg_specs = (grad_spec,) * 4 + (vec_grad_spec,) + state_specs
    return jax.shard_map(local_step, mesh=mesh, in_specs=arg_specs, out_specs=state_specs, check_vma=False)
```

```python
import jax
import jax.numpy as jnp
from jax import lax
from jax.experimental import pallas as pl
from jax.experimental.pallas import tpu as pltpu
from jax.sharding import PartitionSpec as P

TRAIN_STEP = 3
LEARN_RATE = 0.0008
WEIGHT_DECAY = 0.03
MOMENTUM = 0.9
EPSILON = 1e-30
BETA_TWO = 1.0 - TRAIN_STEP ** -0.8
KEEP, MIX = BETA_TWO, 1.0 - BETA_TWO

F32 = jnp.float32
BF16 = jnp.bfloat16
MESH = pl.DeviceIdType.MESH
HIGHEST = lax.Precision.HIGHEST
TP, FSDP, DEVICES = 4, 8, 32
SUB, LANE = 8, 128

ROWS = (176, 176, 176, 768)
COLS = (1056, 352, 1536, 352)
VEC = 4704
R, QO, UP, DR, DC = ROWS[0], COLS[0] + COLS[1], COLS[2], ROWS[3], COLS[3]
HALF_R, HALF_DC = R // 2, DC // 2
STEPS = QO // LANE
D_STEP = HALF_DC // STEPS
Q_FULL = COLS[0] // LANE
Q_LEFT = COLS[0] - Q_FULL * LANE
ROW_TILES = R // SUB
D_TILES = DC // SUB
WIDE = -(-(QO + UP) // (SUB * LANE)) * SUB * LANE
LOOK, SLOTS = 3, 4
OPENING = ((1,), (2, 3))
U_, QO_, D_ = 0, 1, 2
VR_AT, VEC_AT = 4, 8


def lanes(shape):
    return lax.broadcasted_iota(jnp.int32, shape, len(shape) - 1)


def sublanes(shape):
    return lax.broadcasted_iota(jnp.int32, shape, len(shape) - 2)


def total(x):
    return jnp.sum(jnp.sum(x, axis=1, keepdims=True), axis=0, keepdims=True)


def pick(x, lane):
    return jnp.sum(jnp.where(lanes(x.shape) == lane, x, 0.0), axis=1, keepdims=True)


def dot(a, b):
    return lax.dot_general(a, b, (((1,), (0,)), ((), ())), precision=HIGHEST, preferred_element_type=F32)


def own_sublane(n):
    return lanes((SUB, n)) % SUB == sublanes((SUB, n))


def to_tiles(row, at):
    n = row.shape[1]
    chosen = (sublanes((n, LANE)) // SUB + at == lanes((n, LANE))).astype(F32)
    return dot(jnp.where(own_sublane(n), row, 0.0), chosen)


def from_tiles(tiles, at, n):
    chosen = (lanes((LANE, n)) // SUB + at == sublanes((LANE, n))).astype(F32)
    return jnp.sum(jnp.where(own_sublane(n), dot(tiles, chosen), 0.0), axis=0, keepdims=True)


def across(tiles, t):
    return jnp.broadcast_to(tiles[:, t:t + 1], (SUB, LANE))


def reduce_kernel(*refs):
    (gq, go, gu, gd, gv, vrq, vro, vru, vrd, vcq, vco, vcu, vcd, vv,
     hqo, hu, hd, hv, inv_out,
     n_rq, n_ro, n_ru, n_rd, n_cq, n_co, n_cu, n_cd, vv_new,
     stage, own_qo, own_u, own_d, peer_qo, peer_u, peer_d, s_qo,
     a_qo, a_u, a_d, b_qo, b_u, b_d,
     vec_own, vec_in, vec_mid, vv_in,
     r_q, r_o, r_u, r_d, c_q, c_o, c_u, c_d,
     p_q, p_o, cs_qo, cs_u, rs_d, rp_acc, rpd_acc, rp_old, rpd_old, col_buf, rowd_buf,
     cs_all, rp_all, rsd_all, rpd_all, s_all, u_all,
     own_sem, peer_sem, push_sem, first_sem, second_sem, a_sem, b_sem,
     vec_sem, vec_send, vec_recv, small_sem, stat_send, stat_recv, stage_sem, round_sem) = refs

    me = lax.axis_index("fsdp")
    z = lax.axis_index("tp")
    core = lax.rem(me, 2)
    x = lax.rem(me // 2, 2)
    y = me // 4
    linear = z * FSDP + me
    mate = {"fsdp": me + 1 - 2 * core}
    across_x = {"fsdp": me + 2 - 4 * x}
    across_y = {"fsdp": me + 4 - 8 * y}
    every = slice(None)

    def flip(v, bits):
        for bit in range(3):
            step = 2 ** bit
            if bits & step:
                v = v + step - 2 * step * lax.rem(v // step, 2)
        return v

    others = [{"tp": flip(z, a), "fsdp": flip(me, b)} for a in range(TP - 1, -1, -1)
              for b in range(FSDP - 1, -1, -1) if a + b > 0]

    owns, peers = (own_u, own_qo, own_d), (peer_u, peer_qo, peer_d)
    sums, firsts, seconds = (own_u, s_qo, own_d), (a_u, a_qo, a_d), (b_u, b_qo, b_d)

    def send(src, dst, ssem, rsem, to):
        return pltpu.make_async_remote_copy(
            src_ref=src, dst_ref=dst, send_sem=ssem, recv_sem=rsem,
            device_id=to, device_id_type=MESH)

    def index(kind, lead, side, k):
        if kind == QO_:
            return (k,) + lead + (pl.ds(HALF_R * side, HALF_R),)
        if kind == U_:
            return lead + (pl.ds(pl.multiple_of(HALF_R * side + SUB * k, SUB), SUB),)
        return lead + (pl.ds(pl.multiple_of(HALF_DC * side + D_STEP * k, SUB), D_STEP),)

    def whole(kind, lead, side):
        if kind == QO_:
            return (every,) + lead + (pl.ds(HALF_R * side, HALF_R),)
        n = HALF_R if kind == U_ else HALF_DC
        return lead + (pl.ds(n * side, n),)

    def first(kind, side, at, sem):
        lead, to = (((every, 1 - x), across_x), ((1 - y, every), across_y))[side]
        return send(sums[kind].at[at(kind, lead, side)], firsts[kind].at[at(kind, (every,), side)],
                    first_sem.at[kind, side], sem, to)

    def second(kind, side, at, sem):
        lead, to = (((1 - y, x), across_y), ((y, 1 - x), across_x))[side]
        return send(sums[kind].at[at(kind, lead, side)], seconds[kind].at[at(kind, (), side)],
                    second_sem.at[kind, side], sem, to)

    def chunk(k):
        return lambda kind, lead, side: index(kind, lead, side, k)

    def load(kind, k, side, away):
        if away:
            dst, sem, c = peers[kind], peer_sem.at[kind, side, k], 1 - core
            copy = lambda a, b: send(a, b, push_sem.at[kind], sem, mate)
        else:
            dst, sem, c = owns[kind], own_sem.at[kind, side, k], core
            copy = lambda a, b: pltpu.make_async_copy(a, b, sem)
        if kind == U_:
            at = index(kind, (), side, k)
            return [(None, copy(gu.at[(every, every, c) + at], dst.at[(every, every) + at]))]
        if kind == D_:
            at = index(kind, (), side, k)
            return [(None, copy(gd.at[at + (pl.ds(pl.multiple_of(DR * (2 * b + c), LANE), DR),)],
                                dst.at[(b // 2, b % 2) + at])) for b in range(4)]
        slot = dst.at[k if away else lax.rem(k, SLOTS)]
        rest = LANE - Q_LEFT
        at_q = pl.multiple_of(LANE * jnp.minimum(k, Q_FULL - 1), LANE)
        at_o = pl.multiple_of(rest + LANE * jnp.maximum(k - Q_FULL - 1, 0), SUB)
        return [(k < Q_FULL, copy(gq.at[pl.ds(at_q, LANE)], slot)),
                (k == Q_FULL, copy(gq.at[pl.ds(Q_FULL * LANE, Q_LEFT)], slot.at[pl.ds(0, Q_LEFT)])),
                (k == Q_FULL, copy(go.at[pl.ds(0, rest)], slot.at[pl.ds(Q_LEFT, rest)])),
                (k > Q_FULL, copy(go.at[pl.ds(at_o, LANE)], slot))]

    def start_kind(kind, k, away):
        for side in range(1 if kind == QO_ else 2):
            for cond, copy in load(kind, k, side, away):
                if cond is None:
                    copy.start()
                else:
                    pl.when(cond)(copy.start)

    def start_loads(step, away):
        for kind in range(3):
            k = step - kind * STEPS
            pl.when(jnp.logical_and(k >= 0, k < STEPS))(lambda kind=kind, k=k: start_kind(kind, k, away))

    def loaded(kind, side, k):
        if kind == QO_:
            here, there = own_qo.at[lax.rem(k, SLOTS)], peer_qo.at[k]
        else:
            at = index(kind, (every, every), side, k)
            here, there = owns[kind].at[at], peers[kind].at[at]
        pltpu.make_async_copy(here, here, own_sem.at[kind, side, k]).wait()
        send(there, there, push_sem.at[kind], peer_sem.at[kind, side, k], mate).wait_recv()

    smalls = [(vrq, r_q), (vro, r_o), (vru, r_u), (vrd, r_d),
              (vcq, c_q), (vco, c_o), (vcu, c_u), (vcd, c_d), (vv, vv_in)]
    small_copies = [pltpu.make_async_copy(a, b, small_sem.at[i]) for i, (a, b) in enumerate(smalls)]
    vec_copy = pltpu.make_async_copy(gv, vec_own, vec_sem.at[0])

    staged = [pltpu.make_async_copy(gu.at[(every, every, 1 - core) + index(U_, (), side, 0)],
                                    stage.at[side], stage_sem.at[side]) for side in range(2)]
    for copy in staged:
        copy.start()
    start_kind(U_, 0, False)
    barrier = pltpu.get_barrier_semaphore()

    def signal(sem, to):
        pl.semaphore_signal(sem, inc=1, device_id=to, device_id_type=MESH)

    def signal_z(sem):
        pl.when(z > 0)(lambda: signal(sem, {"tp": z - 1}))
        pl.when(z < TP - 1)(lambda: signal(sem, {"tp": z + 1}))

    beside = jnp.where(z > 0, 1, 0) + jnp.where(z < TP - 1, 1, 0)
    near = (mate, across_x, across_y)
    for to in near:
        signal(barrier, to)
    signal_z(barrier)
    pl.semaphore_wait(barrier, len(near) + beside)

    for side in range(2):
        staged[side].wait()
        send(stage.at[side], peer_u.at[index(U_, (every, every), side, 0)],
             push_sem.at[U_], peer_sem.at[U_, side, 0], mate).start()
    vec_copy.start()
    for copy in small_copies:
        copy.start()
    vec_core = send(vec_own, vec_in.at[0], vec_send.at[0], vec_recv.at[0], mate)
    vec_x = send(vec_mid.at[0], vec_in.at[1], vec_send.at[1], vec_recv.at[1], across_x)
    vec_y = send(vec_mid.at[1], vec_in.at[2], vec_send.at[2], vec_recv.at[2], across_y)

    def turn(k, which):
        slot = lax.rem(k, SLOTS)
        for tile in range(STEPS):
            lo = LANE * tile
            cuts = [(b, max(lo, R * (2 * b + which)), min(lo + LANE, R * (2 * b + which) + R)) for b in range(4)]
            cuts = [cut for cut in cuts if cut[1] < cut[2]]
            if cuts:
                at = (every, pl.ds(lo, LANE))
                turned = (own_qo[(slot,) + at] + peer_qo[(k,) + at]).T
                for b, start, stop in cuts:
                    first_row = start - R * (2 * b + which)
                    s_qo[k, b // 2, b % 2, pl.ds(first_row, stop - start), :] = turned[start - lo:stop - lo]

    def stage1(kind, opening=False):
        def body(k, _):
            if not opening:
                start_loads(k + kind * STEPS + LOOK, False)
                start_loads(k + kind * STEPS + LOOK, True)
            if kind == QO_:
                loaded(kind, 0, k)
                for which in range(2):
                    pl.when(core == which)(lambda which=which: turn(k, which))
            for side in range(2):
                if kind != QO_:
                    loaded(kind, side, k)
                    for b in range(4):
                        at = index(kind, (b // 2, b % 2), side, k)
                        owns[kind][at] = owns[kind][at] + peers[kind][at]
                first(kind, side, chunk(k), a_sem.at[kind, side, k]).start()
                if opening:
                    for step in OPENING[side]:
                        start_kind(U_, step, False)
                        start_kind(U_, step, True)
            return _
        return body

    stage1(U_, True)(0, 0)
    vec_copy.wait()
    vec_core.start()
    lax.fori_loop(1, STEPS, stage1(U_), 0)
    vec_core.wait_recv()
    vec_mid[0] = vec_own[...] + vec_in[0]
    vec_x.start()
    for kind in (QO_, D_):
        lax.fori_loop(0, STEPS, stage1(kind), 0)

    for copy in small_copies:
        copy.wait()
    for ref in (cs_qo, cs_u, rs_d, rp_acc, rpd_acc, p_q, p_o):
        ref[...] = jnp.zeros_like(ref)
    old = to_tiles(r_q[...], 0) + to_tiles(r_o[...], ROW_TILES) + to_tiles(r_u[...], 2 * ROW_TILES)
    rp_old[...] = old
    rpd_old[...] = to_tiles(c_d[...], 0)
    lane = lanes((SUB, LANE))
    lane1 = lanes((1, LANE))
    masks = [jnp.logical_and(lane >= ROW_TILES * m, lane < ROW_TILES * (m + 1)) for m in range(3)]
    old_sums = [total(jnp.where(masks[m], old, 0.0)) for m in range(3)] + [total(r_d[...])]

    for i, to in enumerate(near):
        signal(round_sem.at[i], to)
        pl.semaphore_wait(round_sem.at[i], 1)
    for i in range(len(near), len(near) + TP - 2):
        signal_z(round_sem.at[i])
        pl.semaphore_wait(round_sem.at[i], beside)

    def stage2(kind):
        def body(k, _):
            for side in range(2):
                first(kind, side, chunk(k), a_sem.at[kind, side, k]).wait_recv()
                lead, mine = (((1 - y, x), 1 - y), ((y, 1 - x), 1 - x))[side]
                at = index(kind, lead, side, k)
                sums[kind][at] = sums[kind][at] + firsts[kind][index(kind, (mine,), side, k)]
                second(kind, side, chunk(k), b_sem.at[kind, side, k]).start()
            return _
        return body

    for kind in (U_, QO_):
        lax.fori_loop(0, STEPS, stage2(kind), 0)
    vec_x.wait_recv()
    vec_mid[1] = vec_mid[0] + vec_in[1]
    vec_y.start()
    lax.fori_loop(0, STEPS, stage2(D_), 0)

    def finished(kind, side, k):
        second(kind, side, chunk(k), b_sem.at[kind, side, k]).wait_recv()
        return (sums[kind][index(kind, (y, x), side, k)]
                + firsts[kind][index(kind, ((y, x)[side],), side, k)]
                + seconds[kind][index(kind, (), side, k)])

    def stage3_u(k, _):
        for side in range(2):
            full = finished(U_, side, k)
            hu[index(U_, (), side, k)] = full
            sq = full * full
            cs_u[...] += sq
            row = jnp.sum(sq, axis=1, keepdims=True)
            rp_acc[...] = jnp.where(lane == 2 * ROW_TILES + STEPS * side + k, row, rp_acc[...])
        return _

    def stage3_qo(k, _):
        for side in range(2):
            rows = pl.ds(HALF_R * side, HALF_R)
            full = finished(QO_, side, k)
            hqo[rows, pl.ds(pl.multiple_of(LANE * k, LANE), LANE)] = full
            sq = full * full
            in_q = lanes(sq.shape) + LANE * k < COLS[0]
            p_q[rows, :] += jnp.where(in_q, sq, 0.0)
            p_o[rows, :] += jnp.where(in_q, 0.0, sq)
            part = sq[:SUB]
            for t in range(1, STEPS):
                part = part + sq[SUB * t:SUB * t + SUB]
            cs_qo[k] += part
        return _

    def stage3_d(k, _):
        for side in range(2):
            full = finished(D_, side, k)
            hd[index(D_, (), side, k)] = full
            sq = full * full
            both = rpd_acc[...]
            for t in range(D_STEP // SUB):
                part = sq[SUB * t:SUB * t + SUB]
                rs_d[...] += part
                col = jnp.sum(part, axis=1, keepdims=True)
                at = (HALF_DC * side + D_STEP * k) // SUB + t
                both = jnp.where(lane == at, col, both)
            rpd_acc[...] = both
        return _

    def to_group(buf, at, i, n, axis, here):
        for d in range(1, n):
            send(buf.at[at], buf.at[at], stat_send.at[i], stat_recv.at[i],
                 {axis: lax.rem(here + d, n)}).start()

    def to_all(buf, i):
        for to in others:
            send(buf.at[linear], buf.at[linear], stat_send.at[i], stat_recv.at[i], to).start()

    def spread(buf, i, n):
        part = buf.at[pl.ds(0, n - 1)]
        return send(part, part, stat_send.at[i], stat_recv.at[i], mate)

    def gathered(buf, i, n):
        spread(buf, i, n).wait_recv()
        out = buf[0]
        for d in range(1, n):
            out = out + buf[d]
        return out

    lax.fori_loop(0, STEPS, stage3_u, 0)
    lax.fori_loop(0, STEPS, stage3_qo, 0)
    vec_y.wait_recv()
    vec = vec_mid[1] + vec_in[2]
    hv[...] = vec
    rp = rp_acc[...]
    for t in range(ROW_TILES):
        for m, ref in enumerate((p_q, p_o)):
            row = jnp.sum(ref[pl.ds(SUB * t, SUB), :], axis=1, keepdims=True)
            rp = jnp.where(lane == ROW_TILES * m + t, row, rp)
    rp_all[z] = rp
    cs = [jnp.sum(cs_qo[k], axis=0, keepdims=True) for k in range(STEPS)]
    cs.append(jnp.sum(cs_u[...], axis=0, keepdims=True))
    cs_all[me] = jnp.concatenate(cs + [jnp.zeros((1, WIDE - QO - UP), F32)], axis=1)
    to_group(rp_all, z, 0, TP, "tp", z)
    to_group(cs_all, me, 1, FSDP, "fsdp", me)
    pack = jnp.where(lane1 == VEC_AT, jnp.sum(vec * vec, axis=1, keepdims=True), 0.0)
    for m in range(4):
        pack = jnp.where(lane1 == VR_AT + m, old_sums[m], pack)
    for m in range(3):
        pack = jnp.where(lane1 == m, total(jnp.where(masks[m], rp, 0.0)), pack)

    lax.fori_loop(0, STEPS, stage3_d, 0)
    rs = rs_d[...]
    s_all[linear] = jnp.where(lane1 == 3, total(rs), pack)
    to_all(s_all, 4)
    rsd_all[z] = jnp.sum(rs, axis=0, keepdims=True)
    to_group(rsd_all, z, 2, TP, "tp", z)
    rpd_all[me] = rpd_acc[...]
    to_group(rpd_all, me, 3, FSDP, "fsdp", me)

    vc_old = jnp.concatenate([c_q[...], c_o[...], c_u[...], jnp.ones((1, WIDE - QO - UP), F32)], axis=1)
    rp = gathered(rp_all, 0, TP)
    cs = gathered(cs_all, 1, FSDP)
    rsd = gathered(rsd_all, 2, TP)
    rpd = gathered(rpd_all, 3, FSDP)
    pack = gathered(s_all, 4, DEVICES)
    squares = [pick(pack, m) for m in range(4)]
    norm = jnp.sqrt((squares[0] + squares[1]) + (squares[2] + squares[3]) + pick(pack, VEC_AT) / FSDP)
    clip = jnp.minimum(1.0, 1.0 / norm)

    def clipped(v):
        return jnp.where(clip > 0.0, (v * clip) * clip, 0.0)

    means = []
    for m in range(4):
        r_all, c_all = float(ROWS[m] * FSDP), float(COLS[m] * TP)
        means.append(KEEP * (pick(pack, VR_AT + m) / (TP * r_all))
                     + MIX * (clipped(squares[m]) / (r_all * c_all) + EPSILON))
    mean_rp = jnp.where(masks[0], means[0], jnp.where(masks[1], means[1], means[2]))
    wide = jnp.where(masks[0], float(COLS[0] * TP), jnp.where(masks[1], float(COLS[1] * TP), float(COLS[2] * TP)))
    row_new = KEEP * rp_old[...] + MIX * (clipped(rp) / wide + EPSILON)
    row_sq = mean_rp / row_new
    rowd_new = KEEP * r_d[...] + MIX * (clipped(rsd) / float(DC * TP) + EPSILON)
    rowd_buf[...] = clip * jnp.sqrt(means[3] / rowd_new)
    col_new = KEEP * vc_old + MIX * (clipped(cs) / float(R * FSDP) + EPSILON)
    col_buf[...] = clip / jnp.sqrt(col_new)
    cold_new = KEEP * rpd_old[...] + MIX * (clipped(rpd) / float(DR * FSDP) + EPSILON)
    cold_sq = 1.0 / cold_new

    def tile(ref, j):
        return jnp.broadcast_to(ref[:, pl.ds(LANE * j, LANE)], (SUB, LANE))

    zero = jnp.zeros((SUB, LANE), F32)
    acc = [zero] * 4
    in_q = lane < Q_LEFT
    col_t = [tile(col_buf, j) for j in range(STEPS + UP // LANE)]
    for t in range(ROW_TILES):
        rows = pl.ds(SUB * t, SUB)
        part = [zero] * 3
        for j in range(STEPS):
            u = hqo[rows, pl.ds(LANE * j, LANE)] * col_t[j]
            u = u * u
            if j == Q_FULL:
                part[0] = part[0] + jnp.where(in_q, u, 0.0)
                part[1] = part[1] + jnp.where(in_q, 0.0, u)
            else:
                part[j // Q_FULL] = part[j // Q_FULL] + u
        for j in range(UP // LANE):
            u = hu[rows, pl.ds(LANE * j, LANE)] * col_t[STEPS + j]
            part[2] = part[2] + u * u
        for m in range(3):
            acc[m] = acc[m] + part[m] * across(row_sq, ROW_TILES * m + t)
    rowd_t = [tile(rowd_buf, j) for j in range(DR // LANE)]
    for t in range(D_TILES):
        part = zero
        for j in range(DR // LANE):
            u = hd[pl.ds(SUB * t, SUB), pl.ds(LANE * j, LANE)] * rowd_t[j]
            part = part + u * u
        acc[3] = acc[3] + part * across(cold_sq, t)
    vec = hv[...] * clip
    v_new = KEEP * vv_in[...] + MIX * (vec * vec + EPSILON)
    vec = vec / jnp.sqrt(v_new)
    pack = jnp.where(lane1 == VEC_AT, jnp.sum(vec * vec, axis=1, keepdims=True), 0.0)
    for m in range(4):
        pack = jnp.where(lane1 == m, total(acc[m]), pack)
    u_all[linear] = pack
    to_all(u_all, 5)

    vv_new[...] = v_new
    hv[...] = vec
    row = jnp.sqrt(row_sq)
    cold = jnp.sqrt(cold_sq)
    for t in range(ROW_TILES):
        rows = pl.ds(SUB * t, SUB)
        scale = [across(row, ROW_TILES * m + t) for m in range(3)]
        mixed = jnp.where(in_q, scale[0], scale[1])
        for j in range(STEPS):
            at = pl.ds(LANE * j, LANE)
            hqo[rows, at] = hqo[rows, at] * col_t[j] * (mixed if j == Q_FULL else scale[j // Q_FULL])
        for j in range(UP // LANE):
            at = pl.ds(LANE * j, LANE)
            hu[rows, at] = hu[rows, at] * col_t[STEPS + j] * scale[2]
    for t in range(D_TILES):
        rows = pl.ds(SUB * t, SUB)
        scale = across(cold, t)
        for j in range(DR // LANE):
            at = pl.ds(LANE * j, LANE)
            hd[rows, at] = hd[rows, at] * rowd_t[j] * scale
    for m, ref in enumerate((n_rq, n_ro, n_ru)):
        ref[...] = from_tiles(row_new, ROW_TILES * m, R)
    n_rd[...] = rowd_new
    n_cq[...] = col_new[:, :COLS[0]]
    n_co[...] = col_new[:, COLS[0]:QO]
    n_cu[...] = col_new[:, QO:QO + UP]
    n_cd[...] = from_tiles(cold_new, 0, DC)

    for kind in range(3):
        send(peers[kind], peers[kind], push_sem.at[kind], peer_sem.at[kind, 0, 0], mate).wait_send()
        for side in range(2):
            first(kind, side, whole, a_sem.at[kind, side, 0]).wait_send()
            second(kind, side, whole, b_sem.at[kind, side, 0]).wait_send()
    for copy in (vec_core, vec_x, vec_y):
        copy.wait_send()
    groups = ((rp_all, TP), (cs_all, FSDP), (rsd_all, TP), (rpd_all, FSDP), (s_all, DEVICES), (u_all, DEVICES))
    for i, (buf, n) in enumerate(groups):
        if i < len(groups) - 1:
            spread(buf, i, n).wait_send()

    pack = gathered(u_all, len(groups) - 1, DEVICES)
    count = jnp.full((1, LANE), float(VEC * TP * FSDP), F32)
    for m in range(4):
        count = jnp.where(lane1 == m, float(ROWS[m] * FSDP * COLS[m] * TP), count)
    inv_out[...] = 1.0 / jnp.maximum(1.0, jnp.sqrt(pack / count))
    spread(u_all, len(groups) - 1, DEVICES).wait_send()


PIECES = ((3, 0, 48), (3, 48, 128), (3, 176, 176), (2, 0, 96), (2, 96, 80), (0, 0, 96), (0, 96, 80), (1, 0, R))
HELD = (ROWS[:3] + (DC,), COLS[:3] + (DR,))
GROUP = 16


def update_kernel(*refs):
    (hqo, hu, hd, hv, inv, vrq, vro, vru, vrd, vcq, vco, vcu, vcd, vv,
     wq, wo, wu, wd, wv, mq, mo, mu, md, mv,
     wq_out, wo_out, wu_out, wd_out, wv_out, mq_out, mo_out, mu_out, md_out, mv_out,
     vrq_out, vcq_out, vro_out, vco_out, vru_out, vcu_out, vrd_out, vcd_out, vv_out,
     bwq, bwo, bwu, bwd, bmq, bmo, bmu, bmd, bwv, bmv, out_sem, small_sem) = refs
    held = ((hqo, 0), (hqo, COLS[0]), (hu, 0), (hd, 0))
    w_in, m_in = (wq, wo, wu, wd), (mq, mo, mu, md)
    w_buf, m_buf = (bwq, bwo, bwu, bwd), (bmq, bmo, bmu, bmd)
    w_out, m_out = (wq_out, wo_out, wu_out, wd_out), (mq_out, mo_out, mu_out, md_out)

    def finish(u, w, m):
        m_new = (MOMENTUM * m.astype(F32) + (1.0 - MOMENTUM) * u).astype(BF16)
        return w - LEARN_RATE * (m_new.astype(F32) + WEIGHT_DECAY * w), m_new

    passed = ((vrq, vrq_out), (vro, vro_out), (vru, vru_out), (vrd, vrd_out),
              (vcq, vcq_out), (vco, vco_out), (vcu, vcu_out), (vcd, vcd_out), (vv, vv_out))
    stores = [pltpu.make_async_copy(src, dst, small_sem.at[i]) for i, (src, dst) in enumerate(passed)]
    w_new, m_new = finish(hv[...] * inv[:, VEC_AT:VEC_AT + 1], wv[...], mv[...])
    bwv[...] = w_new
    bmv[...] = m_new
    stores.append(pltpu.make_async_copy(bwv, wv_out, small_sem.at[len(passed)]))
    stores.append(pltpu.make_async_copy(bmv, mv_out, small_sem.at[len(passed) + 1]))
    for copy in stores:
        copy.start()
    for i, (m, r0, n) in enumerate(PIECES):
        scale = inv[:, m:m + 1]
        buf, c0 = held[m]

        for k in range(n // GROUP):
            rows = pl.ds(r0 + GROUP * k, GROUP)
            u = buf[rows, pl.ds(c0 // LANE * LANE, c0 % LANE + HELD[1][m])][:, c0 % LANE:]
            w_new, m_new = finish(u * scale, w_in[m][rows, :], m_in[m][rows, :])
            w_buf[m][rows, :] = w_new
            m_buf[m][rows, :] = m_new
        rows = pl.ds(r0, n)
        for j, (src, dst) in enumerate(((w_buf, w_out), (m_buf, m_out))):
            stores.append(pltpu.make_async_copy(src[m].at[rows, :], dst[m].at[rows, :], out_sem.at[i, j]))
            stores[-1].start()
    for copy in stores:
        copy.wait()


IN_HBM = pl.BlockSpec(memory_space=pltpu.HBM)
IN_VMEM = pl.BlockSpec(memory_space=pltpu.VMEM)
MIB = 1024 * 1024


def f32(*shape):
    return jax.ShapeDtypeStruct(shape, F32)


def vmem(*shape):
    return pltpu.VMEM(shape, F32)


def local_step(g_qkv, g_out, g_up, g_down, g_vec, w_qkv, w_out, w_up, w_down, w_vec,
               m_qkv, m_out, m_up, m_down, m_vec, vr_qkv, vc_qkv, vr_out, vc_out,
               vr_up, vc_up, vr_down, vc_down, v_vec):
    dma = pltpu.SemaphoreType.DMA
    rows_shapes = [(1, n) for n in ROWS]
    cols_shapes = [(1, n) for n in COLS]
    h_shapes = [(R, QO), (R, UP), (DC, DR)]
    wide_u, wide_d, vec = (R, UP), (DC, DR), (1, VEC)
    shapes = [
        (2, 2, 2, SUB, UP), (SLOTS, LANE, QO), (2, 2) + wide_u, (2, 2) + wide_d,
        (STEPS, LANE, QO), (2, 2) + wide_u, (2, 2) + wide_d, (STEPS, 2, 2, R, LANE),
        (STEPS, 2, R, LANE), (2,) + wide_u, (2,) + wide_d, (STEPS, R, LANE), wide_u, wide_d,
        vec, (3,) + vec, (2,) + vec, vec] + rows_shapes + cols_shapes + [
        (R, LANE), (R, LANE), (STEPS, SUB, LANE), (SUB, UP), (SUB, DR)] + [(SUB, LANE)] * 4 + [
        (1, WIDE), (1, DR),
        (FSDP, 1, WIDE), (TP, SUB, LANE), (TP, 1, DR), (FSDP, SUB, LANE),
        (DEVICES, 1, LANE), (DEVICES, 1, LANE)]
    sems = [(3, 2, STEPS)] * 2 + [(3,), (3, 2), (3, 2)] + [(3, 2, STEPS)] * 2 + [(1,), (3,), (3,), (9,), (6,), (6,), (2,)]
    inputs = [pltpu.with_memory_space_constraint(a, pltpu.HBM)
              for a in (g_qkv[0, 0].T, g_out[0, 0].T, g_up.reshape(2, 2, 2, R, UP), g_down[0, 0].T, g_vec[0],
                        vr_qkv, vr_out, vr_up, vr_down, vc_qkv, vc_out, vc_up, vc_down, v_vec)]
    reduced = pl.pallas_call(
        reduce_kernel,
        name="reduce_and_scale",
        out_shape=[f32(*s) for s in h_shapes + [vec, (1, LANE)] + rows_shapes + cols_shapes + [vec]],
        in_specs=[IN_HBM] * 14,
        out_specs=[IN_VMEM] * 14,
        scratch_shapes=[vmem(*s) for s in shapes] + [dma(s) for s in sems] + [pltpu.SemaphoreType.REGULAR((TP + 1,))],
        compiler_params=pltpu.CompilerParams(
            collective_id=0, has_side_effects=True, vmem_limit_bytes=A_MIB * MIB),
    )(*inputs)

    ws = [w_qkv[0], w_out[0], w_up[0], w_down[0].T, w_vec]
    ms = [m_qkv[0], m_out[0], m_up[0], m_down[0].T, m_vec]
    mats = list(zip(*HELD))
    outs = pl.pallas_call(
        update_kernel,
        name="update",
        out_shape=([f32(*s) for s in mats + [vec]] + [jax.ShapeDtypeStruct(s, BF16) for s in mats + [vec]]
                   + [f32(*s) for m in range(4) for s in (rows_shapes[m], cols_shapes[m])] + [f32(*vec)]),
        in_specs=[IN_VMEM] * 24,
        out_specs=[IN_HBM] * 19,
        scratch_shapes=([vmem(*s) for s in mats] + [pltpu.VMEM(s, BF16) for s in mats]
                        + [vmem(*vec), pltpu.VMEM(vec, BF16), dma((len(PIECES), 2)), dma((11,))]),
        compiler_params=pltpu.CompilerParams(vmem_limit_bytes=B_MIB * MIB),
    )(*reduced, *ws, *ms)
    outs = list(outs)
    for i in range(10):
        if i % 5 == 3:
            outs[i] = outs[i].T
        if i % 5 != 4:
            outs[i] = outs[i][None]
    return tuple(outs)


A_MIB, B_MIB = 46, 12


def solution(mesh):
    grad_spec = P("fsdp", None, None, "tp")
    vec_grad_spec = P("fsdp", None, "tp")
    mat_spec = P(None, "fsdp", "tp")
    vec_spec = P(None, "tp")
    row_spec = P(None, "fsdp")
    col_spec = P(None, "tp")
    state_specs = ((mat_spec,) * 4 + (vec_spec,) + (mat_spec,) * 4 + (vec_spec,)
                   + (row_spec, col_spec) * 4 + (vec_spec,))
    arg_specs = (grad_spec,) * 4 + (vec_grad_spec,) + state_specs
    return jax.shard_map(local_step, mesh=mesh, in_specs=arg_specs, out_specs=state_specs, check_vma=False)
```

```python
import jax
import jax.numpy as jnp
from jax import lax
from jax.experimental import pallas as pl
from jax.experimental.pallas import tpu as pltpu
from jax.sharding import PartitionSpec as P

TRAIN_STEP = 3
LEARN_RATE = 0.0008
WEIGHT_DECAY = 0.03
MOMENTUM = 0.9
EPSILON = 1e-30
BETA_TWO = 1.0 - TRAIN_STEP ** -0.8
KEEP, MIX = BETA_TWO, 1.0 - BETA_TWO

F32 = jnp.float32
BF16 = jnp.bfloat16
MESH = pl.DeviceIdType.MESH
HIGHEST = lax.Precision.HIGHEST
TP, FSDP, DEVICES = 4, 8, 32
SUB, LANE = 8, 128

ROWS = (176, 176, 176, 768)
COLS = (1056, 352, 1536, 352)
VEC = 4704
R, QO, UP, DR, DC = ROWS[0], COLS[0] + COLS[1], COLS[2], ROWS[3], COLS[3]
HALF_R, HALF_DC = R // 2, DC // 2
STEPS = QO // LANE
D_STEP = HALF_DC // STEPS
Q_FULL = COLS[0] // LANE
Q_LEFT = COLS[0] - Q_FULL * LANE
ROW_TILES = R // SUB
D_TILES = DC // SUB
WIDE = -(-(QO + UP) // (SUB * LANE)) * SUB * LANE
LOOK, SLOTS = 2, 3
OPENING = ((1,), (2,))
U_, QO_, D_ = 0, 1, 2
BATCH = 6
BATCHES = ((0, 6), (6, 5))
SECOND = (BATCHES, BATCHES, ((0, 6), (6, 3), (9, 1), (10, 1)))
SECOND_AT = (0, 2, 4)
VR_AT, VEC_AT = 4, 8


def lanes(shape):
    return lax.broadcasted_iota(jnp.int32, shape, len(shape) - 1)


def sublanes(shape):
    return lax.broadcasted_iota(jnp.int32, shape, len(shape) - 2)


def total(x):
    return jnp.sum(jnp.sum(x, axis=1, keepdims=True), axis=0, keepdims=True)


def pick(x, lane):
    return jnp.sum(jnp.where(lanes(x.shape) == lane, x, 0.0), axis=1, keepdims=True)


def dot(a, b):
    return lax.dot_general(a, b, (((1,), (0,)), ((), ())), precision=HIGHEST, preferred_element_type=F32)


def own_sublane(n):
    return lanes((SUB, n)) % SUB == sublanes((SUB, n))


def to_tiles(row, at):
    n = row.shape[1]
    chosen = (sublanes((n, LANE)) // SUB + at == lanes((n, LANE))).astype(F32)
    return dot(jnp.where(own_sublane(n), row, 0.0), chosen)


def from_tiles(tiles, at, n):
    chosen = (lanes((LANE, n)) // SUB + at == sublanes((LANE, n))).astype(F32)
    return jnp.sum(jnp.where(own_sublane(n), dot(tiles, chosen), 0.0), axis=0, keepdims=True)


def across(tiles, t):
    return jnp.broadcast_to(tiles[:, t:t + 1], (SUB, LANE))


def reduce_kernel(*refs):
    (gq, go, gu, gd, gv, vrq, vro, vru, vrd, vcq, vco, vcu, vcd, vv,
     wq, wo, wu, wd, wv, mq, mo, mu, md, mv,
     hqo, hu, hd, hv, inv_out,
     wq_out, wo_out, wu_out, wd_out, wv_out, mq_out, mo_out, mu_out, md_out, mv_out,
     n_rq, n_ro, n_ru, n_rd, n_cq, n_co, n_cu, n_cd, vv_new,
     stage, own_qo, own_u, own_d, peer_qo, peer_u, peer_d, s_qo,
     a_qo, a_u, a_d, b_qo, b_u, b_d,
     vec_own, vec_in, vec_mid, vv_in,
     r_q, r_o, r_u, r_d, c_q, c_o, c_u, c_d,
     p_q, p_o, cs_qo, cs_u, rs_d, rp_acc, rpd_acc, rp_old, rpd_old, col_buf, rowd_buf,
     cs_all, rp_all, rsd_all, rpd_all, s_all, u_all,
     own_sem, peer_sem, push_sem, first_sem, second_sem, a_sem, b_sem,
     vec_sem, vec_send, vec_recv, small_sem, stat_send, stat_recv, stage_sem, round_sem) = refs

    me = lax.axis_index("fsdp")
    z = lax.axis_index("tp")
    core = lax.rem(me, 2)
    x = lax.rem(me // 2, 2)
    y = me // 4
    linear = z * FSDP + me
    mate = {"fsdp": me + 1 - 2 * core}
    across_x = {"fsdp": me + 2 - 4 * x}
    across_y = {"fsdp": me + 4 - 8 * y}
    every = slice(None)

    def flip(v, bits):
        for bit in range(3):
            step = 2 ** bit
            if bits & step:
                v = v + step - 2 * step * lax.rem(v // step, 2)
        return v

    others = [{"tp": flip(z, a), "fsdp": flip(me, b)} for a in range(TP - 1, -1, -1)
              for b in range(FSDP - 1, -1, -1) if a + b > 0]

    owns, peers = (own_u, own_qo, own_d), (peer_u, peer_qo, peer_d)
    sums, firsts, seconds = (own_u, s_qo, own_d), (a_u, a_qo, a_d), (b_u, b_qo, b_d)

    def send(src, dst, ssem, rsem, to):
        return pltpu.make_async_remote_copy(
            src_ref=src, dst_ref=dst, send_sem=ssem, recv_sem=rsem,
            device_id=to, device_id_type=MESH)

    def index(kind, lead, side, k):
        if kind == QO_:
            return (k,) + lead + (pl.ds(HALF_R * side, HALF_R),)
        if kind == U_:
            return lead + (pl.ds(pl.multiple_of(HALF_R * side + SUB * k, SUB), SUB),)
        return lead + (pl.ds(pl.multiple_of(HALF_DC * side + D_STEP * k, SUB), D_STEP),)

    def first(kind, side, at, sem):
        lead, to = (((every, 1 - x), across_x), ((1 - y, every), across_y))[side]
        return send(sums[kind].at[at(kind, lead, side)], firsts[kind].at[at(kind, (every,), side)],
                    first_sem.at[kind], sem, to)

    def second(kind, side, at, sem):
        lead, to = (((1 - y, x), across_y), ((y, 1 - x), across_x))[side]
        return send(sums[kind].at[at(kind, lead, side)], seconds[kind].at[at(kind, (), side)],
                    second_sem.at[kind], sem, to)

    def chunk(k):
        return lambda kind, lead, side: index(kind, lead, side, k)

    def span(k, n):
        def at(kind, lead, side):
            if kind == QO_:
                return (pl.ds(k, n),) + lead + (pl.ds(HALF_R * side, HALF_R),)
            half, step = ((HALF_R, SUB), None, (HALF_DC, D_STEP))[kind]
            return lead + (pl.ds(half * side + step * k, step * n),)
        return at

    def own_ring(kind, side, k):
        return own_sem.at[side, lax.rem(kind * STEPS + k, SLOTS)]

    def peer_ring(kind, side, k):
        return peer_sem.at[side, lax.rem(kind * STEPS + k, 2 * SLOTS)]

    def load(kind, k, side, away):
        if away:
            dst, sem, c = peers[kind], peer_ring(kind, side, k), 1 - core
            copy = lambda a, b: send(a, b, push_sem.at[kind], sem, mate)
        else:
            dst, sem, c = owns[kind], own_ring(kind, side, k), core
            copy = lambda a, b: pltpu.make_async_copy(a, b, sem)
        if kind == U_:
            at = index(kind, (), side, k)
            return [(None, copy(gu.at[(every, every, c) + at], dst.at[(every, every) + at]))]
        if kind == D_:
            at = index(kind, (), side, k)
            return [(None, copy(gd.at[at + (pl.ds(pl.multiple_of(DR * (2 * b + c), LANE), DR),)],
                                dst.at[(b // 2, b % 2) + at])) for b in range(4)]
        slot = dst.at[k if away else lax.rem(k, SLOTS)]
        rest = LANE - Q_LEFT
        at_q = pl.multiple_of(LANE * jnp.minimum(k, Q_FULL - 1), LANE)
        at_o = pl.multiple_of(rest + LANE * jnp.maximum(k - Q_FULL - 1, 0), SUB)
        return [(k < Q_FULL, copy(gq.at[pl.ds(at_q, LANE)], slot)),
                (k == Q_FULL, copy(gq.at[pl.ds(Q_FULL * LANE, Q_LEFT)], slot.at[pl.ds(0, Q_LEFT)])),
                (k == Q_FULL, copy(go.at[pl.ds(0, rest)], slot.at[pl.ds(Q_LEFT, rest)])),
                (k > Q_FULL, copy(go.at[pl.ds(at_o, LANE)], slot))]

    def start_kind(kind, k, away):
        for side in range(1 if kind == QO_ else 2):
            for cond, copy in load(kind, k, side, away):
                if cond is None:
                    copy.start()
                else:
                    pl.when(cond)(copy.start)

    def start_loads(step, away):
        for kind in range(3):
            k = step - kind * STEPS
            pl.when(jnp.logical_and(k >= 0, k < STEPS))(lambda kind=kind, k=k: start_kind(kind, k, away))

    def loaded(kind, side, k):
        if kind == QO_:
            here, there = own_qo.at[lax.rem(k, SLOTS)], peer_qo.at[k]
        else:
            at = index(kind, (every, every), side, k)
            here, there = owns[kind].at[at], peers[kind].at[at]
        pltpu.make_async_copy(here, here, own_ring(kind, side, k)).wait()
        send(there, there, push_sem.at[kind], peer_ring(kind, side, k), mate).wait_recv()

    smalls = [(vrq, r_q), (vro, r_o), (vru, r_u), (vrd, r_d),
              (vcq, c_q), (vco, c_o), (vcu, c_u), (vcd, c_d), (vv, vv_in)]
    small_copies = [pltpu.make_async_copy(a, b, small_sem.at[i]) for i, (a, b) in enumerate(smalls)]
    vec_copy = pltpu.make_async_copy(gv, vec_own, vec_sem.at[0])

    staged = [pltpu.make_async_copy(gu.at[(every, every, 1 - core) + index(U_, (), side, 0)],
                                    stage.at[side], stage_sem.at[side]) for side in range(2)]
    for copy in staged:
        copy.start()
    start_kind(U_, 0, False)
    barrier = pltpu.get_barrier_semaphore()

    def signal(sem, to):
        pl.semaphore_signal(sem, inc=1, device_id=to, device_id_type=MESH)

    def signal_z(sem):
        pl.when(z > 0)(lambda: signal(sem, {"tp": z - 1}))
        pl.when(z < TP - 1)(lambda: signal(sem, {"tp": z + 1}))

    beside = jnp.where(z > 0, 1, 0) + jnp.where(z < TP - 1, 1, 0)
    near = (mate, across_x, across_y)
    for to in near:
        signal(barrier, to)
    signal_z(barrier)
    pl.semaphore_wait(barrier, len(near) + beside)

    for side in range(2):
        staged[side].wait()
        send(stage.at[side], peer_u.at[index(U_, (every, every), side, 0)],
             push_sem.at[U_], peer_ring(U_, side, 0), mate).start()
    vec_copy.start()
    for copy in small_copies:
        copy.start()
    vec_core = send(vec_own, vec_in.at[0], vec_send.at[0], vec_recv.at[0], mate)
    vec_x = send(vec_mid.at[0], vec_in.at[1], vec_send.at[1], vec_recv.at[1], across_x)
    vec_y = send(vec_mid.at[1], vec_in.at[2], vec_send.at[2], vec_recv.at[2], across_y)

    def turn(k, which):
        slot = lax.rem(k, SLOTS)
        for tile in range(STEPS):
            lo = LANE * tile
            cuts = [(b, max(lo, R * (2 * b + which)), min(lo + LANE, R * (2 * b + which) + R)) for b in range(4)]
            cuts = [cut for cut in cuts if cut[1] < cut[2]]
            if cuts:
                at = (every, pl.ds(lo, LANE))
                turned = (own_qo[(slot,) + at] + peer_qo[(k,) + at]).T
                for b, start, stop in cuts:
                    first_row = start - R * (2 * b + which)
                    s_qo[k, b // 2, b % 2, pl.ds(first_row, stop - start), :] = turned[start - lo:stop - lo]

    def stage1(kind, opening=False):
        def body(k, _):
            if not opening:
                start_loads(k + kind * STEPS + LOOK, False)
                start_loads(k + kind * STEPS + LOOK, True)
            if kind == QO_:
                loaded(kind, 0, k)
                for which in range(2):
                    pl.when(core == which)(lambda which=which: turn(k, which))
            for side in range(2):
                if kind != QO_:
                    loaded(kind, side, k)
                    for b in range(4):
                        at = index(kind, (b // 2, b % 2), side, k)
                        owns[kind][at] = owns[kind][at] + peers[kind][at]
                first(kind, side, chunk(k), a_sem.at[kind, side, k // BATCH]).start()
                if opening:
                    for step in OPENING[side]:
                        start_kind(U_, step, False)
                        start_kind(U_, step, True)
            return _
        return body

    stage1(U_, True)(0, 0)
    vec_copy.wait()
    vec_core.start()
    lax.fori_loop(1, STEPS, stage1(U_), 0)
    vec_core.wait_recv()
    vec_mid[0] = vec_own[...] + vec_in[0]
    vec_x.start()
    for kind in (QO_, D_):
        lax.fori_loop(0, STEPS, stage1(kind), 0)

    for copy in small_copies:
        copy.wait()
    kept = [(wq, wq_out), (wo, wo_out), (wu, wu_out), (wd, wd_out), (wv, wv_out),
            (mq, mq_out), (mo, mo_out), (mu, mu_out), (md, md_out), (mv, mv_out)]
    kept = [pltpu.make_async_copy(a, b, small_sem.at[i]) for i, (a, b) in enumerate(kept)]
    for copy in kept:
        copy.start()

    for ref in (cs_qo, cs_u, rs_d, rp_acc, rpd_acc, p_q, p_o):
        ref[...] = jnp.zeros_like(ref)
    old = to_tiles(r_q[...], 0) + to_tiles(r_o[...], ROW_TILES) + to_tiles(r_u[...], 2 * ROW_TILES)
    rp_old[...] = old
    rpd_old[...] = to_tiles(c_d[...], 0)
    lane = lanes((SUB, LANE))
    lane1 = lanes((1, LANE))
    masks = [jnp.logical_and(lane >= ROW_TILES * m, lane < ROW_TILES * (m + 1)) for m in range(3)]
    old_sums = [total(jnp.where(masks[m], old, 0.0)) for m in range(3)] + [total(r_d[...])]

    for i, to in enumerate(near):
        signal(round_sem.at[i], to)
        pl.semaphore_wait(round_sem.at[i], 1)
    for i in range(len(near), len(near) + TP - 2):
        signal_z(round_sem.at[i])
        pl.semaphore_wait(round_sem.at[i], beside)

    def stage2(kind):
        for g, (k0, n) in enumerate(BATCHES):
            for side in range(2):
                first(kind, side, span(k0, n), a_sem.at[kind, side, g]).wait_recv()
                lead, mine = (((1 - y, x), 1 - y), ((y, 1 - x), 1 - x))[side]

                def add(k, _):
                    at = index(kind, lead, side, k)
                    sums[kind][at] = sums[kind][at] + firsts[kind][index(kind, (mine,), side, k)]
                    return _

                lax.fori_loop(k0, k0 + n, add, 0)
            for b, (k1, m) in enumerate(SECOND[kind]):
                if k0 <= k1 < k0 + n:
                    for side in range(2):
                        second(kind, side, span(k1, m), b_sem.at[side, SECOND_AT[kind] + b]).start()

    for kind in (U_, QO_):
        stage2(kind)
    vec_x.wait_recv()
    vec_mid[1] = vec_mid[0] + vec_in[1]
    vec_y.start()
    stage2(D_)

    def finished(kind, side, k):
        return (sums[kind][index(kind, (y, x), side, k)]
                + firsts[kind][index(kind, ((y, x)[side],), side, k)]
                + seconds[kind][index(kind, (), side, k)])

    def stage3_u(side, k):
        full = finished(U_, side, k)
        hu[index(U_, (), side, k)] = full
        sq = full * full
        cs_u[...] += sq
        row = jnp.sum(sq, axis=1, keepdims=True)
        rp_acc[...] = jnp.where(lane == 2 * ROW_TILES + STEPS * side + k, row, rp_acc[...])

    def stage3_qo(side, k):
        rows = pl.ds(HALF_R * side, HALF_R)
        full = finished(QO_, side, k)
        hqo[rows, pl.ds(pl.multiple_of(LANE * k, LANE), LANE)] = full
        sq = full * full
        in_q = lanes(sq.shape) + LANE * k < COLS[0]
        p_q[rows, :] += jnp.where(in_q, sq, 0.0)
        p_o[rows, :] += jnp.where(in_q, 0.0, sq)
        part = sq[:SUB]
        for t in range(1, STEPS):
            part = part + sq[SUB * t:SUB * t + SUB]
        cs_qo[k] += part

    def stage3_d(side, k):
        full = finished(D_, side, k)
        hd[index(D_, (), side, k)] = full
        sq = full * full
        both = rpd_acc[...]
        for t in range(D_STEP // SUB):
            part = sq[SUB * t:SUB * t + SUB]
            rs_d[...] += part
            col = jnp.sum(part, axis=1, keepdims=True)
            at = (HALF_DC * side + D_STEP * k) // SUB + t
            both = jnp.where(lane == at, col, both)
        rpd_acc[...] = both

    def stage3(kind, take):
        for b, (k0, n) in enumerate(SECOND[kind]):
            for side in range(2):
                second(kind, side, span(k0, n), b_sem.at[side, SECOND_AT[kind] + b]).wait_recv()
                lax.fori_loop(k0, k0 + n, lambda k, _: [take(side, k), _][1], 0)

    def to_group(buf, at, i, n, axis, here):
        for d in range(1, n):
            send(buf.at[at], buf.at[at], stat_send.at[i], stat_recv.at[i],
                 {axis: lax.rem(here + d, n)}).start()

    def to_all(buf, i):
        for to in others:
            send(buf.at[linear], buf.at[linear], stat_send.at[i], stat_recv.at[i], to).start()

    def spread(buf, i, n):
        part = buf.at[pl.ds(0, n - 1)]
        return send(part, part, stat_send.at[i], stat_recv.at[i], mate)

    def gathered(buf, i, n):
        spread(buf, i, n).wait_recv()
        out = buf[0]
        for d in range(1, n):
            out = out + buf[d]
        return out

    stage3(U_, stage3_u)
    stage3(QO_, stage3_qo)
    vec_y.wait_recv()
    vec = vec_mid[1] + vec_in[2]
    hv[...] = vec
    rp = rp_acc[...]
    for t in range(ROW_TILES):
        for m, ref in enumerate((p_q, p_o)):
            row = jnp.sum(ref[pl.ds(SUB * t, SUB), :], axis=1, keepdims=True)
            rp = jnp.where(lane == ROW_TILES * m + t, row, rp)
    rp_all[z] = rp
    cs = [jnp.sum(cs_qo[k], axis=0, keepdims=True) for k in range(STEPS)]
    cs.append(jnp.sum(cs_u[...], axis=0, keepdims=True))
    cs_all[me] = jnp.concatenate(cs + [jnp.zeros((1, WIDE - QO - UP), F32)], axis=1)
    to_group(rp_all, z, 0, TP, "tp", z)
    to_group(cs_all, me, 1, FSDP, "fsdp", me)
    pack = jnp.where(lane1 == VEC_AT, jnp.sum(vec * vec, axis=1, keepdims=True), 0.0)
    for m in range(4):
        pack = jnp.where(lane1 == VR_AT + m, old_sums[m], pack)
    for m in range(3):
        pack = jnp.where(lane1 == m, total(jnp.where(masks[m], rp, 0.0)), pack)

    stage3(D_, stage3_d)
    rs = rs_d[...]
    s_all[linear] = jnp.where(lane1 == 3, total(rs), pack)
    to_all(s_all, 4)
    rsd_all[z] = jnp.sum(rs, axis=0, keepdims=True)
    to_group(rsd_all, z, 2, TP, "tp", z)
    rpd_all[me] = rpd_acc[...]
    to_group(rpd_all, me, 3, FSDP, "fsdp", me)

    vc_old = jnp.concatenate([c_q[...], c_o[...], c_u[...], jnp.ones((1, WIDE - QO - UP), F32)], axis=1)
    rp = gathered(rp_all, 0, TP)
    cs = gathered(cs_all, 1, FSDP)
    rsd = gathered(rsd_all, 2, TP)
    rpd = gathered(rpd_all, 3, FSDP)
    pack = gathered(s_all, 4, DEVICES)
    squares = [pick(pack, m) for m in range(4)]
    norm = jnp.sqrt((squares[0] + squares[1]) + (squares[2] + squares[3]) + pick(pack, VEC_AT) / FSDP)
    clip = jnp.minimum(1.0, 1.0 / norm)

    def clipped(v):
        return jnp.where(clip > 0.0, (v * clip) * clip, 0.0)

    means = []
    for m in range(4):
        r_all, c_all = float(ROWS[m] * FSDP), float(COLS[m] * TP)
        means.append(KEEP * (pick(pack, VR_AT + m) / (TP * r_all))
                     + MIX * (clipped(squares[m]) / (r_all * c_all) + EPSILON))
    mean_rp = jnp.where(masks[0], means[0], jnp.where(masks[1], means[1], means[2]))
    wide = jnp.where(masks[0], float(COLS[0] * TP), jnp.where(masks[1], float(COLS[1] * TP), float(COLS[2] * TP)))
    row_new = KEEP * rp_old[...] + MIX * (clipped(rp) / wide + EPSILON)
    row_sq = mean_rp / row_new
    rowd_new = KEEP * r_d[...] + MIX * (clipped(rsd) / float(DC * TP) + EPSILON)
    rowd_buf[...] = clip * jnp.sqrt(means[3] / rowd_new)
    col_new = KEEP * vc_old + MIX * (clipped(cs) / float(R * FSDP) + EPSILON)
    col_buf[...] = clip / jnp.sqrt(col_new)
    cold_new = KEEP * rpd_old[...] + MIX * (clipped(rpd) / float(DR * FSDP) + EPSILON)
    cold_sq = 1.0 / cold_new

    def tile(ref, j):
        return jnp.broadcast_to(ref[:, pl.ds(LANE * j, LANE)], (SUB, LANE))

    zero = jnp.zeros((SUB, LANE), F32)
    acc = [zero] * 4
    in_q = lane < Q_LEFT
    col_t = [tile(col_buf, j) for j in range(STEPS + UP // LANE)]
    for t in range(ROW_TILES):
        rows = pl.ds(SUB * t, SUB)
        part = [zero] * 3
        for j in range(STEPS):
            u = hqo[rows, pl.ds(LANE * j, LANE)] * col_t[j]
            u = u * u
            if j == Q_FULL:
                part[0] = part[0] + jnp.where(in_q, u, 0.0)
                part[1] = part[1] + jnp.where(in_q, 0.0, u)
            else:
                part[j // Q_FULL] = part[j // Q_FULL] + u
        for j in range(UP // LANE):
            u = hu[rows, pl.ds(LANE * j, LANE)] * col_t[STEPS + j]
            part[2] = part[2] + u * u
        for m in range(3):
            acc[m] = acc[m] + part[m] * across(row_sq, ROW_TILES * m + t)
    rowd_t = [tile(rowd_buf, j) for j in range(DR // LANE)]
    for t in range(D_TILES):
        part = zero
        for j in range(DR // LANE):
            u = hd[pl.ds(SUB * t, SUB), pl.ds(LANE * j, LANE)] * rowd_t[j]
            part = part + u * u
        acc[3] = acc[3] + part * across(cold_sq, t)
    vec = hv[...] * clip
    v_new = KEEP * vv_in[...] + MIX * (vec * vec + EPSILON)
    vec = vec / jnp.sqrt(v_new)
    pack = jnp.where(lane1 == VEC_AT, jnp.sum(vec * vec, axis=1, keepdims=True), 0.0)
    for m in range(4):
        pack = jnp.where(lane1 == m, total(acc[m]), pack)
    u_all[linear] = pack
    to_all(u_all, 5)

    vv_new[...] = v_new
    hv[...] = vec
    row = jnp.sqrt(row_sq)
    cold = jnp.sqrt(cold_sq)
    for t in range(ROW_TILES):
        rows = pl.ds(SUB * t, SUB)
        scale = [across(row, ROW_TILES * m + t) for m in range(3)]
        mixed = jnp.where(in_q, scale[0], scale[1])
        for j in range(STEPS):
            at = pl.ds(LANE * j, LANE)
            hqo[rows, at] = hqo[rows, at] * col_t[j] * (mixed if j == Q_FULL else scale[j // Q_FULL])
        for j in range(UP // LANE):
            at = pl.ds(LANE * j, LANE)
            hu[rows, at] = hu[rows, at] * col_t[STEPS + j] * scale[2]
    for t in range(D_TILES):
        rows = pl.ds(SUB * t, SUB)
        scale = across(cold, t)
        for j in range(DR // LANE):
            at = pl.ds(LANE * j, LANE)
            hd[rows, at] = hd[rows, at] * rowd_t[j] * scale
    for m, ref in enumerate((n_rq, n_ro, n_ru)):
        ref[...] = from_tiles(row_new, ROW_TILES * m, R)
    n_rd[...] = rowd_new
    n_cq[...] = col_new[:, :COLS[0]]
    n_co[...] = col_new[:, COLS[0]:QO]
    n_cu[...] = col_new[:, QO:QO + UP]
    n_cd[...] = from_tiles(cold_new, 0, DC)

    for kind in range(3):
        send(peers[kind], peers[kind], push_sem.at[kind], peer_sem.at[0, 0], mate).wait_send()
        send(firsts[kind], firsts[kind], first_sem.at[kind], a_sem.at[kind, 0, 0], mate).wait_send()
        send(seconds[kind], seconds[kind], second_sem.at[kind], b_sem.at[0, 0], mate).wait_send()
    for copy in (vec_core, vec_x, vec_y):
        copy.wait_send()
    for copy in kept:
        copy.wait()
    groups = ((rp_all, TP), (cs_all, FSDP), (rsd_all, TP), (rpd_all, FSDP), (s_all, DEVICES), (u_all, DEVICES))
    for i, (buf, n) in enumerate(groups):
        if i < len(groups) - 1:
            spread(buf, i, n).wait_send()

    pack = gathered(u_all, len(groups) - 1, DEVICES)
    count = jnp.full((1, LANE), float(VEC * TP * FSDP), F32)
    for m in range(4):
        count = jnp.where(lane1 == m, float(ROWS[m] * FSDP * COLS[m] * TP), count)
    inv_out[...] = 1.0 / jnp.maximum(1.0, jnp.sqrt(pack / count))
    spread(u_all, len(groups) - 1, DEVICES).wait_send()


PIECES = ((3, 0, 48), (3, 48, 128), (3, 176, 176), (2, 0, 96), (2, 96, 80), (0, 0, 96), (0, 96, 80), (1, 0, R))
HELD = (ROWS[:3] + (DC,), COLS[:3] + (DR,))
GROUP = 16


def update_kernel(*refs):
    (hqo, hu, hd, hv, inv, wq, wo, wu, wd, wv, mq, mo, mu, md, mv,
     vrq, vro, vru, vrd, vcq, vco, vcu, vcd, vv,
     wq_out, wo_out, wu_out, wd_out, wv_out, mq_out, mo_out, mu_out, md_out, mv_out,
     vrq_out, vcq_out, vro_out, vco_out, vru_out, vcu_out, vrd_out, vcd_out, vv_out,
     bwq, bwo, bwu, bwd, bmq, bmo, bmu, bmd, bwv, bmv, out_sem, small_sem) = refs
    held = ((hqo, 0), (hqo, COLS[0]), (hu, 0), (hd, 0))
    w_in, m_in = (wq, wo, wu, wd), (mq, mo, mu, md)
    w_buf, m_buf = (bwq, bwo, bwu, bwd), (bmq, bmo, bmu, bmd)
    w_out, m_out = (wq_out, wo_out, wu_out, wd_out), (mq_out, mo_out, mu_out, md_out)

    def finish(u, w, m):
        m_new = (MOMENTUM * m.astype(F32) + (1.0 - MOMENTUM) * u).astype(BF16)
        return w - LEARN_RATE * (m_new.astype(F32) + WEIGHT_DECAY * w), m_new

    passed = ((vrq, vrq_out), (vro, vro_out), (vru, vru_out), (vrd, vrd_out),
              (vcq, vcq_out), (vco, vco_out), (vcu, vcu_out), (vcd, vcd_out), (vv, vv_out))
    stores = [pltpu.make_async_copy(src, dst, small_sem.at[i]) for i, (src, dst) in enumerate(passed)]
    w_new, m_new = finish(hv[...] * inv[:, VEC_AT:VEC_AT + 1], wv[...], mv[...])
    bwv[...] = w_new
    bmv[...] = m_new
    stores.append(pltpu.make_async_copy(bwv, wv_out, small_sem.at[len(passed)]))
    stores.append(pltpu.make_async_copy(bmv, mv_out, small_sem.at[len(passed) + 1]))
    for copy in stores:
        copy.start()
    for m, r0, n in PIECES:
        scale = inv[:, m:m + 1]
        buf, c0 = held[m]

        for k in range(n // GROUP):
            rows = pl.ds(r0 + GROUP * k, GROUP)
            u = buf[rows, pl.ds(c0 // LANE * LANE, c0 % LANE + HELD[1][m])][:, c0 % LANE:]
            w_new, m_new = finish(u * scale, w_in[m][rows, :], m_in[m][rows, :])
            w_buf[m][rows, :] = w_new
            m_buf[m][rows, :] = m_new
        rows = pl.ds(r0, n)
        for j, (src, dst) in enumerate(((w_buf, w_out), (m_buf, m_out))):
            pltpu.make_async_copy(src[m].at[rows, :], dst[m].at[rows, :], out_sem.at[m, j]).start()
    for m in range(4):
        for j, (src, dst) in enumerate(((w_buf, w_out), (m_buf, m_out))):
            stores.append(pltpu.make_async_copy(src[m], dst[m], out_sem.at[m, j]))
    for copy in stores:
        copy.wait()


IN_HBM = pl.BlockSpec(memory_space=pltpu.HBM)
IN_VMEM = pl.BlockSpec(memory_space=pltpu.VMEM)
MIB = 1024 * 1024


def f32(*shape):
    return jax.ShapeDtypeStruct(shape, F32)


def vmem(*shape):
    return pltpu.VMEM(shape, F32)


def local_step(g_qkv, g_out, g_up, g_down, g_vec, w_qkv, w_out, w_up, w_down, w_vec,
               m_qkv, m_out, m_up, m_down, m_vec, vr_qkv, vc_qkv, vr_out, vc_out,
               vr_up, vc_up, vr_down, vc_down, v_vec):
    dma = pltpu.SemaphoreType.DMA
    rows_shapes = [(1, n) for n in ROWS]
    cols_shapes = [(1, n) for n in COLS]
    h_shapes = [(R, QO), (R, UP), (DC, DR)]
    wide_u, wide_d, vec = (R, UP), (DC, DR), (1, VEC)
    shapes = [
        (2, 2, 2, SUB, UP), (SLOTS, LANE, QO), (2, 2) + wide_u, (2, 2) + wide_d,
        (STEPS, LANE, QO), (2, 2) + wide_u, (2, 2) + wide_d, (STEPS, 2, 2, R, LANE),
        (STEPS, 2, R, LANE), (2,) + wide_u, (2,) + wide_d, (STEPS, R, LANE), wide_u, wide_d,
        vec, (3,) + vec, (2,) + vec, vec] + rows_shapes + cols_shapes + [
        (R, LANE), (R, LANE), (STEPS, SUB, LANE), (SUB, UP), (SUB, DR)] + [(SUB, LANE)] * 4 + [
        (1, WIDE), (1, DR),
        (FSDP, 1, WIDE), (TP, SUB, LANE), (TP, 1, DR), (FSDP, SUB, LANE),
        (DEVICES, 1, LANE), (DEVICES, 1, LANE)]
    sems = [(2, SLOTS), (2, 2 * SLOTS), (3,), (3,), (3,), (3, 2, len(BATCHES)),
            (2, SECOND_AT[-1] + len(SECOND[-1])), (1,), (3,), (3,), (10,), (6,), (6,), (2,)]
    ws = [w_qkv[0], w_out[0], w_up[0], w_down[0].T, w_vec]
    ms = [m_qkv[0], m_out[0], m_up[0], m_down[0].T, m_vec]
    mats = list(zip(*HELD))
    state = [f32(*s) for s in mats + [vec]] + [jax.ShapeDtypeStruct(s, BF16) for s in mats + [vec]]
    inputs = [pltpu.with_memory_space_constraint(a, pltpu.HBM)
              for a in (g_qkv[0, 0].T, g_out[0, 0].T, g_up.reshape(2, 2, 2, R, UP), g_down[0, 0].T, g_vec[0],
                        vr_qkv, vr_out, vr_up, vr_down, vc_qkv, vc_out, vc_up, vc_down, v_vec, *ws, *ms)]
    reduced = pl.pallas_call(
        reduce_kernel,
        name="reduce_and_scale",
        out_shape=([f32(*s) for s in h_shapes + [vec, (1, LANE)]] + state
                   + [f32(*s) for s in rows_shapes + cols_shapes + [vec]]),
        in_specs=[IN_HBM] * 24,
        out_specs=[IN_VMEM] * 24,
        scratch_shapes=[vmem(*s) for s in shapes] + [dma(s) for s in sems] + [pltpu.SemaphoreType.REGULAR((TP + 1,))],
        compiler_params=pltpu.CompilerParams(
            collective_id=0, has_side_effects=True, vmem_limit_bytes=A_MIB * MIB),
    )(*inputs)

    outs = pl.pallas_call(
        update_kernel,
        name="update",
        out_shape=(state + [f32(*s) for m in range(4) for s in (rows_shapes[m], cols_shapes[m])] + [f32(*vec)]),
        in_specs=[IN_VMEM] * 24,
        out_specs=[IN_HBM] * 19,
        scratch_shapes=([vmem(*s) for s in mats] + [pltpu.VMEM(s, BF16) for s in mats]
                        + [vmem(*vec), pltpu.VMEM(vec, BF16), dma((4, 2)), dma((11,))]),
        compiler_params=pltpu.CompilerParams(vmem_limit_bytes=B_MIB * MIB),
    )(*reduced)
    outs = list(outs)
    for i in range(10):
        if i % 5 == 3:
            outs[i] = outs[i].T
        if i % 5 != 4:
            outs[i] = outs[i][None]
    return tuple(outs)


A_MIB, B_MIB = 46, 12


def solution(mesh):
    grad_spec = P("fsdp", None, None, "tp")
    vec_grad_spec = P("fsdp", None, "tp")
    mat_spec = P(None, "fsdp", "tp")
    vec_spec = P(None, "tp")
    row_spec = P(None, "fsdp")
    col_spec = P(None, "tp")
    state_specs = ((mat_spec,) * 4 + (vec_spec,) + (mat_spec,) * 4 + (vec_spec,)
                   + (row_spec, col_spec) * 4 + (vec_spec,))
    arg_specs = (grad_spec,) * 4 + (vec_grad_spec,) + state_specs
    return jax.shard_map(local_step, mesh=mesh, in_specs=arg_specs, out_specs=state_specs, check_vma=False)
```

```python
import jax
import jax.numpy as jnp
from jax import lax
from jax.experimental import pallas as pl
from jax.experimental.pallas import tpu as pltpu
from jax.sharding import PartitionSpec as P

TRAIN_STEP = 3
LEARN_RATE = 0.0008
WEIGHT_DECAY = 0.03
MOMENTUM = 0.9
EPSILON = 1e-30
BETA_TWO = 1.0 - TRAIN_STEP ** -0.8
KEEP, MIX = BETA_TWO, 1.0 - BETA_TWO

F32 = jnp.float32
BF16 = jnp.bfloat16
MESH = pl.DeviceIdType.MESH
HIGHEST = lax.Precision.HIGHEST
TP, FSDP, DEVICES = 4, 8, 32
SUB, LANE = 8, 128

ROWS = (176, 176, 176, 768)
COLS = (1056, 352, 1536, 352)
VEC = 4704
R, QO, UP, DR, DC = ROWS[0], COLS[0] + COLS[1], COLS[2], ROWS[3], COLS[3]
HALF_R, HALF_DC = R // 2, DC // 2
STEPS = QO // LANE
D_STEP = HALF_DC // STEPS
Q_FULL = COLS[0] // LANE
Q_LEFT = COLS[0] - Q_FULL * LANE
ROW_TILES = R // SUB
D_TILES = DC // SUB
WIDE = -(-(QO + UP) // (SUB * LANE)) * SUB * LANE
LOOK, SLOTS = 1, 2
OPENING = ((1,), ())
U_, QO_, D_ = 0, 1, 2
BATCH = 11
BATCHES = ((0, 11),)
SECOND = (BATCHES, BATCHES, ((0, 6), (6, 4), (10, 1)))
SECOND_AT = (0, 1, 2)
PARTS = ((0, 0), (1, 0), (0, 1), (1, 1))
VR_AT, VEC_AT = 4, 8


def lanes(shape):
    return lax.broadcasted_iota(jnp.int32, shape, len(shape) - 1)


def sublanes(shape):
    return lax.broadcasted_iota(jnp.int32, shape, len(shape) - 2)


def total(x):
    return jnp.sum(jnp.sum(x, axis=1, keepdims=True), axis=0, keepdims=True)


def pick(x, lane):
    return jnp.sum(jnp.where(lanes(x.shape) == lane, x, 0.0), axis=1, keepdims=True)


def dot(a, b):
    return lax.dot_general(a, b, (((1,), (0,)), ((), ())), precision=HIGHEST, preferred_element_type=F32)


def own_sublane(n):
    return lanes((SUB, n)) % SUB == sublanes((SUB, n))


def to_tiles(row, at):
    n = row.shape[1]
    chosen = (sublanes((n, LANE)) // SUB + at == lanes((n, LANE))).astype(F32)
    return dot(jnp.where(own_sublane(n), row, 0.0), chosen)


def from_tiles(tiles, at, n):
    chosen = (lanes((LANE, n)) // SUB + at == sublanes((LANE, n))).astype(F32)
    return jnp.sum(jnp.where(own_sublane(n), dot(tiles, chosen), 0.0), axis=0, keepdims=True)


def across(tiles, t):
    return jnp.broadcast_to(tiles[:, t:t + 1], (SUB, LANE))


def reduce_kernel(*refs):
    (gq, go, gu, gd, gv, vrq, vro, vru, vrd, vcq, vco, vcu, vcd, vv,
     wq, wo, wu, wd, wv, mq, mo, mu, md, mv,
     hqo, hu, hd, hv, inv_out,
     wq_out, wo_out, wu_out, wd_out, wv_out, mq_out, mo_out, mu_out, md_out, mv_out,
     n_rq, n_ro, n_ru, n_rd, n_cq, n_co, n_cu, n_cd, vv_new,
     stage, own_qo, own_u, own_d, peer_qo, peer_u, peer_d, s_qo,
     a_qo, a_u, a_d, b_qo, b_u, b_d,
     vec_own, vec_in, vec_mid, vv_in,
     r_q, r_o, r_u, r_d, c_q, c_o, c_u, c_d,
     p_q, p_o, cs_qo, cs_u, rs_d, rp_acc, rpd_acc, rp_old, rpd_old, col_buf, rowd_buf,
     cs_all, rp_all, rsd_all, rpd_all, s_all, u_all,
     own_sem, peer_sem, push_sem, first_sem, second_sem, a_sem, b_sem,
     vec_send, vec_recv, stat_send, stat_recv, open_sem, round_sem) = refs

    me = lax.axis_index("fsdp")
    z = lax.axis_index("tp")
    core = lax.rem(me, 2)
    x = lax.rem(me // 2, 2)
    y = me // 4
    linear = z * FSDP + me
    mate = {"fsdp": me + 1 - 2 * core}
    across_x = {"fsdp": me + 2 - 4 * x}
    across_y = {"fsdp": me + 4 - 8 * y}
    every = slice(None)

    def flip(v, bits):
        for bit in range(3):
            step = 2 ** bit
            if bits & step:
                v = v + step - 2 * step * lax.rem(v // step, 2)
        return v

    others = [{"tp": flip(z, a), "fsdp": flip(me, b)} for a in range(TP - 1, -1, -1)
              for b in range(FSDP - 1, -1, -1) if a + b > 0]

    owns, peers = (own_u, own_qo, own_d), (peer_u, peer_qo, peer_d)
    sums, firsts, seconds = (own_u, s_qo, own_d), (a_u, a_qo, a_d), (b_u, b_qo, b_d)

    def send(src, dst, ssem, rsem, to):
        return pltpu.make_async_remote_copy(
            src_ref=src, dst_ref=dst, send_sem=ssem, recv_sem=rsem,
            device_id=to, device_id_type=MESH)

    def index(kind, lead, side, k):
        if kind == QO_:
            return (k,) + lead + (pl.ds(HALF_R * side, HALF_R),)
        if kind == U_:
            return lead + (pl.ds(pl.multiple_of(HALF_R * side + SUB * k, SUB), SUB),)
        return lead + (pl.ds(pl.multiple_of(HALF_DC * side + D_STEP * k, SUB), D_STEP),)

    def first(kind, side, at, sem):
        lead, to = (((every, 1 - x), across_x), ((1 - y, every), across_y))[side]
        return send(sums[kind].at[at(kind, lead, side)], firsts[kind].at[at(kind, (every,), side)],
                    first_sem.at[kind], sem, to)

    def second(kind, side, at, sem):
        lead, to = (((1 - y, x), across_y), ((y, 1 - x), across_x))[side]
        return send(sums[kind].at[at(kind, lead, side)], seconds[kind].at[at(kind, (), side)],
                    second_sem.at[kind], sem, to)

    def chunk(k):
        return lambda kind, lead, side: index(kind, lead, side, k)

    def span(k, n):
        def at(kind, lead, side):
            if kind == QO_:
                return (pl.ds(k, n),) + lead + (pl.ds(HALF_R * side, HALF_R),)
            half, step = ((HALF_R, SUB), None, (HALF_DC, D_STEP))[kind]
            return lead + (pl.ds(half * side + step * k, step * n),)
        return at

    def opened(i):
        side, stays = PARTS[i]
        lead = (((every, 1 - x), (every, x)), ((1 - y, every), (y, every)))[side][stays]
        return send(stage.at[(side,) + lead], peer_u.at[index(U_, lead, side, 0)],
                    push_sem.at[U_], open_sem.at[side] if stays else peer_ring(U_, side, 0), mate)

    def own_ring(kind, side, k):
        return own_sem.at[side, lax.rem(kind * STEPS + k, SLOTS)]

    def peer_ring(kind, side, k):
        return peer_sem.at[side, lax.rem(kind * STEPS + k, 2 * SLOTS)]

    def load(kind, k, side, away):
        if away:
            dst, sem, c = peers[kind], peer_ring(kind, side, k), 1 - core
            copy = lambda a, b: send(a, b, push_sem.at[kind], sem, mate)
        else:
            dst, sem, c = owns[kind], own_ring(kind, side, k), core
            copy = lambda a, b: pltpu.make_async_copy(a, b, sem)
        if kind == U_:
            at = index(kind, (), side, k)
            return [(None, copy(gu.at[(every, every, c) + at], dst.at[(every, every) + at]))]
        if kind == D_:
            at = index(kind, (), side, k)
            return [(None, copy(gd.at[at + (pl.ds(pl.multiple_of(DR * (2 * b + c), LANE), DR),)],
                                dst.at[(b // 2, b % 2) + at])) for b in range(4)]
        slot = dst.at[k if away else lax.rem(k, SLOTS)]
        rest = LANE - Q_LEFT
        at_q = pl.multiple_of(LANE * jnp.minimum(k, Q_FULL - 1), LANE)
        at_o = pl.multiple_of(rest + LANE * jnp.maximum(k - Q_FULL - 1, 0), SUB)
        return [(k < Q_FULL, copy(gq.at[pl.ds(at_q, LANE)], slot)),
                (k == Q_FULL, copy(gq.at[pl.ds(Q_FULL * LANE, Q_LEFT)], slot.at[pl.ds(0, Q_LEFT)])),
                (k == Q_FULL, copy(go.at[pl.ds(0, rest)], slot.at[pl.ds(Q_LEFT, rest)])),
                (k > Q_FULL, copy(go.at[pl.ds(at_o, LANE)], slot))]

    def start_kind(kind, k, away):
        for side in range(1 if kind == QO_ else 2):
            for cond, copy in load(kind, k, side, away):
                if cond is None:
                    copy.start()
                else:
                    pl.when(cond)(copy.start)

    def start_loads(step, away):
        for kind in range(3):
            k = step - kind * STEPS
            pl.when(jnp.logical_and(k >= 0, k < STEPS))(lambda kind=kind, k=k: start_kind(kind, k, away))

    def loaded(kind, side, k):
        if kind == QO_:
            here, there = own_qo.at[lax.rem(k, SLOTS)], peer_qo.at[k]
        else:
            at = index(kind, (every, every), side, k)
            here, there = owns[kind].at[at], peers[kind].at[at]
        pltpu.make_async_copy(here, here, own_ring(kind, side, k)).wait()
        send(there, there, push_sem.at[kind], peer_ring(kind, side, k), mate).wait_recv()

    smalls = [(vrq, r_q), (vro, r_o), (vru, r_u), (vrd, r_d),
              (vcq, c_q), (vco, c_o), (vcu, c_u), (vcd, c_d), (vv, vv_in)]
    spare = [stat_send.at[i] for i in range(6)] + [second_sem.at[i] for i in range(3)] + [vec_send.at[2]]
    small_copies = [pltpu.make_async_copy(a, b, sem) for (a, b), sem in zip(smalls, spare)]
    vec_copy = pltpu.make_async_copy(gv, vec_own, vec_send.at[0])

    staged = [pltpu.make_async_copy(gu.at[(every, every, 1 - core) + index(U_, (), side, 0)],
                                    stage.at[side], push_sem.at[(QO_, D_)[side]]) for side in range(2)]
    for copy in staged:
        copy.start()
    start_kind(U_, 0, False)
    barrier = pltpu.get_barrier_semaphore()

    def signal(sem, to):
        pl.semaphore_signal(sem, inc=1, device_id=to, device_id_type=MESH)

    def signal_z(sem):
        pl.when(z > 0)(lambda: signal(sem, {"tp": z - 1}))
        pl.when(z < TP - 1)(lambda: signal(sem, {"tp": z + 1}))

    beside = jnp.where(z > 0, 1, 0) + jnp.where(z < TP - 1, 1, 0)
    near = (mate, across_x, across_y)
    for to in near:
        signal(barrier, to)
    signal_z(barrier)
    pl.semaphore_wait(barrier, len(near) + beside)

    for copy in staged:
        copy.wait()
    for i, (side, part) in enumerate(PARTS):
        opened(i).start()
    vec_copy.start()
    for copy in small_copies:
        copy.start()
    vec_core = send(vec_own, vec_in.at[0], vec_send.at[0], vec_recv.at[0], mate)
    vec_x = send(vec_mid.at[0], vec_in.at[1], vec_send.at[1], vec_recv.at[1], across_x)
    vec_y = send(vec_mid.at[1], vec_in.at[2], vec_send.at[2], vec_recv.at[2], across_y)

    def turn(k, which):
        slot = lax.rem(k, SLOTS)
        for tile in range(STEPS):
            lo = LANE * tile
            cuts = [(b, max(lo, R * (2 * b + which)), min(lo + LANE, R * (2 * b + which) + R)) for b in range(4)]
            cuts = [cut for cut in cuts if cut[1] < cut[2]]
            if cuts:
                at = (every, pl.ds(lo, LANE))
                turned = (own_qo[(slot,) + at] + peer_qo[(k,) + at]).T
                for b, start, stop in cuts:
                    first_row = start - R * (2 * b + which)
                    s_qo[k, b // 2, b % 2, pl.ds(first_row, stop - start), :] = turned[start - lo:stop - lo]

    def stage1(kind):
        def body(k, _):
            start_loads(k + kind * STEPS + LOOK, False)
            start_loads(k + kind * STEPS + LOOK, True)
            if kind == QO_:
                loaded(kind, 0, k)
                for which in range(2):
                    pl.when(core == which)(lambda which=which: turn(k, which))
            for side in range(2):
                if kind != QO_:
                    loaded(kind, side, k)
                    for b in range(4):
                        at = index(kind, (b // 2, b % 2), side, k)
                        owns[kind][at] = owns[kind][at] + peers[kind][at]
                first(kind, side, chunk(k), a_sem.at[kind, side, k // BATCH]).start()
            return _
        return body

    for side in range(2):
        at = index(U_, (every, every), side, 0)
        pltpu.make_async_copy(own_u.at[at], own_u.at[at], own_ring(U_, side, 0)).wait()
    for i, (side, stays) in enumerate(PARTS):
        opened(i).wait_recv()
        for b in range(2):
            lead = (((b, 1 - x), (b, x)), ((1 - y, b), (y, b)))[side][stays]
            at = index(U_, lead, side, 0)
            own_u[at] = own_u[at] + peer_u[at]
        if not stays:
            first(U_, side, chunk(0), a_sem.at[U_, side, 0]).start()
            for step in OPENING[side]:
                start_kind(U_, step, False)
                start_kind(U_, step, True)
    vec_copy.wait()
    vec_core.start()
    lax.fori_loop(1, STEPS, stage1(U_), 0)
    vec_core.wait_recv()
    vec_mid[0] = vec_own[...] + vec_in[0]
    vec_x.start()
    for kind in (QO_, D_):
        lax.fori_loop(0, STEPS, stage1(kind), 0)

    for copy in small_copies:
        copy.wait()
    kept = [(wq, wq_out), (wo, wo_out), (wu, wu_out), (wd, wd_out), (wv, wv_out),
            (mq, mq_out), (mo, mo_out), (mu, mu_out), (md, md_out), (mv, mv_out)]
    kept = [pltpu.make_async_copy(a, b, sem) for (a, b), sem in zip(kept, spare)]
    for copy in kept:
        copy.start()

    for ref in (cs_qo, cs_u, rs_d, rp_acc, rpd_acc, p_q, p_o):
        ref[...] = jnp.zeros_like(ref)
    old = to_tiles(r_q[...], 0) + to_tiles(r_o[...], ROW_TILES) + to_tiles(r_u[...], 2 * ROW_TILES)
    rp_old[...] = old
    rpd_old[...] = to_tiles(c_d[...], 0)
    lane = lanes((SUB, LANE))
    lane1 = lanes((1, LANE))
    masks = [jnp.logical_and(lane >= ROW_TILES * m, lane < ROW_TILES * (m + 1)) for m in range(3)]
    old_sums = [total(jnp.where(masks[m], old, 0.0)) for m in range(3)] + [total(r_d[...])]

    for copy in kept:
        copy.wait()

    for i, to in enumerate(near):
        signal(round_sem.at[i], to)
        pl.semaphore_wait(round_sem.at[i], 1)
    for i in range(len(near), len(near) + TP - 2):
        signal_z(round_sem.at[i])
        pl.semaphore_wait(round_sem.at[i], beside)

    def stage2(kind):
        for g, (k0, n) in enumerate(BATCHES):
            for side in range(2):
                first(kind, side, span(k0, n), a_sem.at[kind, side, g]).wait_recv()
                lead, mine = (((1 - y, x), 1 - y), ((y, 1 - x), 1 - x))[side]

                def add(k, _):
                    at = index(kind, lead, side, k)
                    sums[kind][at] = sums[kind][at] + firsts[kind][index(kind, (mine,), side, k)]
                    return _

                lax.fori_loop(k0, k0 + n, add, 0)
            for b, (k1, m) in enumerate(SECOND[kind]):
                if k0 <= k1 < k0 + n:
                    for side in range(2):
                        second(kind, side, span(k1, m), b_sem.at[side, SECOND_AT[kind] + b]).start()

    for kind in (U_, QO_):
        stage2(kind)
    vec_x.wait_recv()
    vec_mid[1] = vec_mid[0] + vec_in[1]
    vec_y.start()
    stage2(D_)

    def finished(kind, side, k):
        return (sums[kind][index(kind, (y, x), side, k)]
                + firsts[kind][index(kind, ((y, x)[side],), side, k)]
                + seconds[kind][index(kind, (), side, k)])

    def stage3_u(side, k):
        full = finished(U_, side, k)
        hu[index(U_, (), side, k)] = full
        sq = full * full
        cs_u[...] += sq
        row = jnp.sum(sq, axis=1, keepdims=True)
        rp_acc[...] = jnp.where(lane == 2 * ROW_TILES + STEPS * side + k, row, rp_acc[...])

    def stage3_qo(side, k):
        rows = pl.ds(HALF_R * side, HALF_R)
        full = finished(QO_, side, k)
        hqo[rows, pl.ds(pl.multiple_of(LANE * k, LANE), LANE)] = full
        sq = full * full
        in_q = lanes(sq.shape) + LANE * k < COLS[0]
        p_q[rows, :] += jnp.where(in_q, sq, 0.0)
        p_o[rows, :] += jnp.where(in_q, 0.0, sq)
        part = sq[:SUB]
        for t in range(1, STEPS):
            part = part + sq[SUB * t:SUB * t + SUB]
        cs_qo[k] += part

    def stage3_d(side, k):
        full = finished(D_, side, k)
        hd[index(D_, (), side, k)] = full
        sq = full * full
        both = rpd_acc[...]
        for t in range(D_STEP // SUB):
            part = sq[SUB * t:SUB * t + SUB]
            rs_d[...] += part
            col = jnp.sum(part, axis=1, keepdims=True)
            at = (HALF_DC * side + D_STEP * k) // SUB + t
            both = jnp.where(lane == at, col, both)
        rpd_acc[...] = both

    def stage3(kind, take):
        for b, (k0, n) in enumerate(SECOND[kind]):
            for side in range(2):
                second(kind, side, span(k0, n), b_sem.at[side, SECOND_AT[kind] + b]).wait_recv()
                lax.fori_loop(k0, k0 + n, lambda k, _: [take(side, k), _][1], 0)

    def to_group(buf, at, i, n, axis, here):
        for d in range(1, n):
            send(buf.at[at], buf.at[at], stat_send.at[i], stat_recv.at[i],
                 {axis: lax.rem(here + d, n)}).start()

    def to_all(buf, i):
        for to in others:
            send(buf.at[linear], buf.at[linear], stat_send.at[i], stat_recv.at[i], to).start()

    def spread(buf, i, n):
        part = buf.at[pl.ds(0, n - 1)]
        return send(part, part, stat_send.at[i], stat_recv.at[i], mate)

    def gathered(buf, i, n):
        spread(buf, i, n).wait_recv()
        out = buf[0]
        for d in range(1, n):
            out = out + buf[d]
        return out

    stage3(U_, stage3_u)
    stage3(QO_, stage3_qo)
    vec_y.wait_recv()
    vec = vec_mid[1] + vec_in[2]
    hv[...] = vec
    rp = rp_acc[...]
    for t in range(ROW_TILES):
        for m, ref in enumerate((p_q, p_o)):
            row = jnp.sum(ref[pl.ds(SUB * t, SUB), :], axis=1, keepdims=True)
            rp = jnp.where(lane == ROW_TILES * m + t, row, rp)
    rp_all[z] = rp
    cs = [jnp.sum(cs_qo[k], axis=0, keepdims=True) for k in range(STEPS)]
    cs.append(jnp.sum(cs_u[...], axis=0, keepdims=True))
    cs_all[me] = jnp.concatenate(cs + [jnp.zeros((1, WIDE - QO - UP), F32)], axis=1)
    to_group(rp_all, z, 0, TP, "tp", z)
    to_group(cs_all, me, 1, FSDP, "fsdp", me)
    pack = jnp.where(lane1 == VEC_AT, jnp.sum(vec * vec, axis=1, keepdims=True), 0.0)
    for m in range(4):
        pack = jnp.where(lane1 == VR_AT + m, old_sums[m], pack)
    for m in range(3):
        pack = jnp.where(lane1 == m, total(jnp.where(masks[m], rp, 0.0)), pack)

    stage3(D_, stage3_d)
    rs = rs_d[...]
    s_all[linear] = jnp.where(lane1 == 3, total(rs), pack)
    to_all(s_all, 4)
    rsd_all[z] = jnp.sum(rs, axis=0, keepdims=True)
    to_group(rsd_all, z, 2, TP, "tp", z)
    rpd_all[me] = rpd_acc[...]
    to_group(rpd_all, me, 3, FSDP, "fsdp", me)

    vc_old = jnp.concatenate([c_q[...], c_o[...], c_u[...], jnp.ones((1, WIDE - QO - UP), F32)], axis=1)
    rp = gathered(rp_all, 0, TP)
    cs = gathered(cs_all, 1, FSDP)
    rsd = gathered(rsd_all, 2, TP)
    rpd = gathered(rpd_all, 3, FSDP)
    pack = gathered(s_all, 4, DEVICES)
    squares = [pick(pack, m) for m in range(4)]
    norm = jnp.sqrt((squares[0] + squares[1]) + (squares[2] + squares[3]) + pick(pack, VEC_AT) / FSDP)
    clip = jnp.minimum(1.0, 1.0 / norm)

    def clipped(v):
        return jnp.where(clip > 0.0, (v * clip) * clip, 0.0)

    means = []
    for m in range(4):
        r_all, c_all = float(ROWS[m] * FSDP), float(COLS[m] * TP)
        means.append(KEEP * (pick(pack, VR_AT + m) / (TP * r_all))
                     + MIX * (clipped(squares[m]) / (r_all * c_all) + EPSILON))
    mean_rp = jnp.where(masks[0], means[0], jnp.where(masks[1], means[1], means[2]))
    wide = jnp.where(masks[0], float(COLS[0] * TP), jnp.where(masks[1], float(COLS[1] * TP), float(COLS[2] * TP)))
    row_new = KEEP * rp_old[...] + MIX * (clipped(rp) / wide + EPSILON)
    row_sq = mean_rp / row_new
    rowd_new = KEEP * r_d[...] + MIX * (clipped(rsd) / float(DC * TP) + EPSILON)
    rowd_buf[...] = clip * jnp.sqrt(means[3] / rowd_new)
    col_new = KEEP * vc_old + MIX * (clipped(cs) / float(R * FSDP) + EPSILON)
    col_buf[...] = clip / jnp.sqrt(col_new)
    cold_new = KEEP * rpd_old[...] + MIX * (clipped(rpd) / float(DR * FSDP) + EPSILON)
    cold_sq = 1.0 / cold_new

    def tile(ref, j):
        return jnp.broadcast_to(ref[:, pl.ds(LANE * j, LANE)], (SUB, LANE))

    zero = jnp.zeros((SUB, LANE), F32)
    acc = [zero] * 4
    in_q = lane < Q_LEFT
    col_t = [tile(col_buf, j) for j in range(STEPS + UP // LANE)]
    for t in range(ROW_TILES):
        rows = pl.ds(SUB * t, SUB)
        part = [zero] * 3
        for j in range(STEPS):
            u = hqo[rows, pl.ds(LANE * j, LANE)] * col_t[j]
            u = u * u
            if j == Q_FULL:
                part[0] = part[0] + jnp.where(in_q, u, 0.0)
                part[1] = part[1] + jnp.where(in_q, 0.0, u)
            else:
                part[j // Q_FULL] = part[j // Q_FULL] + u
        for j in range(UP // LANE):
            u = hu[rows, pl.ds(LANE * j, LANE)] * col_t[STEPS + j]
            part[2] = part[2] + u * u
        for m in range(3):
            acc[m] = acc[m] + part[m] * across(row_sq, ROW_TILES * m + t)
    rowd_t = [tile(rowd_buf, j) for j in range(DR // LANE)]
    for t in range(D_TILES):
        part = zero
        for j in range(DR // LANE):
            u = hd[pl.ds(SUB * t, SUB), pl.ds(LANE * j, LANE)] * rowd_t[j]
            part = part + u * u
        acc[3] = acc[3] + part * across(cold_sq, t)
    vec = hv[...] * clip
    v_new = KEEP * vv_in[...] + MIX * (vec * vec + EPSILON)
    vec = vec / jnp.sqrt(v_new)
    pack = jnp.where(lane1 == VEC_AT, jnp.sum(vec * vec, axis=1, keepdims=True), 0.0)
    for m in range(4):
        pack = jnp.where(lane1 == m, total(acc[m]), pack)
    u_all[linear] = pack
    to_all(u_all, 5)

    vv_new[...] = v_new
    hv[...] = vec
    row = jnp.sqrt(row_sq)
    cold = jnp.sqrt(cold_sq)
    for t in range(ROW_TILES):
        rows = pl.ds(SUB * t, SUB)
        scale = [across(row, ROW_TILES * m + t) for m in range(3)]
        mixed = jnp.where(in_q, scale[0], scale[1])
        for j in range(STEPS):
            at = pl.ds(LANE * j, LANE)
            hqo[rows, at] = hqo[rows, at] * col_t[j] * (mixed if j == Q_FULL else scale[j // Q_FULL])
        for j in range(UP // LANE):
            at = pl.ds(LANE * j, LANE)
            hu[rows, at] = hu[rows, at] * col_t[STEPS + j] * scale[2]
    for t in range(D_TILES):
        rows = pl.ds(SUB * t, SUB)
        scale = across(cold, t)
        for j in range(DR // LANE):
            at = pl.ds(LANE * j, LANE)
            hd[rows, at] = hd[rows, at] * rowd_t[j] * scale
    for m, ref in enumerate((n_rq, n_ro, n_ru)):
        ref[...] = from_tiles(row_new, ROW_TILES * m, R)
    n_rd[...] = rowd_new
    n_cq[...] = col_new[:, :COLS[0]]
    n_co[...] = col_new[:, COLS[0]:QO]
    n_cu[...] = col_new[:, QO:QO + UP]
    n_cd[...] = from_tiles(cold_new, 0, DC)

    for kind in range(3):
        send(peers[kind], peers[kind], push_sem.at[kind], peer_sem.at[0, 0], mate).wait_send()
        send(firsts[kind], firsts[kind], first_sem.at[kind], a_sem.at[kind, 0, 0], mate).wait_send()
        send(seconds[kind], seconds[kind], second_sem.at[kind], b_sem.at[0, 0], mate).wait_send()
    for copy in (vec_core, vec_x, vec_y):
        copy.wait_send()
    groups = ((rp_all, TP), (cs_all, FSDP), (rsd_all, TP), (rpd_all, FSDP), (s_all, DEVICES), (u_all, DEVICES))
    for i, (buf, n) in enumerate(groups):
        if i < len(groups) - 1:
            spread(buf, i, n).wait_send()

    pack = gathered(u_all, len(groups) - 1, DEVICES)
    count = jnp.full((1, LANE), float(VEC * TP * FSDP), F32)
    for m in range(4):
        count = jnp.where(lane1 == m, float(ROWS[m] * FSDP * COLS[m] * TP), count)
    inv_out[...] = 1.0 / jnp.maximum(1.0, jnp.sqrt(pack / count))
    spread(u_all, len(groups) - 1, DEVICES).wait_send()


PIECES = ((3, 0, 96), (3, 96, 128), (3, 224, 128), (2, 0, 64), (2, 64, 64), (2, 128, 48), (0, 0, 96), (0, 96, 80), (1, 0, R))
HELD = (ROWS[:3] + (DC,), COLS[:3] + (DR,))
GROUP = 16


def update_kernel(*refs):
    (hqo, hu, hd, hv, inv, wq, wo, wu, wd, wv, mq, mo, mu, md, mv,
     vrq, vro, vru, vrd, vcq, vco, vcu, vcd, vv,
     wq_out, wo_out, wu_out, wd_out, wv_out, mq_out, mo_out, mu_out, md_out, mv_out,
     vrq_out, vcq_out, vro_out, vco_out, vru_out, vcu_out, vrd_out, vcd_out, vv_out,
     bwq, bwo, bwu, bwd, bmq, bmo, bmu, bmd, bwv, bmv, out_sem, small_sem) = refs
    held = ((hqo, 0), (hqo, COLS[0]), (hu, 0), (hd, 0))
    w_in, m_in = (wq, wo, wu, wd), (mq, mo, mu, md)
    w_buf, m_buf = (bwq, bwo, bwu, bwd), (bmq, bmo, bmu, bmd)
    w_out, m_out = (wq_out, wo_out, wu_out, wd_out), (mq_out, mo_out, mu_out, md_out)

    def finish(u, w, m):
        m_new = (MOMENTUM * m.astype(F32) + (1.0 - MOMENTUM) * u).astype(BF16)
        return w - LEARN_RATE * (m_new.astype(F32) + WEIGHT_DECAY * w), m_new

    passed = ((vrq, vrq_out), (vro, vro_out), (vru, vru_out), (vrd, vrd_out),
              (vcq, vcq_out), (vco, vco_out), (vcu, vcu_out), (vcd, vcd_out), (vv, vv_out))
    stores = [pltpu.make_async_copy(src, dst, small_sem.at[i]) for i, (src, dst) in enumerate(passed)]
    w_new, m_new = finish(hv[...] * inv[:, VEC_AT:VEC_AT + 1], wv[...], mv[...])
    bwv[...] = w_new
    bmv[...] = m_new
    stores.append(pltpu.make_async_copy(bwv, wv_out, small_sem.at[len(passed)]))
    stores.append(pltpu.make_async_copy(bmv, mv_out, small_sem.at[len(passed) + 1]))
    for copy in stores:
        copy.start()
    for m, r0, n in PIECES:
        scale = inv[:, m:m + 1]
        buf, c0 = held[m]

        for k in range(n // GROUP):
            rows = pl.ds(r0 + GROUP * k, GROUP)
            u = buf[rows, pl.ds(c0 // LANE * LANE, c0 % LANE + HELD[1][m])][:, c0 % LANE:]
            w_new, m_new = finish(u * scale, w_in[m][rows, :], m_in[m][rows, :])
            w_buf[m][rows, :] = w_new
            m_buf[m][rows, :] = m_new
        rows = pl.ds(r0, n)
        for j, (src, dst) in enumerate(((w_buf, w_out), (m_buf, m_out))):
            pltpu.make_async_copy(src[m].at[rows, :], dst[m].at[rows, :], out_sem.at[m, j]).start()
    for m in range(4):
        for j, (src, dst) in enumerate(((w_buf, w_out), (m_buf, m_out))):
            stores.append(pltpu.make_async_copy(src[m], dst[m], out_sem.at[m, j]))
    for copy in stores:
        copy.wait()


IN_HBM = pl.BlockSpec(memory_space=pltpu.HBM)
IN_VMEM = pl.BlockSpec(memory_space=pltpu.VMEM)
MIB = 1024 * 1024


def f32(*shape):
    return jax.ShapeDtypeStruct(shape, F32)


def vmem(*shape):
    return pltpu.VMEM(shape, F32)


def local_step(g_qkv, g_out, g_up, g_down, g_vec, w_qkv, w_out, w_up, w_down, w_vec,
               m_qkv, m_out, m_up, m_down, m_vec, vr_qkv, vc_qkv, vr_out, vc_out,
               vr_up, vc_up, vr_down, vc_down, v_vec):
    dma = pltpu.SemaphoreType.DMA
    rows_shapes = [(1, n) for n in ROWS]
    cols_shapes = [(1, n) for n in COLS]
    h_shapes = [(R, QO), (R, UP), (DC, DR)]
    wide_u, wide_d, vec = (R, UP), (DC, DR), (1, VEC)
    shapes = [
        (2, 2, 2, SUB, UP), (SLOTS, LANE, QO), (2, 2) + wide_u, (2, 2) + wide_d,
        (STEPS, LANE, QO), (2, 2) + wide_u, (2, 2) + wide_d, (STEPS, 2, 2, R, LANE),
        (STEPS, 2, R, LANE), (2,) + wide_u, (2,) + wide_d, (STEPS, R, LANE), wide_u, wide_d,
        vec, (3,) + vec, (2,) + vec, vec] + rows_shapes + cols_shapes + [
        (R, LANE), (R, LANE), (STEPS, SUB, LANE), (SUB, UP), (SUB, DR)] + [(SUB, LANE)] * 4 + [
        (1, WIDE), (1, DR),
        (FSDP, 1, WIDE), (TP, SUB, LANE), (TP, 1, DR), (FSDP, SUB, LANE),
        (DEVICES, 1, LANE), (DEVICES, 1, LANE)]
    sems = [(2, SLOTS), (2, 2 * SLOTS), (3,), (3,), (3,), (3, 2, len(BATCHES)),
            (2, SECOND_AT[-1] + len(SECOND[-1])), (3,), (3,), (6,), (6,), (2,)]
    ws = [w_qkv[0], w_out[0], w_up[0], w_down[0].T, w_vec]
    ms = [m_qkv[0], m_out[0], m_up[0], m_down[0].T, m_vec]
    mats = list(zip(*HELD))
    state = [f32(*s) for s in mats + [vec]] + [jax.ShapeDtypeStruct(s, BF16) for s in mats + [vec]]
    inputs = [pltpu.with_memory_space_constraint(a, pltpu.HBM)
              for a in (g_qkv[0, 0].T, g_out[0, 0].T, g_up.reshape(2, 2, 2, R, UP), g_down[0, 0].T, g_vec[0],
                        vr_qkv, vr_out, vr_up, vr_down, vc_qkv, vc_out, vc_up, vc_down, v_vec, *ws, *ms)]
    reduced = pl.pallas_call(
        reduce_kernel,
        name="reduce_and_scale",
        out_shape=([f32(*s) for s in h_shapes + [vec, (1, LANE)]] + state
                   + [f32(*s) for s in rows_shapes + cols_shapes + [vec]]),
        in_specs=[IN_HBM] * 24,
        out_specs=[IN_VMEM] * 24,
        scratch_shapes=[vmem(*s) for s in shapes] + [dma(s) for s in sems] + [pltpu.SemaphoreType.REGULAR((TP + 1,))],
        compiler_params=pltpu.CompilerParams(
            collective_id=0, has_side_effects=True, vmem_limit_bytes=A_MIB * MIB),
    )(*inputs)

    outs = pl.pallas_call(
        update_kernel,
        name="update",
        out_shape=(state + [f32(*s) for m in range(4) for s in (rows_shapes[m], cols_shapes[m])] + [f32(*vec)]),
        in_specs=[IN_VMEM] * 24,
        out_specs=[IN_HBM] * 19,
        scratch_shapes=([vmem(*s) for s in mats] + [pltpu.VMEM(s, BF16) for s in mats]
                        + [vmem(*vec), pltpu.VMEM(vec, BF16), dma((4, 2)), dma((11,))]),
        compiler_params=pltpu.CompilerParams(vmem_limit_bytes=B_MIB * MIB),
    )(*reduced)
    outs = list(outs)
    for i in range(10):
        if i % 5 == 3:
            outs[i] = outs[i].T
        if i % 5 != 4:
            outs[i] = outs[i][None]
    return tuple(outs)


A_MIB, B_MIB = 46, 12


def solution(mesh):
    grad_spec = P("fsdp", None, None, "tp")
    vec_grad_spec = P("fsdp", None, "tp")
    mat_spec = P(None, "fsdp", "tp")
    vec_spec = P(None, "tp")
    row_spec = P(None, "fsdp")
    col_spec = P(None, "tp")
    state_specs = ((mat_spec,) * 4 + (vec_spec,) + (mat_spec,) * 4 + (vec_spec,)
                   + (row_spec, col_spec) * 4 + (vec_spec,))
    arg_specs = (grad_spec,) * 4 + (vec_grad_spec,) + state_specs
    return jax.shard_map(local_step, mesh=mesh, in_specs=arg_specs, out_specs=state_specs, check_vma=False)
```

```python
import jax
import jax.numpy as jnp
from jax import lax
from jax.experimental import pallas as pl
from jax.experimental.pallas import tpu as pltpu
from jax.sharding import PartitionSpec as P

TRAIN_STEP = 3
LEARN_RATE = 0.0008
WEIGHT_DECAY = 0.03
MOMENTUM = 0.9
EPSILON = 1e-30
BETA_TWO = 1.0 - TRAIN_STEP ** -0.8
KEEP, MIX = BETA_TWO, 1.0 - BETA_TWO

F32 = jnp.float32
BF16 = jnp.bfloat16
MESH = pl.DeviceIdType.MESH
HIGHEST = lax.Precision.HIGHEST
TP, FSDP, DEVICES = 4, 8, 32
SUB, LANE = 8, 128

ROWS = (176, 176, 176, 768)
COLS = (1056, 352, 1536, 352)
VEC = 4704
R, QO, UP, DR, DC = ROWS[0], COLS[0] + COLS[1], COLS[2], ROWS[3], COLS[3]
HALF_R, HALF_DC = R // 2, DC // 2
STEPS = QO // LANE
D_STEP = HALF_DC // STEPS
Q_FULL = COLS[0] // LANE
Q_LEFT = COLS[0] - Q_FULL * LANE
ROW_TILES = R // SUB
D_TILES = DC // SUB
WIDE = -(-(QO + UP) // (SUB * LANE)) * SUB * LANE
LOOK, SLOTS = 2, 3
OPENING = ((1,), (2,))
U_, QO_, D_ = 0, 1, 2
BATCH = 11
BATCHES = ((0, 11),)
SECOND = (BATCHES, BATCHES, ((0, 6), (6, 4), (10, 1)))
SECOND_AT = (0, 1, 2)
PARTS = ((0, 0), (1, 0), (0, 1), (1, 1))
VR_AT, VEC_AT = 4, 8


def lanes(shape):
    return lax.broadcasted_iota(jnp.int32, shape, len(shape) - 1)


def sublanes(shape):
    return lax.broadcasted_iota(jnp.int32, shape, len(shape) - 2)


def total(x):
    return jnp.sum(jnp.sum(x, axis=1, keepdims=True), axis=0, keepdims=True)


def pick(x, lane):
    return jnp.sum(jnp.where(lanes(x.shape) == lane, x, 0.0), axis=1, keepdims=True)


def dot(a, b):
    return lax.dot_general(a, b, (((1,), (0,)), ((), ())), precision=HIGHEST, preferred_element_type=F32)


def own_sublane(n):
    return lanes((SUB, n)) % SUB == sublanes((SUB, n))


def to_tiles(row, at):
    n = row.shape[1]
    chosen = (sublanes((n, LANE)) // SUB + at == lanes((n, LANE))).astype(F32)
    return dot(jnp.where(own_sublane(n), row, 0.0), chosen)


def from_tiles(tiles, at, n):
    chosen = (lanes((LANE, n)) // SUB + at == sublanes((LANE, n))).astype(F32)
    return jnp.sum(jnp.where(own_sublane(n), dot(tiles, chosen), 0.0), axis=0, keepdims=True)


def across(tiles, t):
    return jnp.broadcast_to(tiles[:, t:t + 1], (SUB, LANE))


def reduce_kernel(*refs):
    (gq, go, gu, gd, gv, vrq, vro, vru, vrd, vcq, vco, vcu, vcd, vv,
     wq, wo, wu, wd, wv, mq, mo, mu, md, mv,
     hqo, hu, hd, hv, inv_out,
     wq_out, wo_out, wu_out, wd_out, wv_out, mq_out, mo_out, mu_out, md_out, mv_out,
     n_rq, n_ro, n_ru, n_rd, n_cq, n_co, n_cu, n_cd, vv_new,
     stage, own_qo, own_u, own_d, peer_qo, peer_u, peer_d, s_qo,
     a_qo, a_u, a_d, b_qo, b_u, b_d,
     vec_own, vec_in, vec_mid, vv_in,
     r_q, r_o, r_u, r_d, c_q, c_o, c_u, c_d,
     p_q, p_o, cs_qo, cs_u, rs_d, rp_acc, rpd_acc, rp_old, rpd_old, col_buf, rowd_buf,
     cs_all, rp_all, rsd_all, rpd_all, s_all, u_all,
     own_sem, peer_sem, push_sem, first_sem, second_sem, a_sem, b_sem,
     vec_send, vec_recv, stat_send, stat_recv, open_sem, round_sem) = refs

    me = lax.axis_index("fsdp")
    z = lax.axis_index("tp")
    core = lax.rem(me, 2)
    x = lax.rem(me // 2, 2)
    y = me // 4
    linear = z * FSDP + me
    mate = {"fsdp": me + 1 - 2 * core}
    across_x = {"fsdp": me + 2 - 4 * x}
    across_y = {"fsdp": me + 4 - 8 * y}
    every = slice(None)

    def flip(v, bits):
        for bit in range(3):
            step = 2 ** bit
            if bits & step:
                v = v + step - 2 * step * lax.rem(v // step, 2)
        return v

    others = [{"tp": flip(z, a), "fsdp": flip(me, b)} for a in range(TP - 1, -1, -1)
              for b in range(FSDP - 1, -1, -1) if a + b > 0]

    owns, peers = (own_u, own_qo, own_d), (peer_u, peer_qo, peer_d)
    sums, firsts, seconds = (own_u, s_qo, own_d), (a_u, a_qo, a_d), (b_u, b_qo, b_d)

    def send(src, dst, ssem, rsem, to):
        return pltpu.make_async_remote_copy(
            src_ref=src, dst_ref=dst, send_sem=ssem, recv_sem=rsem,
            device_id=to, device_id_type=MESH)

    def index(kind, lead, side, k):
        if kind == QO_:
            return (k,) + lead + (pl.ds(HALF_R * side, HALF_R),)
        if kind == U_:
            return lead + (pl.ds(pl.multiple_of(HALF_R * side + SUB * k, SUB), SUB),)
        return lead + (pl.ds(pl.multiple_of(HALF_DC * side + D_STEP * k, SUB), D_STEP),)

    def first(kind, side, at, sem):
        lead, to = (((every, 1 - x), across_x), ((1 - y, every), across_y))[side]
        return send(sums[kind].at[at(kind, lead, side)], firsts[kind].at[at(kind, (every,), side)],
                    first_sem.at[kind], sem, to)

    def second(kind, side, at, sem):
        lead, to = (((1 - y, x), across_y), ((y, 1 - x), across_x))[side]
        return send(sums[kind].at[at(kind, lead, side)], seconds[kind].at[at(kind, (), side)],
                    second_sem.at[kind], sem, to)

    def chunk(k):
        return lambda kind, lead, side: index(kind, lead, side, k)

    def span(k, n):
        def at(kind, lead, side):
            if kind == QO_:
                return (pl.ds(k, n),) + lead + (pl.ds(HALF_R * side, HALF_R),)
            half, step = ((HALF_R, SUB), None, (HALF_DC, D_STEP))[kind]
            return lead + (pl.ds(half * side + step * k, step * n),)
        return at

    def opened(i):
        side, stays = PARTS[i]
        lead = (((every, 1 - x), (every, x)), ((1 - y, every), (y, every)))[side][stays]
        return send(stage.at[(side,) + lead], peer_u.at[index(U_, lead, side, 0)],
                    push_sem.at[U_], open_sem.at[side] if stays else peer_ring(U_, side, 0), mate)

    def own_ring(kind, side, k):
        return own_sem.at[side, lax.rem(kind * STEPS + k, SLOTS)]

    def peer_ring(kind, side, k):
        return peer_sem.at[side, lax.rem(kind * STEPS + k, 2 * SLOTS)]

    def load(kind, k, side, away):
        if away:
            dst, sem, c = peers[kind], peer_ring(kind, side, k), 1 - core
            copy = lambda a, b: send(a, b, push_sem.at[kind], sem, mate)
        else:
            dst, sem, c = owns[kind], own_ring(kind, side, k), core
            copy = lambda a, b: pltpu.make_async_copy(a, b, sem)
        if kind == U_:
            at = index(kind, (), side, k)
            return [(None, copy(gu.at[(every, every, c) + at], dst.at[(every, every) + at]))]
        if kind == D_:
            at = index(kind, (), side, k)
            return [(None, copy(gd.at[at + (pl.ds(pl.multiple_of(DR * (2 * b + c), LANE), DR),)],
                                dst.at[(b // 2, b % 2) + at])) for b in range(4)]
        slot = dst.at[k if away else lax.rem(k, SLOTS)]
        rest = LANE - Q_LEFT
        at_q = pl.multiple_of(LANE * jnp.minimum(k, Q_FULL - 1), LANE)
        at_o = pl.multiple_of(rest + LANE * jnp.maximum(k - Q_FULL - 1, 0), SUB)
        return [(k < Q_FULL, copy(gq.at[pl.ds(at_q, LANE)], slot)),
                (k == Q_FULL, copy(gq.at[pl.ds(Q_FULL * LANE, Q_LEFT)], slot.at[pl.ds(0, Q_LEFT)])),
                (k == Q_FULL, copy(go.at[pl.ds(0, rest)], slot.at[pl.ds(Q_LEFT, rest)])),
                (k > Q_FULL, copy(go.at[pl.ds(at_o, LANE)], slot))]

    def start_kind(kind, k, away):
        for side in range(1 if kind == QO_ else 2):
            for cond, copy in load(kind, k, side, away):
                if cond is None:
                    copy.start()
                else:
                    pl.when(cond)(copy.start)

    def start_loads(step, away):
        for kind in range(3):
            k = step - kind * STEPS
            pl.when(jnp.logical_and(k >= 0, k < STEPS))(lambda kind=kind, k=k: start_kind(kind, k, away))

    def loaded(kind, side, k):
        if kind == QO_:
            here, there = own_qo.at[lax.rem(k, SLOTS)], peer_qo.at[k]
        else:
            at = index(kind, (every, every), side, k)
            here, there = owns[kind].at[at], peers[kind].at[at]
        pltpu.make_async_copy(here, here, own_ring(kind, side, k)).wait()
        send(there, there, push_sem.at[kind], peer_ring(kind, side, k), mate).wait_recv()

    smalls = [(vrq, r_q), (vro, r_o), (vru, r_u), (vrd, r_d),
              (vcq, c_q), (vco, c_o), (vcu, c_u), (vcd, c_d), (vv, vv_in)]
    spare = [stat_send.at[i] for i in range(6)] + [second_sem.at[i] for i in range(3)] + [vec_send.at[2]]
    small_copies = [pltpu.make_async_copy(a, b, sem) for (a, b), sem in zip(smalls, spare)]
    vec_copy = pltpu.make_async_copy(gv, vec_own, vec_send.at[0])

    staged = [pltpu.make_async_copy(gu.at[(every, every, 1 - core) + index(U_, (), side, 0)],
                                    stage.at[side], push_sem.at[(QO_, D_)[side]]) for side in range(2)]
    for copy in staged:
        copy.start()
    start_kind(U_, 0, False)
    barrier = pltpu.get_barrier_semaphore()

    def signal(sem, to):
        pl.semaphore_signal(sem, inc=1, device_id=to, device_id_type=MESH)

    def signal_z(sem):
        pl.when(z > 0)(lambda: signal(sem, {"tp": z - 1}))
        pl.when(z < TP - 1)(lambda: signal(sem, {"tp": z + 1}))

    beside = jnp.where(z > 0, 1, 0) + jnp.where(z < TP - 1, 1, 0)
    near = (mate, across_x, across_y)
    for to in near:
        signal(barrier, to)
    signal_z(barrier)
    pl.semaphore_wait(barrier, len(near) + beside)

    for copy in staged:
        copy.wait()
    for i, (side, part) in enumerate(PARTS):
        opened(i).start()
    vec_copy.start()
    for copy in small_copies:
        copy.start()
    vec_core = send(vec_own, vec_in.at[0], vec_send.at[0], vec_recv.at[0], mate)
    vec_x = send(vec_mid.at[0], vec_in.at[1], vec_send.at[1], vec_recv.at[1], across_x)
    vec_y = send(vec_mid.at[1], vec_in.at[2], vec_send.at[2], vec_recv.at[2], across_y)

    def turn(k, which):
        slot = lax.rem(k, SLOTS)
        for tile in range(STEPS):
            lo = LANE * tile
            cuts = [(b, max(lo, R * (2 * b + which)), min(lo + LANE, R * (2 * b + which) + R)) for b in range(4)]
            cuts = [cut for cut in cuts if cut[1] < cut[2]]
            if cuts:
                at = (every, pl.ds(lo, LANE))
                turned = (own_qo[(slot,) + at] + peer_qo[(k,) + at]).T
                for b, start, stop in cuts:
                    first_row = start - R * (2 * b + which)
                    s_qo[k, b // 2, b % 2, pl.ds(first_row, stop - start), :] = turned[start - lo:stop - lo]

    def stage1(kind):
        def body(k, _):
            start_loads(k + kind * STEPS + LOOK, False)
            start_loads(k + kind * STEPS + LOOK, True)
            if kind == QO_:
                loaded(kind, 0, k)
                for which in range(2):
                    pl.when(core == which)(lambda which=which: turn(k, which))
            for side in range(2):
                if kind != QO_:
                    loaded(kind, side, k)
                    for b in range(4):
                        at = index(kind, (b // 2, b % 2), side, k)
                        owns[kind][at] = owns[kind][at] + peers[kind][at]
                first(kind, side, chunk(k), a_sem.at[kind, side, k // BATCH]).start()
            return _
        return body

    for side in range(2):
        at = index(U_, (every, every), side, 0)
        pltpu.make_async_copy(own_u.at[at], own_u.at[at], own_ring(U_, side, 0)).wait()
    for i, (side, stays) in enumerate(PARTS):
        opened(i).wait_recv()
        for b in range(2):
            lead = (((b, 1 - x), (b, x)), ((1 - y, b), (y, b)))[side][stays]
            at = index(U_, lead, side, 0)
            own_u[at] = own_u[at] + peer_u[at]
        if not stays:
            first(U_, side, chunk(0), a_sem.at[U_, side, 0]).start()
            for step in OPENING[side]:
                start_kind(U_, step, False)
                start_kind(U_, step, True)
    vec_copy.wait()
    vec_core.start()
    lax.fori_loop(1, STEPS, stage1(U_), 0)
    vec_core.wait_recv()
    vec_mid[0] = vec_own[...] + vec_in[0]
    vec_x.start()
    for kind in (QO_, D_):
        lax.fori_loop(0, STEPS, stage1(kind), 0)

    for copy in small_copies:
        copy.wait()
    kept = [(wq, wq_out), (wo, wo_out), (wu, wu_out), (wd, wd_out), (wv, wv_out),
            (mq, mq_out), (mo, mo_out), (mu, mu_out), (md, md_out), (mv, mv_out)]
    kept = [pltpu.make_async_copy(a, b, sem) for (a, b), sem in zip(kept, spare)]
    for copy in kept:
        copy.start()

    for ref in (cs_qo, cs_u, rs_d, rp_acc, rpd_acc, p_q, p_o):
        ref[...] = jnp.zeros_like(ref)
    old = to_tiles(r_q[...], 0) + to_tiles(r_o[...], ROW_TILES) + to_tiles(r_u[...], 2 * ROW_TILES)
    rp_old[...] = old
    rpd_old[...] = to_tiles(c_d[...], 0)
    lane = lanes((SUB, LANE))
    lane1 = lanes((1, LANE))
    masks = [jnp.logical_and(lane >= ROW_TILES * m, lane < ROW_TILES * (m + 1)) for m in range(3)]
    old_sums = [total(jnp.where(masks[m], old, 0.0)) for m in range(3)] + [total(r_d[...])]

    for copy in kept:
        copy.wait()

    for i, to in enumerate(near):
        signal(round_sem.at[i], to)
        pl.semaphore_wait(round_sem.at[i], 1)
    for i in range(len(near), len(near) + TP - 2):
        signal_z(round_sem.at[i])
        pl.semaphore_wait(round_sem.at[i], beside)

    def stage2(kind):
        for g, (k0, n) in enumerate(BATCHES):
            for side in range(2):
                first(kind, side, span(k0, n), a_sem.at[kind, side, g]).wait_recv()
                lead, mine = (((1 - y, x), 1 - y), ((y, 1 - x), 1 - x))[side]

                def add(k, _):
                    at = index(kind, lead, side, k)
                    sums[kind][at] = sums[kind][at] + firsts[kind][index(kind, (mine,), side, k)]
                    return _

                lax.fori_loop(k0, k0 + n, add, 0)
            for b, (k1, m) in enumerate(SECOND[kind]):
                if k0 <= k1 < k0 + n:
                    for side in range(2):
                        second(kind, side, span(k1, m), b_sem.at[side, SECOND_AT[kind] + b]).start()

    for kind in (U_, QO_):
        stage2(kind)
    vec_x.wait_recv()
    vec_mid[1] = vec_mid[0] + vec_in[1]
    vec_y.start()
    stage2(D_)

    def finished(kind, side, k):
        return (sums[kind][index(kind, (y, x), side, k)]
                + firsts[kind][index(kind, ((y, x)[side],), side, k)]
                + seconds[kind][index(kind, (), side, k)])

    def stage3_u(side, k):
        full = finished(U_, side, k)
        hu[index(U_, (), side, k)] = full
        sq = full * full
        cs_u[...] += sq
        row = jnp.sum(sq, axis=1, keepdims=True)
        rp_acc[...] = jnp.where(lane == 2 * ROW_TILES + STEPS * side + k, row, rp_acc[...])

    def stage3_qo(side, k):
        rows = pl.ds(HALF_R * side, HALF_R)
        full = finished(QO_, side, k)
        hqo[rows, pl.ds(pl.multiple_of(LANE * k, LANE), LANE)] = full
        sq = full * full
        in_q = lanes(sq.shape) + LANE * k < COLS[0]
        p_q[rows, :] += jnp.where(in_q, sq, 0.0)
        p_o[rows, :] += jnp.where(in_q, 0.0, sq)
        part = sq[:SUB]
        for t in range(1, STEPS):
            part = part + sq[SUB * t:SUB * t + SUB]
        cs_qo[k] += part

    def stage3_d(side, k):
        full = finished(D_, side, k)
        hd[index(D_, (), side, k)] = full
        sq = full * full
        both = rpd_acc[...]
        for t in range(D_STEP // SUB):
            part = sq[SUB * t:SUB * t + SUB]
            rs_d[...] += part
            col = jnp.sum(part, axis=1, keepdims=True)
            at = (HALF_DC * side + D_STEP * k) // SUB + t
            both = jnp.where(lane == at, col, both)
        rpd_acc[...] = both

    def stage3(kind, take):
        for b, (k0, n) in enumerate(SECOND[kind]):
            for side in range(2):
                second(kind, side, span(k0, n), b_sem.at[side, SECOND_AT[kind] + b]).wait_recv()
                lax.fori_loop(k0, k0 + n, lambda k, _: [take(side, k), _][1], 0)

    def to_group(buf, at, i, n, axis, here):
        for d in range(1, n):
            send(buf.at[at], buf.at[at], stat_send.at[i], stat_recv.at[i],
                 {axis: lax.rem(here + d, n)}).start()

    def to_all(buf, i):
        for to in others:
            send(buf.at[linear], buf.at[linear], stat_send.at[i], stat_recv.at[i], to).start()

    def spread(buf, i, n):
        part = buf.at[pl.ds(0, n - 1)]
        return send(part, part, stat_send.at[i], stat_recv.at[i], mate)

    def gathered(buf, i, n):
        spread(buf, i, n).wait_recv()
        out = buf[0]
        for d in range(1, n):
            out = out + buf[d]
        return out

    stage3(U_, stage3_u)
    stage3(QO_, stage3_qo)
    vec_y.wait_recv()
    vec = vec_mid[1] + vec_in[2]
    hv[...] = vec
    rp = rp_acc[...]
    for t in range(ROW_TILES):
        for m, ref in enumerate((p_q, p_o)):
            row = jnp.sum(ref[pl.ds(SUB * t, SUB), :], axis=1, keepdims=True)
            rp = jnp.where(lane == ROW_TILES * m + t, row, rp)
    rp_all[z] = rp
    cs = [jnp.sum(cs_qo[k], axis=0, keepdims=True) for k in range(STEPS)]
    cs.append(jnp.sum(cs_u[...], axis=0, keepdims=True))
    cs_all[me] = jnp.concatenate(cs + [jnp.zeros((1, WIDE - QO - UP), F32)], axis=1)
    to_group(rp_all, z, 0, TP, "tp", z)
    to_group(cs_all, me, 1, FSDP, "fsdp", me)
    pack = jnp.where(lane1 == VEC_AT, jnp.sum(vec * vec, axis=1, keepdims=True), 0.0)
    for m in range(4):
        pack = jnp.where(lane1 == VR_AT + m, old_sums[m], pack)
    for m in range(3):
        pack = jnp.where(lane1 == m, total(jnp.where(masks[m], rp, 0.0)), pack)

    stage3(D_, stage3_d)
    rs = rs_d[...]
    s_all[linear] = jnp.where(lane1 == 3, total(rs), pack)
    to_all(s_all, 4)
    rsd_all[z] = jnp.sum(rs, axis=0, keepdims=True)
    to_group(rsd_all, z, 2, TP, "tp", z)
    rpd_all[me] = rpd_acc[...]
    to_group(rpd_all, me, 3, FSDP, "fsdp", me)

    vc_old = jnp.concatenate([c_q[...], c_o[...], c_u[...], jnp.ones((1, WIDE - QO - UP), F32)], axis=1)
    rp = gathered(rp_all, 0, TP)
    cs = gathered(cs_all, 1, FSDP)
    rsd = gathered(rsd_all, 2, TP)
    rpd = gathered(rpd_all, 3, FSDP)
    pack = gathered(s_all, 4, DEVICES)
    squares = [pick(pack, m) for m in range(4)]
    norm = jnp.sqrt((squares[0] + squares[1]) + (squares[2] + squares[3]) + pick(pack, VEC_AT) / FSDP)
    clip = jnp.minimum(1.0, 1.0 / norm)

    def clipped(v):
        return jnp.where(clip > 0.0, (v * clip) * clip, 0.0)

    means = []
    for m in range(4):
        r_all, c_all = float(ROWS[m] * FSDP), float(COLS[m] * TP)
        means.append(KEEP * (pick(pack, VR_AT + m) / (TP * r_all))
                     + MIX * (clipped(squares[m]) / (r_all * c_all) + EPSILON))
    mean_rp = jnp.where(masks[0], means[0], jnp.where(masks[1], means[1], means[2]))
    wide = jnp.where(masks[0], float(COLS[0] * TP), jnp.where(masks[1], float(COLS[1] * TP), float(COLS[2] * TP)))
    row_new = KEEP * rp_old[...] + MIX * (clipped(rp) / wide + EPSILON)
    row_sq = mean_rp / row_new
    rowd_new = KEEP * r_d[...] + MIX * (clipped(rsd) / float(DC * TP) + EPSILON)
    rowd_buf[...] = clip * jnp.sqrt(means[3] / rowd_new)
    col_new = KEEP * vc_old + MIX * (clipped(cs) / float(R * FSDP) + EPSILON)
    col_buf[...] = clip / jnp.sqrt(col_new)
    cold_new = KEEP * rpd_old[...] + MIX * (clipped(rpd) / float(DR * FSDP) + EPSILON)
    cold_sq = 1.0 / cold_new

    def tile(ref, j):
        return jnp.broadcast_to(ref[:, pl.ds(LANE * j, LANE)], (SUB, LANE))

    zero = jnp.zeros((SUB, LANE), F32)
    acc = [zero] * 4
    in_q = lane < Q_LEFT
    col_t = [tile(col_buf, j) for j in range(STEPS + UP // LANE)]
    for t in range(ROW_TILES):
        rows = pl.ds(SUB * t, SUB)
        part = [zero] * 3
        for j in range(STEPS):
            u = hqo[rows, pl.ds(LANE * j, LANE)] * col_t[j]
            u = u * u
            if j == Q_FULL:
                part[0] = part[0] + jnp.where(in_q, u, 0.0)
                part[1] = part[1] + jnp.where(in_q, 0.0, u)
            else:
                part[j // Q_FULL] = part[j // Q_FULL] + u
        for j in range(UP // LANE):
            u = hu[rows, pl.ds(LANE * j, LANE)] * col_t[STEPS + j]
            part[2] = part[2] + u * u
        for m in range(3):
            acc[m] = acc[m] + part[m] * across(row_sq, ROW_TILES * m + t)
    rowd_t = [tile(rowd_buf, j) for j in range(DR // LANE)]
    for t in range(D_TILES):
        part = zero
        for j in range(DR // LANE):
            u = hd[pl.ds(SUB * t, SUB), pl.ds(LANE * j, LANE)] * rowd_t[j]
            part = part + u * u
        acc[3] = acc[3] + part * across(cold_sq, t)
    vec = hv[...] * clip
    v_new = KEEP * vv_in[...] + MIX * (vec * vec + EPSILON)
    vec = vec / jnp.sqrt(v_new)
    pack = jnp.where(lane1 == VEC_AT, jnp.sum(vec * vec, axis=1, keepdims=True), 0.0)
    for m in range(4):
        pack = jnp.where(lane1 == m, total(acc[m]), pack)
    u_all[linear] = pack
    to_all(u_all, 5)

    vv_new[...] = v_new
    hv[...] = vec
    row = jnp.sqrt(row_sq)
    cold = jnp.sqrt(cold_sq)
    for t in range(ROW_TILES):
        rows = pl.ds(SUB * t, SUB)
        scale = [across(row, ROW_TILES * m + t) for m in range(3)]
        mixed = jnp.where(in_q, scale[0], scale[1])
        for j in range(STEPS):
            at = pl.ds(LANE * j, LANE)
            hqo[rows, at] = hqo[rows, at] * col_t[j] * (mixed if j == Q_FULL else scale[j // Q_FULL])
        for j in range(UP // LANE):
            at = pl.ds(LANE * j, LANE)
            hu[rows, at] = hu[rows, at] * col_t[STEPS + j] * scale[2]
    for t in range(D_TILES):
        rows = pl.ds(SUB * t, SUB)
        scale = across(cold, t)
        for j in range(DR // LANE):
            at = pl.ds(LANE * j, LANE)
            hd[rows, at] = hd[rows, at] * rowd_t[j] * scale
    for m, ref in enumerate((n_rq, n_ro, n_ru)):
        ref[...] = from_tiles(row_new, ROW_TILES * m, R)
    n_rd[...] = rowd_new
    n_cq[...] = col_new[:, :COLS[0]]
    n_co[...] = col_new[:, COLS[0]:QO]
    n_cu[...] = col_new[:, QO:QO + UP]
    n_cd[...] = from_tiles(cold_new, 0, DC)

    for kind in range(3):
        send(peers[kind], peers[kind], push_sem.at[kind], peer_sem.at[0, 0], mate).wait_send()
        send(firsts[kind], firsts[kind], first_sem.at[kind], a_sem.at[kind, 0, 0], mate).wait_send()
        send(seconds[kind], seconds[kind], second_sem.at[kind], b_sem.at[0, 0], mate).wait_send()
    for copy in (vec_core, vec_x, vec_y):
        copy.wait_send()
    groups = ((rp_all, TP), (cs_all, FSDP), (rsd_all, TP), (rpd_all, FSDP), (s_all, DEVICES), (u_all, DEVICES))
    for i, (buf, n) in enumerate(groups):
        if i < len(groups) - 1:
            spread(buf, i, n).wait_send()

    pack = gathered(u_all, len(groups) - 1, DEVICES)
    count = jnp.full((1, LANE), float(VEC * TP * FSDP), F32)
    for m in range(4):
        count = jnp.where(lane1 == m, float(ROWS[m] * FSDP * COLS[m] * TP), count)
    inv_out[...] = 1.0 / jnp.maximum(1.0, jnp.sqrt(pack / count))
    spread(u_all, len(groups) - 1, DEVICES).wait_send()


PIECES = ((3, 0, 96), (3, 96, 128), (3, 224, 128), (2, 0, 64), (2, 64, 64), (2, 128, 48), (0, 0, 96), (0, 96, 80), (1, 0, R))
HELD = (ROWS[:3] + (DC,), COLS[:3] + (DR,))
GROUP = 16


def update_kernel(*refs):
    (hqo, hu, hd, hv, inv, wq, wo, wu, wd, wv, mq, mo, mu, md, mv,
     vrq, vro, vru, vrd, vcq, vco, vcu, vcd, vv,
     wq_out, wo_out, wu_out, wd_out, wv_out, mq_out, mo_out, mu_out, md_out, mv_out,
     vrq_out, vcq_out, vro_out, vco_out, vru_out, vcu_out, vrd_out, vcd_out, vv_out,
     bwq, bwo, bwu, bwd, bmq, bmo, bmu, bmd, bwv, bmv, out_sem, small_sem) = refs
    held = ((hqo, 0), (hqo, COLS[0]), (hu, 0), (hd, 0))
    w_in, m_in = (wq, wo, wu, wd), (mq, mo, mu, md)
    w_buf, m_buf = (bwq, bwo, bwu, bwd), (bmq, bmo, bmu, bmd)
    w_out, m_out = (wq_out, wo_out, wu_out, wd_out), (mq_out, mo_out, mu_out, md_out)

    def finish(u, w, m):
        m_new = (MOMENTUM * m.astype(F32) + (1.0 - MOMENTUM) * u).astype(BF16)
        return w - LEARN_RATE * (m_new.astype(F32) + WEIGHT_DECAY * w), m_new

    passed = ((vrq, vrq_out), (vro, vro_out), (vru, vru_out), (vrd, vrd_out),
              (vcq, vcq_out), (vco, vco_out), (vcu, vcu_out), (vcd, vcd_out), (vv, vv_out))
    stores = [pltpu.make_async_copy(src, dst, small_sem.at[i]) for i, (src, dst) in enumerate(passed)]
    w_new, m_new = finish(hv[...] * inv[:, VEC_AT:VEC_AT + 1], wv[...], mv[...])
    bwv[...] = w_new
    bmv[...] = m_new
    stores.append(pltpu.make_async_copy(bwv, wv_out, small_sem.at[len(passed)]))
    stores.append(pltpu.make_async_copy(bmv, mv_out, small_sem.at[len(passed) + 1]))
    for copy in stores:
        copy.start()
    for m, r0, n in PIECES:
        scale = inv[:, m:m + 1]
        buf, c0 = held[m]

        for k in range(n // GROUP):
            rows = pl.ds(r0 + GROUP * k, GROUP)
            u = buf[rows, pl.ds(c0 // LANE * LANE, c0 % LANE + HELD[1][m])][:, c0 % LANE:]
            w_new, m_new = finish(u * scale, w_in[m][rows, :], m_in[m][rows, :])
            w_buf[m][rows, :] = w_new
            m_buf[m][rows, :] = m_new
        rows = pl.ds(r0, n)
        for j, (src, dst) in enumerate(((w_buf, w_out), (m_buf, m_out))):
            pltpu.make_async_copy(src[m].at[rows, :], dst[m].at[rows, :], out_sem.at[m, j]).start()
    for m in range(4):
        for j, (src, dst) in enumerate(((w_buf, w_out), (m_buf, m_out))):
            stores.append(pltpu.make_async_copy(src[m], dst[m], out_sem.at[m, j]))
    for copy in stores:
        copy.wait()


IN_HBM = pl.BlockSpec(memory_space=pltpu.HBM)
IN_VMEM = pl.BlockSpec(memory_space=pltpu.VMEM)
MIB = 1024 * 1024


def f32(*shape):
    return jax.ShapeDtypeStruct(shape, F32)


def vmem(*shape):
    return pltpu.VMEM(shape, F32)


def local_step(g_qkv, g_out, g_up, g_down, g_vec, w_qkv, w_out, w_up, w_down, w_vec,
               m_qkv, m_out, m_up, m_down, m_vec, vr_qkv, vc_qkv, vr_out, vc_out,
               vr_up, vc_up, vr_down, vc_down, v_vec):
    dma = pltpu.SemaphoreType.DMA
    rows_shapes = [(1, n) for n in ROWS]
    cols_shapes = [(1, n) for n in COLS]
    h_shapes = [(R, QO), (R, UP), (DC, DR)]
    wide_u, wide_d, vec = (R, UP), (DC, DR), (1, VEC)
    shapes = [
        (2, 2, 2, SUB, UP), (SLOTS, LANE, QO), (2, 2) + wide_u, (2, 2) + wide_d,
        (STEPS, LANE, QO), (2, 2) + wide_u, (2, 2) + wide_d, (STEPS, 2, 2, R, LANE),
        (STEPS, 2, R, LANE), (2,) + wide_u, (2,) + wide_d, (STEPS, R, LANE), wide_u, wide_d,
        vec, (3,) + vec, (2,) + vec, vec] + rows_shapes + cols_shapes + [
        (R, LANE), (R, LANE), (STEPS, SUB, LANE), (SUB, UP), (SUB, DR)] + [(SUB, LANE)] * 4 + [
        (1, WIDE), (1, DR),
        (FSDP, 1, WIDE), (TP, SUB, LANE), (TP, 1, DR), (FSDP, SUB, LANE),
        (DEVICES, 1, LANE), (DEVICES, 1, LANE)]
    sems = [(2, SLOTS), (2, 2 * SLOTS), (3,), (3,), (3,), (3, 2, len(BATCHES)),
            (2, SECOND_AT[-1] + len(SECOND[-1])), (3,), (3,), (6,), (6,), (2,)]
    ws = [w_qkv[0], w_out[0], w_up[0], w_down[0].T, w_vec]
    ms = [m_qkv[0], m_out[0], m_up[0], m_down[0].T, m_vec]
    mats = list(zip(*HELD))
    state = [f32(*s) for s in mats + [vec]] + [jax.ShapeDtypeStruct(s, BF16) for s in mats + [vec]]
    inputs = [pltpu.with_memory_space_constraint(a, pltpu.HBM)
              for a in (g_qkv[0, 0].T, g_out[0, 0].T, g_up.reshape(2, 2, 2, R, UP), g_down[0, 0].T, g_vec[0],
                        vr_qkv, vr_out, vr_up, vr_down, vc_qkv, vc_out, vc_up, vc_down, v_vec, *ws, *ms)]
    reduced = pl.pallas_call(
        reduce_kernel,
        name="reduce_and_scale",
        out_shape=([f32(*s) for s in h_shapes + [vec, (1, LANE)]] + state
                   + [f32(*s) for s in rows_shapes + cols_shapes + [vec]]),
        in_specs=[IN_HBM] * 24,
        out_specs=[IN_VMEM] * 24,
        scratch_shapes=[vmem(*s) for s in shapes] + [dma(s) for s in sems] + [pltpu.SemaphoreType.REGULAR((TP + 1,))],
        compiler_params=pltpu.CompilerParams(
            collective_id=0, has_side_effects=True, vmem_limit_bytes=A_MIB * MIB),
    )(*inputs)

    outs = pl.pallas_call(
        update_kernel,
        name="update",
        out_shape=(state + [f32(*s) for m in range(4) for s in (rows_shapes[m], cols_shapes[m])] + [f32(*vec)]),
        in_specs=[IN_VMEM] * 24,
        out_specs=[IN_HBM] * 19,
        scratch_shapes=([vmem(*s) for s in mats] + [pltpu.VMEM(s, BF16) for s in mats]
                        + [vmem(*vec), pltpu.VMEM(vec, BF16), dma((4, 2)), dma((11,))]),
        compiler_params=pltpu.CompilerParams(vmem_limit_bytes=B_MIB * MIB),
    )(*reduced)
    outs = list(outs)
    for i in range(10):
        if i % 5 == 3:
            outs[i] = outs[i].T
        if i % 5 != 4:
            outs[i] = outs[i][None]
    return tuple(outs)


A_MIB, B_MIB = 46, 12


def solution(mesh):
    grad_spec = P("fsdp", None, None, "tp")
    vec_grad_spec = P("fsdp", None, "tp")
    mat_spec = P(None, "fsdp", "tp")
    vec_spec = P(None, "tp")
    row_spec = P(None, "fsdp")
    col_spec = P(None, "tp")
    state_specs = ((mat_spec,) * 4 + (vec_spec,) + (mat_spec,) * 4 + (vec_spec,)
                   + (row_spec, col_spec) * 4 + (vec_spec,))
    arg_specs = (grad_spec,) * 4 + (vec_grad_spec,) + state_specs
    return jax.shard_map(local_step, mesh=mesh, in_specs=arg_specs, out_specs=state_specs, check_vma=False)
```
